32 devices in a mesh: grp: 2 (over y), sp: 16 (over z, x, core).
Axes of the slice: x: 2, y: 2, z: 4, core: 2. Of those that a mesh axis runs over, the one named last changes fastest.
Arguments:
- alpha: float32 [20, 16, 4096], P('grp', None, 'sp'), may hold values from -6 to 6
- ensemble: bfloat16 [20, 3, 16, 4096], P('grp', None, None, 'sp'), may hold values from -6 to 6
- static_std: float32 [3, 16, 4096], P(None, 'grp', 'sp'), may hold values from 0.2 to 1
- control: float32 [3, 16, 4096], P(None, 'grp', 'sp'), may hold values from -6 to 6
- loc_spectrum: float32 [1024], replicated, may hold values from 0.00024414062 to 0.001953125
- obs_cell: int32 [32768], P(('grp', 'sp')), may hold values from 0 to 65535, as said below
- obs_step: int32 [32768], P(('grp', 'sp')), may hold values from 0 to 2
- innovation: float32 [32768], P(('grp', 'sp')), may hold values from -6 to 6
- obs_weight: float32 [32768], P(('grp', 'sp')), may hold values from 0.5 to 4
Outputs:
- grad_alpha: float32 [20, 16, 4096], P('grp', None, 'sp')
- grad_control: float32 [3, 16, 4096], P(None, 'grp', 'sp')
The draws below stay inside these ranges and needn't reach their ends.
Inputs may be any that keep to these rules, and one draw needn't show every extreme that they name: `obs_cell`: an entry is row * 4096 + column. Entries 1024 * b to 1024 * (b + 1) - 1 lie in the tile of 8 rows from row 8 * (b // 16) and 256 columns from column 256 * (b % 16).
All inputs are finite; a program needn't handle non-finite values.
Results may differ from the reference program's by a relative error of at most 0.0075.
Values may be sent and summed in bfloat16 or wider, within the bound.
A program may use at most 128 MiB of HBM per device.

```python
import math
import jax
import jax.numpy as jnp
from jax import lax

NX = 4096
KEEP = 1024
STEPS = 2
OBS_DEV = 1024
MEMBERS = 20
NY = 16
TILE_ROWS = 8
TILE_COLS = 256
OBS = 32768


def draw_obs_cell(key, part):
    base = jax.random.fold_in(key, 11)
    row_key, col_key = jax.random.split(base)
    blocks = jnp.arange(OBS, dtype=jnp.int32) // OBS_DEV
    col_blocks = NX // TILE_COLS
    block_row = blocks // col_blocks
    block_col = blocks % col_blocks
    local_row = jax.random.randint(row_key, (OBS,), 0, TILE_ROWS, dtype=jnp.int32)
    local_col = jax.random.randint(col_key, (OBS,), 0, TILE_COLS, dtype=jnp.int32)
    return ((block_row * TILE_ROWS + local_row) * NX + block_col * TILE_COLS + local_col).astype(jnp.int32)


def plant(result, key, low, high):
    spot = [jax.random.randint(jax.random.fold_in(key, axis), (), 0, length) for axis, length in enumerate(result.shape)]
    main_axis = result.shape.index(max(result.shape))
    beside = spot[:main_axis] + [(spot[main_axis] + 1) % result.shape[main_axis]] + spot[main_axis + 1:]
    return result.at[tuple(spot)].set(low).at[tuple(beside)].set(high)


def strengthened(array, rng, source, target, parts, factor):
    def block_of(dim):
        return (jnp.arange(array.shape[dim]) // (array.shape[dim] // parts)).reshape((-1,) + (1,) * (array.ndim - 1 - dim))

    one_side = jax.random.permutation(rng, parts)[block_of(target)]
    other_side = (block_of(target) + parts // 2) % parts
    return jnp.where((block_of(source) == one_side) | (block_of(source) == other_side), factor * array, array)


def block_scale(key, extent, shards, low, high):
    def one(axis_at, blocks):
        draws = jax.random.uniform(jax.random.fold_in(jax.random.fold_in(key, 6), axis_at), (blocks,), jnp.float32, low / len(shards), high / len(shards))
        return jnp.repeat(jnp.exp(draws), extent[axis_at] // blocks).reshape((-1,) + (1,) * (len(extent) - axis_at - 1))

    level = one(*shards[0])
    for cut in shards[1:]:
        level = level * one(*cut)
    return level


def centred(stream_key, shape, scale, limit, pieces=(), kind=jnp.bfloat16):
    drawn = jax.random.normal(stream_key, shape, jnp.float32) * scale
    if len(pieces) > 0:
        drawn = block_scale(stream_key, shape, pieces, -0.22, 0.18) * drawn
    return jnp.clip(drawn, min=-limit, max=limit).astype(kind)


def noise_with(key, dims, scale, limit, pieces, heavy, held_as=jnp.bfloat16):
    array = scale * jax.random.normal(key, dims, jnp.float32)
    if pieces:
        array = array * block_scale(key, dims, pieces, -0.22, 0.18)
    return jnp.clip(strengthened(array, jax.random.fold_in(key, 3), *heavy), -limit, limit).astype(held_as)


def setup_inputs(seed: int = 0) -> dict:
    key_of = jax.random.split(jax.random.key(seed), 10)
    alpha = centred(key_of[0], (MEMBERS, NY, NX), 1.0, 6.0, ((0, 2), (2, 16)), jnp.float32)
    ensemble = noise_with(key_of[1], (MEMBERS, 3, NY, NX), 1.0, 6.0, ((0, 2), (3, 16)), (0, 2, 2, 2.0))
    static_std = jnp.clip(jnp.exp(math.log(1.0) - 1.609438 * jax.random.uniform(key_of[2], (3, NY, NX), jnp.float32) ** block_scale(key_of[2], (3, NY, NX), ((1, 2), (2, 16)), -0.2, 0.2)), 0.2, 1.0)
    control = centred(key_of[3], (3, NY, NX), 1.0, 6.0, ((1, 2), (2, 16)), jnp.float32)
    loc_spectrum = jnp.clip(jnp.exp(jax.random.uniform(key_of[4], (KEEP,), jnp.float32, math.log(0.00024414062), math.log(0.001953125))), 0.00024414062, 0.001953125)
    obs_cell = draw_obs_cell(jax.random.fold_in(key_of[9], 71), 0)
    obs_step = plant(jax.random.randint(key_of[6], (OBS,), 0, STEPS + 1), jax.random.fold_in(key_of[6], 1), 0, STEPS).astype(jnp.int32)
    innovation = centred(key_of[7], (OBS,), 1.0, 6.0, ((0, 32),), jnp.float32)
    obs_weight = jnp.clip(jnp.exp(math.log(4.0) - 2.0794415 * jax.random.uniform(key_of[8], (OBS,), jnp.float32) ** block_scale(key_of[8], (OBS,), ((0, 32),), -0.2, 0.2)), 0.5, 4.0)
    return {"alpha": alpha, "ensemble": ensemble, "static_std": static_std, "control": control, "loc_spectrum": loc_spectrum, "obs_cell": obs_cell, "obs_step": obs_step, "innovation": innovation, "obs_weight": obs_weight}


courant = 0.4

def spectral_filter(rows_data, loc_spectrum):
    length_x = rows_data.shape[1]
    kept_waves = loc_spectrum.shape[0]
    freq_block = math.gcd(kept_waves, 256)
    positions = jnp.arange(length_x, dtype=jnp.int32)
    filtered = jnp.zeros(rows_data.shape, jnp.float32)
    for start_wave in range(0, kept_waves, freq_block):
        waves = start_wave + jnp.arange(freq_block, dtype=jnp.int32)
        phases = positions[:, None] * waves[None, :] % length_x
        radians = 2.0 * math.pi / length_x * phases.astype(jnp.float32)
        fourier_basis = jnp.concatenate([jnp.cos(radians), jnp.sin(radians)], axis=1)
        weights = loc_spectrum[start_wave:start_wave + freq_block]
        weights = jnp.concatenate([weights, weights])
        coeffs = jnp.dot(rows_data, fourier_basis, precision=lax.Precision.HIGHEST, preferred_element_type=jnp.float32)
        filtered = filtered + jnp.dot(coeffs * weights[None, :], fourier_basis.T, precision=lax.Precision.HIGHEST, preferred_element_type=jnp.float32)
    return filtered

def diff_x(field):
    return 0.5 * (jnp.roll(field, -1, axis=-1) - jnp.roll(field, 1, axis=-1))

def diff_y(field):
    padded = jnp.pad(field, ((1, 1), (0, 0)))
    return 0.5 * (padded[2:] - padded[:-2])

def coriolis():
    rows_index = jnp.arange(NY, dtype=jnp.int32).astype(jnp.float32)
    return (0.1 + 0.2 * (rows_index + 0.5) / NY)[:, None]

def model_step(state, rotation):
    height, eastward, northward = (state[0], state[1], state[2])
    new_height = height - courant * (diff_x(eastward) + diff_y(northward))
    new_east = eastward - courant * diff_x(new_height) + rotation * northward
    new_north = northward - courant * diff_y(new_height) - rotation * eastward
    return jnp.stack([new_height, new_east, new_north])

def adjoint_step(state, rotation):
    back_h, back_u, back_w = (state[0], state[1], state[2])
    adj_height = back_h + courant * (diff_x(back_u) + diff_y(back_w))
    adj_east = back_u - rotation * back_w + courant * diff_x(adj_height)
    adj_north = back_w + rotation * back_u + courant * diff_y(adj_height)
    return jnp.stack([adj_height, adj_east, adj_north])

def reference(alpha, ensemble, static_std, control, loc_spectrum, obs_cell, obs_step, innovation, obs_weight):
    spread = 1.0 / math.sqrt(MEMBERS - 1)
    rotation = coriolis()
    localized = spectral_filter(alpha.reshape(MEMBERS * NY, NX), loc_spectrum).reshape(alpha.shape).astype(jnp.bfloat16)
    partial_value = jnp.einsum('mvyx,myx->vyx', ensemble.astype(jnp.float32), localized.astype(jnp.float32), precision=lax.Precision.HIGHEST)
    increment = static_std * control + spread * partial_value
    first_state = model_step(increment, rotation)
    second_state = model_step(first_state, rotation)
    states = (increment, first_state, second_state)
    observed = jnp.zeros(innovation.shape, jnp.float32)
    for moment in range(3):
        values = states[moment][0].reshape(-1)[obs_cell]
        observed = jnp.where(obs_step == moment, values, observed)
    misfit = obs_weight * (observed - innovation)
    zero_field = jnp.zeros((NY, NX), jnp.float32)
    forcings = []
    for moment in range(3):
        spread_obs = jnp.where(obs_step == moment, misfit, jnp.zeros_like(misfit))
        height_force = jnp.zeros((NY * NX,), jnp.float32).at[obs_cell].add(spread_obs).reshape(NY, NX)
        forcings.append(jnp.stack([height_force, zero_field, zero_field]))
    adjoint = adjoint_step(forcings[2], rotation) + forcings[1]
    adjoint = adjoint_step(adjoint, rotation) + forcings[0]
    grad_control = control + static_std * adjoint
    half = adjoint.astype(jnp.bfloat16)
    weighted = jnp.einsum('mvyx,vyx->myx', ensemble.astype(jnp.float32), half.astype(jnp.float32), precision=lax.Precision.HIGHEST)
    grad_alpha = alpha + spread * spectral_filter(weighted.reshape(MEMBERS * NY, NX), loc_spectrum).reshape(alpha.shape)
    return (grad_alpha, grad_control)
```

```python
import functools
import math

import jax
import jax.numpy as jnp
import numpy as np
from jax import lax
from jax.experimental import pallas as pl
from jax.experimental.pallas import tpu as pltpu
from jax.sharding import PartitionSpec as P

COURANT = 0.4
LANES = 128
HALO = 8
SLOTS = 16
BF16, F32 = jnp.bfloat16, jnp.float32
ANY = pl.BlockSpec(memory_space=pl.ANY)


def dot(a, b, contract=((1,), (0,))):
    return lax.dot_general(a, b, (contract, ((), ())), preferred_element_type=F32)


def split2(x):
    hi = x.astype(BF16)
    return hi, (x - hi.astype(F32)).astype(BF16)


def both(table):
    table = np.asarray(table, np.float32)
    hi = table.astype(BF16)
    return hi, (table - hi.astype(np.float32)).astype(BF16)


def add(a, b, sign=1.0):
    re = a[0] + b[0] if sign > 0 else a[0] - b[0]
    if b[1] is None:
        return re, a[1]
    if a[1] is None:
        return re, b[1] if sign > 0 else -b[1]
    return re, a[1] + b[1] if sign > 0 else a[1] - b[1]


def conj(a):
    return a[0], None if a[1] is None else -a[1]


def turn(a, eighths, n):
    at = (eighths % n) / n
    if at == 0:
        return a
    re, im = a
    if at == 0.25:
        return (jnp.zeros_like(re) if im is None else -im), re
    if at == 0.75:
        return (jnp.zeros_like(re) if im is None else im), -re
    c, s = math.cos(2 * math.pi * at), math.sin(2 * math.pi * at)
    if im is None:
        return c * re, s * re
    return c * re - s * im, c * im + s * re


def real_dft(xs):
    n = len(xs)
    if n == 1:
        return [(xs[0], None)]
    if n == 2:
        return [(xs[0] + xs[1], None), (xs[0] - xs[1], None)]
    half = n // 2
    even, odd = real_dft(xs[0::2]), real_dft(xs[1::2])
    out = [None] * (half + 1)
    for k in range(half // 2 + 1):
        t = turn(odd[k], -k, n)
        out[k] = add(even[k], t)
        if half - k != k:
            out[half - k] = conj(add(even[k], t, -1.0))
    return out


def real_sum(zs, n):
    if n == 1:
        return [zs[0][0]]
    if n == 2:
        return [zs[0][0] + zs[1][0], zs[0][0] - zs[1][0]]
    half = n // 2
    even, odd = [], []
    for k in range(half // 2 + 1):
        if half - k == k:
            even.append(zs[k])
            odd.append(turn(zs[k], k, n))
        else:
            other = conj(zs[half - k])
            even.append(add(zs[k], other))
            odd.append(turn(add(zs[k], other, -1.0), k, n))
    even, odd = real_sum(even, half), real_sum(odd, half)
    return [(even, odd)[p % 2][p // 2] for p in range(n)]


def dx(q):
    width = q.shape[1]
    return 0.5 * (pltpu.roll(q, width - 1, 1) - pltpu.roll(q, 1, 1))


def dy(q):
    rows = q.shape[0]
    at = lax.broadcasted_iota(jnp.int32, q.shape, 0)
    above = jnp.where(at < rows - 1, pltpu.roll(q, rows - 1, 0), 0.0)
    below = jnp.where(at > 0, pltpu.roll(q, 1, 0), 0.0)
    return 0.5 * (above - below)


def model_step(state, rotation):
    h, u, w = state
    h = h - COURANT * (dx(u) + dy(w))
    return h, u - COURANT * dx(h) + rotation * w, w - COURANT * dy(h) - rotation * u


def adjoint_step(state, rotation):
    h, u, w = state
    a = h + COURANT * (dx(u) + dy(w))
    return a, u - rotation * w + COURANT * dx(a), w + rotation * u + COURANT * dy(a)


def slot_of(v, m, members):
    spare = min(SLOTS - members, members)
    if v < 2:
        return v * SLOTS + m
    return members + m if m < spare else SLOTS + members + m - spare


def kernel(
    groups, parts, spread,
    alpha_any, ens_any, std_any, control_any, spectrum_any, cell_any, step_any, innovation_any, weight_any,
    fwd_hi_any, fwd_lo_any, inv_hi_any, inv_lo_any, tw_c_any, tw_s_any, pick_any,
    corr_ref, grad_control_ref,
    alpha, ens, std, control, spectrum, cell, step, innovation, weight,
    fwd_hi, fwd_lo, inv_hi, inv_lo, tw_c, tw_s, pick,
    stage, ens_stage, adjoint, waves, fields, wide,
    snd_a, rcv_a, snd_e, rcv_e, snd_i, rcv_i, snd_h, rcv_h, snd_o, rcv_o, rcv_f, edge, rcv_edge,
    load_sem, a_send, a_recv, e_send, e_recv, i_send, i_recv, h_send, h_recv, o_send, o_recv, f_send, f_recv,
):
    group, part = lax.axis_index("grp"), lax.axis_index("sp")
    left, right = lax.rem(part + parts - 1, parts), lax.rem(part + 1, parts)
    members, rows, cols = alpha.shape
    tile_rows = control.shape[1]
    tile = pl.ds(pl.multiple_of(group * tile_rows, tile_rows), tile_rows)
    spare = min(SLOTS - members, members)
    shift = members - spare
    halves = cols // LANES
    residues = parts // 2 + 1
    started = []

    barrier = pltpu.get_barrier_semaphore()
    for j in range(groups):
        for i in range(parts):
            if i + j > 0:
                device = {"grp": lax.rem(group + j, groups), "sp": lax.rem(part + i, parts)}
                pl.semaphore_signal(barrier, inc=1, device_id=device)

    pairs = [
        (alpha_any, alpha), (ens_any, ens), (cell_any, cell), (step_any, step), (innovation_any, innovation),
        (weight_any, weight), (std_any, std), (control_any, control), (spectrum_any, spectrum),
        (fwd_hi_any, fwd_hi), (fwd_lo_any, fwd_lo), (inv_hi_any, inv_hi), (inv_lo_any, inv_lo),
        (tw_c_any, tw_c), (tw_s_any, tw_s), (pick_any, pick),
    ]
    loads = [pltpu.make_async_copy(a, b, load_sem.at[i]) for i, (a, b) in enumerate(pairs)]
    for load in loads:
        load.start()

    loads[0].wait()
    for m in range(members):
        stage[:, m, :] = alpha[m]
    for m in range(SLOTS - members):
        stage[:, members + m, :] = alpha[m] if m < spare else jnp.zeros((rows, cols), F32)
    snd_a[...] = stage[...].astype(BF16)
    loads[1].wait()
    used = set()
    for v in range(3):
        for m in range(members):
            at = slot_of(v, m, members)
            used.add(at)
            ens_stage[:, at, :] = ens[m, v].astype(F32)
    for at in range(2 * SLOTS):
        if at not in used:
            ens_stage[:, at, :] = jnp.zeros((rows, cols), F32)
    snd_e[...] = ens_stage[...].astype(BF16)

    for load in loads[2:]:
        load.wait()
    pitch = -(-tile_rows // 8) * 8
    nx = cols * parts
    first = group * tile_rows
    row = jnp.zeros_like(cell)
    cells = cell[...]
    for r in range(1, tile_rows):
        row = row + jnp.where(cells >= (first + r) * nx, 1, 0)
    col = cells - (first + row) * nx - part * cols
    slot = step[...] * pitch + row
    observations = cells.shape[1]
    in_col = (lax.broadcasted_iota(jnp.int32, (cols, observations), 0) == col).astype(F32).astype(BF16)
    in_slot = lax.broadcasted_iota(jnp.int32, (3 * pitch, observations), 0) == slot
    obs_weight = weight[...]
    values = jnp.concatenate([
        jnp.where(in_slot, obs_weight, 0.0), jnp.where(in_slot, obs_weight * innovation[...], 0.0)
    ], axis=0)
    hi, lo = split2(values)
    summed = dot(hi, in_col, ((1,), (1,))) + dot(lo, in_col, ((1,), (1,)))
    for v in range(3):
        fields[v] = std[v] * control[v]
    for f in range(6):
        fields[3 + f] = summed[f * pitch : f * pitch + tile_rows]
    haloed = (0, 1, 2, 4, 5, 7, 8)
    lane = lax.broadcasted_iota(jnp.int32, (tile_rows, LANES), 1)
    packed = jnp.zeros((tile_rows, LANES), F32)
    for e, f in enumerate(haloed):
        ends = jnp.where(lane < LANES // 2, fields[f, :, :LANES], fields[f, :, cols - LANES :])
        window = (lane >= 2 * HALO * e) & (lane < 2 * HALO * (e + 1))
        packed = jnp.where(window, pltpu.roll(ends, (2 * HALO * e + HALO) % LANES, 1), packed)
    edge[...] = packed

    count = spectrum.shape[1]
    inner = count // parts
    wave = lax.broadcasted_iota(jnp.int32, (SLOTS * (-(-residues // SLOTS)), count), 1)
    residue = lax.broadcasted_iota(jnp.int32, wave.shape, 0)
    weights = jnp.broadcast_to(spectrum[...], wave.shape)
    forward = jnp.where((lax.rem(wave, parts) == residue) & (residue < residues), weights, 0.0)
    mirrored = (lax.rem(wave + residue, parts) == 0) & (residue > 0) & (residue < residues - 1)
    backward = jnp.where(mirrored, weights, 0.0)
    k = lax.broadcasted_iota(jnp.int32, (count, 4 * inner), 0)
    j = lax.rem(lax.broadcasted_iota(jnp.int32, (count, 4 * inner), 1), 2 * inner)
    ahead, behind = k - parts * (j - inner), k - parts * (inner - 1 - j)
    ahead = jnp.where((ahead >= 0) & (ahead < parts), 1.0, 0.0).astype(BF16)
    behind = jnp.where((behind >= 0) & (behind < parts), 1.0, 0.0).astype(BF16)
    f_hi, f_lo = split2(forward)
    b_hi, b_lo = split2(backward)
    waves[...] = dot(f_hi, ahead) + dot(f_lo, ahead) + dot(b_hi, behind) + dot(b_lo, behind)

    pl.semaphore_wait(barrier, groups * parts - 1)

    def all_to_all(source, target, send, recv):
        copies = []
        for i in range(1, parts):
            to = lax.rem(part + i, parts)
            copies.append(pltpu.make_async_remote_copy(
                src_ref=source.at[to], dst_ref=target.at[part],
                send_sem=send.at[i], recv_sem=recv.at[i], device_id={"sp": to},
            ))
            copies[-1].start()
        target[part] = source[part]
        started.extend(copies)
        return copies

    def received(copies):
        for copy in copies:
            copy.wait_recv()

    alpha_copies = all_to_all(snd_a, rcv_a, a_send, a_recv)
    ens_copies = all_to_all(snd_e, rcv_e, e_send, e_recv)
    field_copies = []
    for j in range(groups):
        to = lax.rem(group + j, groups)
        plans = [(1, right, edge, rcv_edge.at[0, group]), (2, left, edge, rcv_edge.at[1, group])]
        if j > 0:
            plans.append((0, part, fields, rcv_f.at[group]))
        for kind, at, source, target in plans:
            field_copies.append(pltpu.make_async_remote_copy(
                src_ref=source, dst_ref=target,
                send_sem=f_send.at[kind, j], recv_sem=f_recv.at[kind, j], device_id={"grp": to, "sp": at},
            ))
            field_copies[-1].start()
    started.extend(field_copies)
    rcv_f[group] = fields[...]

    def filtered(xs):
        pieces = [[x[:, h * LANES : (h + 1) * LANES] for x in xs] for h in range(halves)]
        spectra = [real_dft(piece) for piece in pieces]
        res, ims = [], []
        for k1 in range(residues):
            parts_re, parts_im = [], []
            for h in range(halves):
                c = tw_c[k1 : k1 + 1, h * LANES : (h + 1) * LANES]
                s = tw_s[k1 : k1 + 1, h * LANES : (h + 1) * LANES]
                re, im = spectra[h][k1]
                if k1 == 0:
                    parts_re.append(re)
                    parts_im.append(jnp.zeros_like(re))
                elif im is None:
                    parts_re.append(re * c)
                    parts_im.append(-re * s)
                else:
                    parts_re.append(re * c + im * s)
                    parts_im.append(im * c - re * s)
            res.append(jnp.concatenate(parts_re + parts_im, axis=1))
        y_hi, y_lo = split2(jnp.concatenate(res, axis=0))
        z = dot(y_hi, fwd_hi[...]) + dot(y_lo, fwd_hi[...]) + dot(y_hi, fwd_lo[...])
        z = jnp.concatenate(
            [z[k1 * SLOTS : (k1 + 1) * SLOTS] * waves[k1 : k1 + 1, :] for k1 in range(residues)], axis=0
        )
        z_hi, z_lo = split2(z)
        v = dot(z_hi, inv_hi[...]) + dot(z_lo, inv_hi[...]) + dot(z_hi, inv_lo[...])
        outs = []
        for h in range(halves):
            zs = []
            for k1 in range(residues):
                c = tw_c[k1 : k1 + 1, h * LANES : (h + 1) * LANES]
                s = tw_s[k1 : k1 + 1, h * LANES : (h + 1) * LANES]
                at = slice(k1 * SLOTS, (k1 + 1) * SLOTS)
                re = v[at, h * LANES : (h + 1) * LANES]
                im = v[at, cols + h * LANES : cols + (h + 1) * LANES]
                zs.append((re, im) if k1 == 0 else (re * c - im * s, im * c + re * s))
            outs.append(real_sum(zs, parts))
        return [jnp.concatenate([outs[h][p] for h in range(halves)], axis=1) for p in range(parts)]

    received(alpha_copies)
    localized = filtered([rcv_a[p].astype(F32) for p in range(parts)])
    received(ens_copies)
    at_slot = lax.broadcasted_iota(jnp.int32, (SLOTS, cols), 0)
    firsts, seconds = [], []
    for p in range(parts):
        loc = localized[p].astype(BF16).astype(F32)
        moved = jnp.where(at_slot < members, loc, pltpu.roll(loc, shift, 0)) if shift else loc
        firsts.append(rcv_e[p, :SLOTS].astype(F32) * loc)
        seconds.append(rcv_e[p, SLOTS:].astype(F32) * moved)
    a_hi, a_lo = split2(jnp.concatenate(firsts, axis=0))
    b_hi, b_lo = split2(jnp.concatenate(seconds, axis=0))
    pick_a, pick_b = pick[:, : parts * SLOTS], pick[:, parts * SLOTS :]
    inc = spread * (dot(pick_a, a_hi) + dot(pick_a, a_lo) + dot(pick_b, b_hi) + dot(pick_b, b_lo))
    lane = lax.broadcasted_iota(jnp.int32, (parts, LANES), 1)
    packed = jnp.zeros((parts, LANES), F32)
    for v in range(3):
        field = inc[v * parts : (v + 1) * parts]
        for h in range(halves):
            snd_i[:, v * halves + h, :] = field[:, h * LANES : (h + 1) * LANES]
        after = pltpu.roll(field[:, :LANES], parts - 1, 0)
        before = pltpu.roll(field[:, cols - LANES :], 1, 0)
        ends = pltpu.roll(jnp.where(lane < LANES // 2, after, before), 2 * HALO * v + HALO, 1)
        packed = jnp.where((lane >= 2 * HALO * v) & (lane < 2 * HALO * (v + 1)), ends, packed)
    snd_i[:, 3 * halves, :] = packed
    copies = []
    for i in range(parts):
        for j in range(groups):
            if i + j > 0:
                g, to = lax.rem(group + j, groups), lax.rem(part + i, parts)
                copies.append(pltpu.make_async_remote_copy(
                    src_ref=snd_i.at[to], dst_ref=rcv_i.at[group, part],
                    send_sem=i_send.at[i, j], recv_sem=i_recv.at[i, j], device_id={"grp": g, "sp": to},
                ))
                copies[-1].start()
    rcv_i[group, part] = snd_i[part]
    started.extend(copies)

    received(field_copies)
    lane = lax.broadcasted_iota(jnp.int32, (tile_rows, LANES), 1)
    for g in range(groups):
        at = slice(g * tile_rows, (g + 1) * tile_rows)
        for f in range(9):
            wide[f, at, :cols] = rcv_f[g, f]
            if f in haloed:
                back = LANES - (2 * HALO * haloed.index(f) + HALO)
                before, after = (pltpu.roll(rcv_edge[side, g], back, 1) for side in (0, 1))
                wide[f, at, cols:] = jnp.where(lane < LANES // 2, after, before)
            else:
                wide[f, at, cols:] = jnp.zeros((tile_rows, LANES), F32)

    received(copies)

    def gathered(index):
        total = rcv_i[0, :, index, :]
        for g in range(1, groups):
            total = total + rcv_i[g, :, index, :]
        return total

    ends = gathered(3 * halves)
    state0 = []
    for v in range(3):
        pieces = [gathered(v * halves + h) for h in range(halves)]
        pieces.append(pltpu.roll(ends, LANES - (2 * HALO * v + HALO), 1))
        state0.append(jnp.concatenate(pieces, axis=1) + wide[v])
    row_at = lax.broadcasted_iota(jnp.int32, (rows, cols + LANES), 0).astype(F32)
    rotation = 0.1 + 0.2 * (row_at + 0.5) / rows
    state1 = model_step(state0, rotation)
    state2 = model_step(state1, rotation)
    forcing = [wide[3 + t] * s[0] - wide[6 + t] for t, s in enumerate((state0, state1, state2))]
    zero = jnp.zeros_like(rotation)
    h, u, w = adjoint_step((forcing[2], zero, zero), rotation)
    h, u, w = adjoint_step((h + forcing[1], u, w), rotation)
    for v, field in enumerate((h + forcing[0], u, w)):
        field = field[:, :cols]
        adjoint[v] = field
        half = field.astype(BF16).astype(F32)
        for h in range(halves):
            snd_h[:, v * halves + h, :] = half[:, h * LANES : (h + 1) * LANES]
    copies = all_to_all(snd_h, rcv_h, h_send, h_recv)
    for v in range(3):
        grad_control_ref[v] = control[v] + std[v] * adjoint[v, tile, :]
    received(copies)
    weighted = []
    for p in range(parts):
        halfs = []
        for v in range(3):
            pieces = [
                jnp.broadcast_to(rcv_h[p, v * halves + h : v * halves + h + 1, :], (SLOTS, LANES)) for h in range(halves)
            ]
            halfs.append(jnp.concatenate(pieces, axis=1))
        a = rcv_e[p, :SLOTS].astype(F32) * jnp.where(at_slot < members, halfs[0], halfs[2])
        b = rcv_e[p, SLOTS:].astype(F32) * jnp.where(at_slot < members, halfs[1], halfs[2])
        own = jnp.where(at_slot < spare, pltpu.roll(a, SLOTS - members, 0), 0.0)
        if shift:
            own = jnp.where((at_slot >= spare) & (at_slot < members), pltpu.roll(b, SLOTS - shift, 0), own)
        weighted.append(a + b + own)
    outs = filtered(weighted)
    for p in range(parts):
        snd_o[p] = outs[p].astype(BF16)
    received(all_to_all(snd_o, rcv_o, o_send, o_recv))
    stage[...] = rcv_o[...].astype(F32)
    for m in range(members):
        corr_ref[m] = alpha[m] + spread * stage[:, m, :]
    for copy in started:
        copy.wait_send()


def tables(parts, cols, waves, members):
    length = parts * cols
    inner = waves // parts
    residues = parts // 2 + 1
    twist = 2 * np.pi * np.outer(np.arange(residues), np.arange(cols)) / length
    quotient = np.arange(-inner, inner)
    phase = 2 * np.pi * (np.outer(np.arange(cols), quotient) % cols) / cols
    c, s = np.cos(phase), np.sin(phase)
    forward = np.block([[c, -s], [s, c]])
    pick = np.zeros((3 * parts, 2, parts, SLOTS), np.float32)
    for p in range(parts):
        for v in range(3):
            for m in range(members):
                at = slot_of(v, m, members)
                pick[v * parts + p, at // SLOTS, p, at % SLOTS] = 1.0
    return (
        *both(forward), *both(forward.T.copy()), np.cos(twist).astype(np.float32), np.sin(twist).astype(np.float32),
        pick.reshape(3 * parts, 2 * parts * SLOTS).astype(BF16),
    )


def per_device(alpha, ensemble, static_std, control, loc_spectrum, obs_cell, obs_step, innovation, obs_weight):
    members, rows, cols = alpha.shape
    groups, parts = lax.axis_size("grp"), lax.axis_size("sp")
    spread = 1.0 / math.sqrt(members * groups - 1)
    assert rows == parts and 3 * members <= 2 * SLOTS
    tile_rows = control.shape[1]
    residues = parts // 2 + 1
    inner = loc_spectrum.shape[0] // parts
    operands = (
        alpha, ensemble, static_std, control, loc_spectrum[None],
        obs_cell[None], obs_step[None], innovation[None], obs_weight[None],
        *tables(parts, cols, loc_spectrum.shape[0], members),
    )
    message = (8 * (-(-(3 * cols // LANES + 1) // 8)), LANES)
    vmem = pl.BlockSpec(memory_space=pltpu.VMEM)
    dma = pltpu.SemaphoreType.DMA
    corr, grad_control = pl.pallas_call(
        functools.partial(kernel, groups, parts, spread),
        out_shape=(
            jax.ShapeDtypeStruct(alpha.shape, F32),
            jax.ShapeDtypeStruct(control.shape, F32),
        ),
        in_specs=[ANY] * len(operands),
        out_specs=(vmem, vmem),
        scratch_shapes=[
            *[pltpu.VMEM(t.shape, t.dtype) for t in operands],
            pltpu.VMEM((rows, SLOTS, cols), F32),
            pltpu.VMEM((rows, 2 * SLOTS, cols), F32),
            pltpu.VMEM((3, rows, cols), F32),
            pltpu.VMEM((SLOTS * (-(-residues // SLOTS)), 4 * inner), F32),
            pltpu.VMEM((9, tile_rows, cols), F32),
            pltpu.VMEM((9, rows, cols + LANES), F32),
            pltpu.VMEM((parts, SLOTS, cols), BF16), pltpu.VMEM((parts, SLOTS, cols), BF16),
            pltpu.VMEM((parts, 2 * SLOTS, cols), BF16), pltpu.VMEM((parts, 2 * SLOTS, cols), BF16),
            pltpu.VMEM((parts, *message), F32), pltpu.VMEM((groups, parts, *message), F32),
            pltpu.VMEM((parts, *message), F32), pltpu.VMEM((parts, *message), F32),
            pltpu.VMEM((parts, SLOTS, cols), BF16), pltpu.VMEM((parts, SLOTS, cols), BF16),
            pltpu.VMEM((groups, 9, tile_rows, cols), F32),
            pltpu.VMEM((tile_rows, LANES), F32), pltpu.VMEM((2, groups, tile_rows, LANES), F32),
            dma((len(operands),)),
            dma((parts,)), dma((parts,)), dma((parts,)), dma((parts,)),
            dma((parts, groups)), dma((parts, groups)),
            dma((parts,)), dma((parts,)), dma((parts,)), dma((parts,)),
            dma((3, groups)), dma((3, groups)),
        ],
        compiler_params=pltpu.CompilerParams(collective_id=0, has_side_effects=True, vmem_limit_bytes=40 << 20),
    )(*operands)
    return corr, grad_control


def solution(mesh):
    flat = P(("grp", "sp"))
    tile = P(None, "grp", "sp")
    return jax.shard_map(
        per_device,
        mesh=mesh,
        in_specs=(P("grp", None, "sp"), P("grp", None, None, "sp"), tile, tile, P(), flat, flat, flat, flat),
        out_specs=(P("grp", None, "sp"), tile),
        check_vma=False,
    )
```

```python
import functools
import math

import jax
import jax.numpy as jnp
import numpy as np
from jax import lax
from jax.experimental import pallas as pl
from jax.experimental.pallas import tpu as pltpu
from jax.sharding import PartitionSpec as P

COURANT = 0.4
LANES = 128
HALO = 8
SLOTS = 16
BF16, F32 = jnp.bfloat16, jnp.float32
HBM = pl.BlockSpec(memory_space=pltpu.HBM)


def dot(a, b, contract=((1,), (0,))):
    return lax.dot_general(a, b, (contract, ((), ())), preferred_element_type=F32)


def split2(x):
    hi = x.astype(BF16)
    return hi, (x - hi.astype(F32)).astype(BF16)


def both(table):
    table = np.asarray(table, np.float32)
    hi = table.astype(BF16)
    return hi, (table - hi.astype(np.float32)).astype(BF16)


def add(a, b, sign=1.0):
    re = a[0] + b[0] if sign > 0 else a[0] - b[0]
    if b[1] is None:
        return re, a[1]
    if a[1] is None:
        return re, b[1] if sign > 0 else -b[1]
    return re, a[1] + b[1] if sign > 0 else a[1] - b[1]


def conj(a):
    return a[0], None if a[1] is None else -a[1]


def turn(a, eighths, n):
    at = (eighths % n) / n
    if at == 0:
        return a
    re, im = a
    if at == 0.25:
        return (jnp.zeros_like(re) if im is None else -im), re
    if at == 0.75:
        return (jnp.zeros_like(re) if im is None else im), -re
    c, s = math.cos(2 * math.pi * at), math.sin(2 * math.pi * at)
    if im is None:
        return c * re, s * re
    return c * re - s * im, c * im + s * re


def real_dft(xs):
    n = len(xs)
    if n == 1:
        return [(xs[0], None)]
    if n == 2:
        return [(xs[0] + xs[1], None), (xs[0] - xs[1], None)]
    half = n // 2
    even, odd = real_dft(xs[0::2]), real_dft(xs[1::2])
    out = [None] * (half + 1)
    for k in range(half // 2 + 1):
        t = turn(odd[k], -k, n)
        out[k] = add(even[k], t)
        if half - k != k:
            out[half - k] = conj(add(even[k], t, -1.0))
    return out


def real_sum(zs, n):
    if n == 1:
        return [zs[0][0]]
    if n == 2:
        return [zs[0][0] + zs[1][0], zs[0][0] - zs[1][0]]
    half = n // 2
    even, odd = [], []
    for k in range(half // 2 + 1):
        if half - k == k:
            even.append(zs[k])
            odd.append(turn(zs[k], k, n))
        else:
            other = conj(zs[half - k])
            even.append(add(zs[k], other))
            odd.append(turn(add(zs[k], other, -1.0), k, n))
    even, odd = real_sum(even, half), real_sum(odd, half)
    return [(even, odd)[p % 2][p // 2] for p in range(n)]


def dx(q):
    width = q.shape[1]
    return 0.5 * (pltpu.roll(q, width - 1, 1) - pltpu.roll(q, 1, 1))


def dy(q):
    rows = q.shape[0]
    at = lax.broadcasted_iota(jnp.int32, q.shape, 0)
    above = jnp.where(at < rows - 1, pltpu.roll(q, rows - 1, 0), 0.0)
    below = jnp.where(at > 0, pltpu.roll(q, 1, 0), 0.0)
    return 0.5 * (above - below)


def model_step(state, rotation):
    h, u, w = state
    h = h - COURANT * (dx(u) + dy(w))
    return h, u - COURANT * dx(h) + rotation * w, w - COURANT * dy(h) - rotation * u


def adjoint_step(state, rotation):
    h, u, w = state
    a = h + COURANT * (dx(u) + dy(w))
    return a, u - rotation * w + COURANT * dx(a), w + rotation * u + COURANT * dy(a)


def slot_of(v, m, members):
    spare = min(SLOTS - members, members)
    if v < 2:
        return v * SLOTS + m
    return members + m if m < spare else SLOTS + members + m - spare


def kernel(
    groups, parts, spread,
    alpha_any, ens_any, std_any, control_any, spectrum_any, cell_any, step_any, innovation_any, weight_any,
    fwd_hi_any, fwd_lo_any, inv_hi_any, inv_lo_any, tw_c_any, tw_s_any, pick_any,
    corr_ref, grad_control_ref,
    alpha, ens, std, control, spectrum, cell, step, innovation, weight,
    fwd_hi, fwd_lo, inv_hi, inv_lo, tw_c, tw_s, pick,
    stage, ens_stage, adjoint, waves, fields, wide,
    snd_a, rcv_a, snd_e, rcv_e, snd_i, rcv_i, snd_h, rcv_h, snd_o, rcv_o, rcv_f, edge, rcv_edge,
    load_sem, a_send, a_recv, e_send, e_recv, i_send, i_recv, h_send, h_recv, o_send, o_recv, f_send, f_recv,
):
    group, part = lax.axis_index("grp"), lax.axis_index("sp")
    left, right = lax.rem(part + parts - 1, parts), lax.rem(part + 1, parts)
    members, rows, cols = alpha.shape
    tile_rows = control.shape[1]
    tile = pl.ds(pl.multiple_of(group * tile_rows, tile_rows), tile_rows)
    spare = min(SLOTS - members, members)
    shift = members - spare
    halves = cols // LANES
    residues = parts // 2 + 1
    started = []

    barrier = pltpu.get_barrier_semaphore()
    for j in range(groups):
        for i in range(parts):
            if i + j > 0:
                device = {"grp": lax.rem(group + j, groups), "sp": lax.rem(part + i, parts)}
                pl.semaphore_signal(barrier, inc=1, device_id=device)

    pairs = [
        (alpha_any, alpha), (ens_any, ens), (cell_any, cell), (step_any, step), (innovation_any, innovation),
        (weight_any, weight), (std_any, std), (control_any, control), (spectrum_any, spectrum),
        (fwd_hi_any, fwd_hi), (fwd_lo_any, fwd_lo), (inv_hi_any, inv_hi), (inv_lo_any, inv_lo),
        (tw_c_any, tw_c), (tw_s_any, tw_s), (pick_any, pick),
    ]
    loads = [pltpu.make_async_copy(a, b, load_sem.at[i]) for i, (a, b) in enumerate(pairs)]
    for load in loads:
        load.start()

    loads[0].wait()
    for m in range(members):
        stage[:, m, :] = alpha[m]
    for m in range(SLOTS - members):
        stage[:, members + m, :] = alpha[m] if m < spare else jnp.zeros((rows, cols), F32)
    snd_a[...] = stage[...].astype(BF16)
    def all_to_all(source, target, send, recv):
        copies = []
        for i in range(1, parts):
            to = lax.rem(part + i, parts)
            copies.append(pltpu.make_async_remote_copy(
                src_ref=source.at[to], dst_ref=target.at[part],
                send_sem=send.at[i], recv_sem=recv.at[i], device_id={"sp": to},
            ))
            copies[-1].start()
        target[part] = source[part]
        started.extend(copies)
        return copies

    def received(copies):
        for copy in copies:
            copy.wait_recv()

    pl.semaphore_wait(barrier, groups * parts - 1)

    alpha_copies = all_to_all(snd_a, rcv_a, a_send, a_recv)
    loads[1].wait()
    used = set()
    for v in range(3):
        for m in range(members):
            at = slot_of(v, m, members)
            used.add(at)
            ens_stage[:, at, :] = ens[m, v].astype(F32)
    for at in range(2 * SLOTS):
        if at not in used:
            ens_stage[:, at, :] = jnp.zeros((rows, cols), F32)
    snd_e[...] = ens_stage[...].astype(BF16)

    ens_copies = all_to_all(snd_e, rcv_e, e_send, e_recv)
    for load in loads[8:]:
        load.wait()
    count = spectrum.shape[1]
    inner = count // parts
    wave = lax.broadcasted_iota(jnp.int32, (SLOTS * (-(-residues // SLOTS)), count), 1)
    residue = lax.broadcasted_iota(jnp.int32, wave.shape, 0)
    weights = jnp.broadcast_to(spectrum[...], wave.shape)
    forward = jnp.where((lax.rem(wave, parts) == residue) & (residue < residues), weights, 0.0)
    mirrored = (lax.rem(wave + residue, parts) == 0) & (residue > 0) & (residue < residues - 1)
    backward = jnp.where(mirrored, weights, 0.0)
    k = lax.broadcasted_iota(jnp.int32, (count, 4 * inner), 0)
    j = lax.rem(lax.broadcasted_iota(jnp.int32, (count, 4 * inner), 1), 2 * inner)
    ahead, behind = k - parts * (j - inner), k - parts * (inner - 1 - j)
    ahead = jnp.where((ahead >= 0) & (ahead < parts), 1.0, 0.0).astype(BF16)
    behind = jnp.where((behind >= 0) & (behind < parts), 1.0, 0.0).astype(BF16)
    f_hi, f_lo = split2(forward)
    b_hi, b_lo = split2(backward)
    waves[...] = dot(f_hi, ahead) + dot(f_lo, ahead) + dot(b_hi, behind) + dot(b_lo, behind)

    def filtered(xs):
        pieces = [[x[:, h * LANES : (h + 1) * LANES] for x in xs] for h in range(halves)]
        spectra = [real_dft(piece) for piece in pieces]
        res, ims = [], []
        for k1 in range(residues):
            parts_re, parts_im = [], []
            for h in range(halves):
                c = tw_c[k1 : k1 + 1, h * LANES : (h + 1) * LANES]
                s = tw_s[k1 : k1 + 1, h * LANES : (h + 1) * LANES]
                re, im = spectra[h][k1]
                if k1 == 0:
                    parts_re.append(re)
                    parts_im.append(jnp.zeros_like(re))
                elif im is None:
                    parts_re.append(re * c)
                    parts_im.append(-re * s)
                else:
                    parts_re.append(re * c + im * s)
                    parts_im.append(im * c - re * s)
            res.append(jnp.concatenate(parts_re + parts_im, axis=1))
        y_hi, y_lo = split2(jnp.concatenate(res, axis=0))
        z = dot(y_hi, fwd_hi[...]) + dot(y_lo, fwd_hi[...]) + dot(y_hi, fwd_lo[...])
        z = jnp.concatenate(
            [z[k1 * SLOTS : (k1 + 1) * SLOTS] * waves[k1 : k1 + 1, :] for k1 in range(residues)], axis=0
        )
        z_hi, z_lo = split2(z)
        v = dot(z_hi, inv_hi[...]) + dot(z_lo, inv_hi[...]) + dot(z_hi, inv_lo[...])
        outs = []
        for h in range(halves):
            zs = []
            for k1 in range(residues):
                c = tw_c[k1 : k1 + 1, h * LANES : (h + 1) * LANES]
                s = tw_s[k1 : k1 + 1, h * LANES : (h + 1) * LANES]
                at = slice(k1 * SLOTS, (k1 + 1) * SLOTS)
                re = v[at, h * LANES : (h + 1) * LANES]
                im = v[at, cols + h * LANES : cols + (h + 1) * LANES]
                zs.append((re, im) if k1 == 0 else (re * c - im * s, im * c + re * s))
            outs.append(real_sum(zs, parts))
        return [jnp.concatenate([outs[h][p] for h in range(halves)], axis=1) for p in range(parts)]

    received(alpha_copies)
    localized = filtered([rcv_a[p].astype(F32) for p in range(parts)])
    for load in loads[2:8]:
        load.wait()
    pitch = -(-tile_rows // 8) * 8
    nx = cols * parts
    first = group * tile_rows
    row = jnp.zeros_like(cell)
    cells = cell[...]
    for r in range(1, tile_rows):
        row = row + jnp.where(cells >= (first + r) * nx, 1, 0)
    col = cells - (first + row) * nx - part * cols
    slot = step[...] * pitch + row
    observations = cells.shape[1]
    in_col = (lax.broadcasted_iota(jnp.int32, (cols, observations), 0) == col).astype(F32).astype(BF16)
    in_slot = lax.broadcasted_iota(jnp.int32, (3 * pitch, observations), 0) == slot
    obs_weight = weight[...]
    values = jnp.concatenate([
        jnp.where(in_slot, obs_weight, 0.0), jnp.where(in_slot, obs_weight * innovation[...], 0.0)
    ], axis=0)
    hi, lo = split2(values)
    summed = dot(hi, in_col, ((1,), (1,))) + dot(lo, in_col, ((1,), (1,)))
    for v in range(3):
        fields[v] = std[v] * control[v]
    for f in range(6):
        fields[3 + f] = summed[f * pitch : f * pitch + tile_rows]
    haloed = (0, 1, 2, 4, 5, 7, 8)
    lane = lax.broadcasted_iota(jnp.int32, (tile_rows, LANES), 1)
    packed = jnp.zeros((tile_rows, LANES), F32)
    for e, f in enumerate(haloed):
        ends = jnp.where(lane < LANES // 2, fields[f, :, :LANES], fields[f, :, cols - LANES :])
        window = (lane >= 2 * HALO * e) & (lane < 2 * HALO * (e + 1))
        packed = jnp.where(window, pltpu.roll(ends, (2 * HALO * e + HALO) % LANES, 1), packed)
    edge[...] = packed

    field_copies = []
    for j in range(groups):
        to = lax.rem(group + j, groups)
        plans = [(1, right, edge, rcv_edge.at[0, group]), (2, left, edge, rcv_edge.at[1, group])]
        if j > 0:
            plans.append((0, part, fields, rcv_f.at[group]))
        for kind, at, source, target in plans:
            field_copies.append(pltpu.make_async_remote_copy(
                src_ref=source, dst_ref=target,
                send_sem=f_send.at[kind, j], recv_sem=f_recv.at[kind, j], device_id={"grp": to, "sp": at},
            ))
            field_copies[-1].start()
    started.extend(field_copies)
    rcv_f[group] = fields[...]

    received(ens_copies)
    at_slot = lax.broadcasted_iota(jnp.int32, (SLOTS, cols), 0)
    firsts, seconds = [], []
    for p in range(parts):
        loc = localized[p].astype(BF16).astype(F32)
        moved = jnp.where(at_slot < members, loc, pltpu.roll(loc, shift, 0)) if shift else loc
        firsts.append(rcv_e[p, :SLOTS].astype(F32) * loc)
        seconds.append(rcv_e[p, SLOTS:].astype(F32) * moved)
    a_hi, a_lo = split2(jnp.concatenate(firsts, axis=0))
    b_hi, b_lo = split2(jnp.concatenate(seconds, axis=0))
    pick_a, pick_b = pick[:, : parts * SLOTS], pick[:, parts * SLOTS :]
    inc = spread * (dot(pick_a, a_hi) + dot(pick_a, a_lo) + dot(pick_b, b_hi) + dot(pick_b, b_lo))
    lane = lax.broadcasted_iota(jnp.int32, (parts, LANES), 1)
    packed = jnp.zeros((parts, LANES), F32)
    for v in range(3):
        field = inc[v * parts : (v + 1) * parts]
        for h in range(halves):
            snd_i[:, v * halves + h, :] = field[:, h * LANES : (h + 1) * LANES]
        after = pltpu.roll(field[:, :LANES], parts - 1, 0)
        before = pltpu.roll(field[:, cols - LANES :], 1, 0)
        ends = pltpu.roll(jnp.where(lane < LANES // 2, after, before), 2 * HALO * v + HALO, 1)
        packed = jnp.where((lane >= 2 * HALO * v) & (lane < 2 * HALO * (v + 1)), ends, packed)
    snd_i[:, 3 * halves, :] = packed
    copies = []
    for i in range(parts):
        for j in range(groups):
            if i + j > 0:
                g, to = lax.rem(group + j, groups), lax.rem(part + i, parts)
                copies.append(pltpu.make_async_remote_copy(
                    src_ref=snd_i.at[to], dst_ref=rcv_i.at[group, part],
                    send_sem=i_send.at[i, j], recv_sem=i_recv.at[i, j], device_id={"grp": g, "sp": to},
                ))
                copies[-1].start()
    rcv_i[group, part] = snd_i[part]
    started.extend(copies)

    received(field_copies)
    lane = lax.broadcasted_iota(jnp.int32, (tile_rows, LANES), 1)
    for g in range(groups):
        at = slice(g * tile_rows, (g + 1) * tile_rows)
        for f in range(9):
            wide[f, at, :cols] = rcv_f[g, f]
            if f in haloed:
                back = LANES - (2 * HALO * haloed.index(f) + HALO)
                before, after = (pltpu.roll(rcv_edge[side, g], back, 1) for side in (0, 1))
                wide[f, at, cols:] = jnp.where(lane < LANES // 2, after, before)
            else:
                wide[f, at, cols:] = jnp.zeros((tile_rows, LANES), F32)

    received(copies)

    def gathered(index):
        total = rcv_i[0, :, index, :]
        for g in range(1, groups):
            total = total + rcv_i[g, :, index, :]
        return total

    ends = gathered(3 * halves)
    state0 = []
    for v in range(3):
        pieces = [gathered(v * halves + h) for h in range(halves)]
        pieces.append(pltpu.roll(ends, LANES - (2 * HALO * v + HALO), 1))
        state0.append(jnp.concatenate(pieces, axis=1) + wide[v])
    row_at = lax.broadcasted_iota(jnp.int32, (rows, cols + LANES), 0).astype(F32)
    rotation = 0.1 + 0.2 * (row_at + 0.5) / rows
    state1 = model_step(state0, rotation)
    state2 = model_step(state1, rotation)
    forcing = [wide[3 + t] * s[0] - wide[6 + t] for t, s in enumerate((state0, state1, state2))]
    zero = jnp.zeros_like(rotation)
    h, u, w = adjoint_step((forcing[2], zero, zero), rotation)
    h, u, w = adjoint_step((h + forcing[1], u, w), rotation)
    for v, field in enumerate((h + forcing[0], u, w)):
        field = field[:, :cols]
        adjoint[v] = field
        half = field.astype(BF16).astype(F32)
        for h in range(halves):
            snd_h[:, v * halves + h, :] = half[:, h * LANES : (h + 1) * LANES]
    copies = all_to_all(snd_h, rcv_h, h_send, h_recv)
    for v in range(3):
        grad_control_ref[v] = control[v] + std[v] * adjoint[v, tile, :]
    received(copies)
    weighted = []
    for p in range(parts):
        halfs = []
        for v in range(3):
            pieces = [
                jnp.broadcast_to(rcv_h[p, v * halves + h : v * halves + h + 1, :], (SLOTS, LANES)) for h in range(halves)
            ]
            halfs.append(jnp.concatenate(pieces, axis=1))
        a = rcv_e[p, :SLOTS].astype(F32) * jnp.where(at_slot < members, halfs[0], halfs[2])
        b = rcv_e[p, SLOTS:].astype(F32) * jnp.where(at_slot < members, halfs[1], halfs[2])
        own = jnp.where(at_slot < spare, pltpu.roll(a, SLOTS - members, 0), 0.0)
        if shift:
            own = jnp.where((at_slot >= spare) & (at_slot < members), pltpu.roll(b, SLOTS - shift, 0), own)
        weighted.append(a + b + own)
    outs = filtered(weighted)
    for p in range(parts):
        snd_o[p] = outs[p].astype(BF16)
    received(all_to_all(snd_o, rcv_o, o_send, o_recv))
    stage[...] = rcv_o[...].astype(F32)
    for m in range(members):
        corr_ref[m] = alpha[m] + spread * stage[:, m, :]
    for copy in started:
        copy.wait_send()


def tables(parts, cols, waves, members):
    length = parts * cols
    inner = waves // parts
    residues = parts // 2 + 1
    twist = 2 * np.pi * np.outer(np.arange(residues), np.arange(cols)) / length
    quotient = np.arange(-inner, inner)
    phase = 2 * np.pi * (np.outer(np.arange(cols), quotient) % cols) / cols
    c, s = np.cos(phase), np.sin(phase)
    forward = np.block([[c, -s], [s, c]])
    pick = np.zeros((3 * parts, 2, parts, SLOTS), np.float32)
    for p in range(parts):
        for v in range(3):
            for m in range(members):
                at = slot_of(v, m, members)
                pick[v * parts + p, at // SLOTS, p, at % SLOTS] = 1.0
    return (
        *both(forward), *both(forward.T.copy()), np.cos(twist).astype(np.float32), np.sin(twist).astype(np.float32),
        pick.reshape(3 * parts, 2 * parts * SLOTS).astype(BF16),
    )


def per_device(alpha, ensemble, static_std, control, loc_spectrum, obs_cell, obs_step, innovation, obs_weight):
    members, rows, cols = alpha.shape
    groups, parts = lax.axis_size("grp"), lax.axis_size("sp")
    spread = 1.0 / math.sqrt(members * groups - 1)
    assert rows == parts and 3 * members <= 2 * SLOTS
    tile_rows = control.shape[1]
    residues = parts // 2 + 1
    inner = loc_spectrum.shape[0] // parts
    operands = (
        alpha, ensemble, static_std, control, loc_spectrum[None],
        obs_cell[None], obs_step[None], innovation[None], obs_weight[None],
        *tables(parts, cols, loc_spectrum.shape[0], members),
    )
    message = (8 * (-(-(3 * cols // LANES + 1) // 8)), LANES)
    vmem = pl.BlockSpec(memory_space=pltpu.VMEM)
    dma = pltpu.SemaphoreType.DMA
    corr, grad_control = pl.pallas_call(
        functools.partial(kernel, groups, parts, spread),
        out_shape=(
            jax.ShapeDtypeStruct(alpha.shape, F32),
            jax.ShapeDtypeStruct(control.shape, F32),
        ),
        in_specs=[HBM] * len(operands),
        out_specs=(vmem, vmem),
        scratch_shapes=[
            *[pltpu.VMEM(t.shape, t.dtype) for t in operands],
            pltpu.VMEM((rows, SLOTS, cols), F32),
            pltpu.VMEM((rows, 2 * SLOTS, cols), F32),
            pltpu.VMEM((3, rows, cols), F32),
            pltpu.VMEM((SLOTS * (-(-residues // SLOTS)), 4 * inner), F32),
            pltpu.VMEM((9, tile_rows, cols), F32),
            pltpu.VMEM((9, rows, cols + LANES), F32),
            pltpu.VMEM((parts, SLOTS, cols), BF16), pltpu.VMEM((parts, SLOTS, cols), BF16),
            pltpu.VMEM((parts, 2 * SLOTS, cols), BF16), pltpu.VMEM((parts, 2 * SLOTS, cols), BF16),
            pltpu.VMEM((parts, *message), F32), pltpu.VMEM((groups, parts, *message), F32),
            pltpu.VMEM((parts, *message), F32), pltpu.VMEM((parts, *message), F32),
            pltpu.VMEM((parts, SLOTS, cols), BF16), pltpu.VMEM((parts, SLOTS, cols), BF16),
            pltpu.VMEM((groups, 9, tile_rows, cols), F32),
            pltpu.VMEM((tile_rows, LANES), F32), pltpu.VMEM((2, groups, tile_rows, LANES), F32),
            dma((len(operands),)),
            dma((parts,)), dma((parts,)), dma((parts,)), dma((parts,)),
            dma((parts, groups)), dma((parts, groups)),
            dma((parts,)), dma((parts,)), dma((parts,)), dma((parts,)),
            dma((3, groups)), dma((3, groups)),
        ],
        compiler_params=pltpu.CompilerParams(collective_id=0, has_side_effects=True, vmem_limit_bytes=66700000),
    )(*operands)
    return corr, grad_control


def solution(mesh):
    flat = P(("grp", "sp"))
    tile = P(None, "grp", "sp")
    return jax.shard_map(
        per_device,
        mesh=mesh,
        in_specs=(P("grp", None, "sp"), P("grp", None, None, "sp"), tile, tile, P(), flat, flat, flat, flat),
        out_specs=(P("grp", None, "sp"), tile),
        check_vma=False,
    )
```

```python
import functools
import math

import jax
import jax.numpy as jnp
import numpy as np
from jax import lax
from jax.experimental import pallas as pl
from jax.experimental.pallas import tpu as pltpu
from jax.sharding import PartitionSpec as P

COURANT = 0.4
LANES = 128
HALO = 8
SLOTS = 16
BF16, F32 = jnp.bfloat16, jnp.float32
HBM = pl.BlockSpec(memory_space=pltpu.HBM)


def dot(a, b, contract=((1,), (0,))):
    return lax.dot_general(a, b, (contract, ((), ())), preferred_element_type=F32)


def split2(x):
    hi = x.astype(BF16)
    return hi, (x - hi.astype(F32)).astype(BF16)


def both(table):
    table = np.asarray(table, np.float32)
    hi = table.astype(BF16)
    return hi, (table - hi.astype(np.float32)).astype(BF16)


def add(a, b, sign=1.0):
    re = a[0] + b[0] if sign > 0 else a[0] - b[0]
    if b[1] is None:
        return re, a[1]
    if a[1] is None:
        return re, b[1] if sign > 0 else -b[1]
    return re, a[1] + b[1] if sign > 0 else a[1] - b[1]


def conj(a):
    return a[0], None if a[1] is None else -a[1]


def turn(a, eighths, n):
    at = (eighths % n) / n
    if at == 0:
        return a
    re, im = a
    if at == 0.25:
        return (jnp.zeros_like(re) if im is None else -im), re
    if at == 0.75:
        return (jnp.zeros_like(re) if im is None else im), -re
    c, s = math.cos(2 * math.pi * at), math.sin(2 * math.pi * at)
    if im is None:
        return c * re, s * re
    return c * re - s * im, c * im + s * re


def real_dft(xs):
    n = len(xs)
    if n == 1:
        return [(xs[0], None)]
    if n == 2:
        return [(xs[0] + xs[1], None), (xs[0] - xs[1], None)]
    half = n // 2
    even, odd = real_dft(xs[0::2]), real_dft(xs[1::2])
    out = [None] * (half + 1)
    for k in range(half // 2 + 1):
        t = turn(odd[k], -k, n)
        out[k] = add(even[k], t)
        if half - k != k:
            out[half - k] = conj(add(even[k], t, -1.0))
    return out


def real_sum(zs, n):
    if n == 1:
        return [zs[0][0]]
    if n == 2:
        return [zs[0][0] + zs[1][0], zs[0][0] - zs[1][0]]
    half = n // 2
    even, odd = [], []
    for k in range(half // 2 + 1):
        if half - k == k:
            even.append(zs[k])
            odd.append(turn(zs[k], k, n))
        else:
            other = conj(zs[half - k])
            even.append(add(zs[k], other))
            odd.append(turn(add(zs[k], other, -1.0), k, n))
    even, odd = real_sum(even, half), real_sum(odd, half)
    return [(even, odd)[p % 2][p // 2] for p in range(n)]


def dx(q):
    width = q.shape[1]
    return 0.5 * (pltpu.roll(q, width - 1, 1) - pltpu.roll(q, 1, 1))


def dy(q):
    rows = q.shape[0]
    at = lax.broadcasted_iota(jnp.int32, q.shape, 0)
    above = jnp.where(at < rows - 1, pltpu.roll(q, rows - 1, 0), 0.0)
    below = jnp.where(at > 0, pltpu.roll(q, 1, 0), 0.0)
    return 0.5 * (above - below)


def model_step(state, rotation):
    h, u, w = state
    h = h - COURANT * (dx(u) + dy(w))
    return h, u - COURANT * dx(h) + rotation * w, w - COURANT * dy(h) - rotation * u


def adjoint_step(state, rotation):
    h, u, w = state
    a = h + COURANT * (dx(u) + dy(w))
    return a, u - rotation * w + COURANT * dx(a), w + rotation * u + COURANT * dy(a)


def slot_of(v, m, members):
    spare = min(SLOTS - members, members)
    if v < 2:
        return v * SLOTS + m
    return members + m if m < spare else SLOTS + members + m - spare


def kernel(
    groups, parts, spread,
    alpha_any, ens_any, std_any, control_any, spectrum_any, cell_any, step_any, innovation_any, weight_any,
    fwd_hi_any, fwd_lo_any, inv_hi_any, inv_lo_any, tw_c_any, tw_s_any, pick_any,
    corr_ref, grad_control_ref,
    alpha, ens, std, control, spectrum, cell, step, innovation, weight,
    fwd_hi, fwd_lo, inv_hi, inv_lo, tw_c, tw_s, pick,
    stage, ens_stage, adjoint, waves, fields, wide,
    snd_a, rcv_a, snd_e, rcv_e, message, snd_i, rcv_i, snd_h, rcv_h, snd_o, rcv_o, rcv_f, edge, rcv_edge,
    load_sem, a_send, a_recv, e_send, e_recv, i_send, i_recv, h_send, h_recv, o_send, o_recv, f_send, f_recv, whole,
):
    group, part = lax.axis_index("grp"), lax.axis_index("sp")
    left, right = lax.rem(part + parts - 1, parts), lax.rem(part + 1, parts)
    members, rows, cols = alpha.shape
    tile_rows = control.shape[1]
    tile = pl.ds(pl.multiple_of(group * tile_rows, tile_rows), tile_rows)
    spare = min(SLOTS - members, members)
    shift = members - spare
    halves = cols // LANES
    residues = parts // 2 + 1
    started = []

    barrier = pltpu.get_barrier_semaphore()
    for i in range(1, parts):
        pl.semaphore_signal(barrier, inc=1, device_id={"sp": lax.rem(part + i, parts)})
    for j in range(1, groups):
        pl.semaphore_signal(barrier, inc=1, device_id={"grp": lax.rem(group + j, groups)})

    pairs = [
        (alpha_any, alpha), (ens_any, ens), (cell_any, cell), (step_any, step), (innovation_any, innovation),
        (weight_any, weight), (std_any, std), (control_any, control), (spectrum_any, spectrum),
        (fwd_hi_any, fwd_hi), (fwd_lo_any, fwd_lo), (inv_hi_any, inv_hi), (inv_lo_any, inv_lo),
        (tw_c_any, tw_c), (tw_s_any, tw_s), (pick_any, pick),
    ]
    loads = [pltpu.make_async_copy(a, b, load_sem.at[i]) for i, (a, b) in enumerate(pairs)]
    for load in loads:
        load.start()

    loads[0].wait()
    if stage.shape[1] > halves * members:
        stage[:, halves * members :, :] = jnp.zeros((rows, stage.shape[1] - halves * members, LANES), F32)
    for m in range(members):
        for h in range(halves):
            stage[:, h * members + m, :] = alpha[m, :, h * LANES : (h + 1) * LANES]
    snd_a[...] = stage[...].astype(BF16)
    for load in loads[2:8]:
        load.wait()
    pitch = -(-tile_rows // 8) * 8
    nx = cols * parts
    first = group * tile_rows
    row = jnp.zeros_like(cell)
    cells = cell[...]
    for r in range(1, tile_rows):
        row = row + jnp.where(cells >= (first + r) * nx, 1, 0)
    col = cells - (first + row) * nx - part * cols
    slot = step[...] * pitch + row
    observations = cells.shape[1]
    in_col = (lax.broadcasted_iota(jnp.int32, (cols, observations), 0) == col).astype(F32).astype(BF16)
    in_slot = lax.broadcasted_iota(jnp.int32, (3 * pitch, observations), 0) == slot
    obs_weight = weight[...]
    values = jnp.concatenate([
        jnp.where(in_slot, obs_weight, 0.0), jnp.where(in_slot, obs_weight * innovation[...], 0.0)
    ], axis=0)
    hi, lo = split2(values)
    summed = dot(hi, in_col, ((1,), (1,))) + dot(lo, in_col, ((1,), (1,)))
    for v in range(3):
        fields[v] = std[v] * control[v]
    for f in range(6):
        fields[3 + f] = summed[f * pitch : f * pitch + tile_rows]
    haloed = (0, 1, 2, 4, 5, 7, 8)
    lane = lax.broadcasted_iota(jnp.int32, (tile_rows, LANES), 1)
    packed = jnp.zeros((tile_rows, LANES), F32)
    for e, f in enumerate(haloed):
        ends = jnp.where(lane < LANES // 2, fields[f, :, :LANES], fields[f, :, cols - LANES :])
        window = (lane >= 2 * HALO * e) & (lane < 2 * HALO * (e + 1))
        packed = jnp.where(window, pltpu.roll(ends, (2 * HALO * e + HALO) % LANES, 1), packed)
    edge[...] = packed

    def all_to_all(source, target, send, recv):
        copies = []
        for i in range(1, parts):
            to = lax.rem(part + i, parts)
            copies.append(pltpu.make_async_remote_copy(
                src_ref=source.at[to], dst_ref=target.at[part],
                send_sem=send.at[i], recv_sem=recv.at[i], device_id={"sp": to},
            ))
            copies[-1].start()
        target[part] = source[part]
        started.extend(copies)
        return copies

    def received(copies):
        for copy in copies:
            copy.wait_recv()

    pl.semaphore_wait(barrier, parts + groups - 2)
    for j in range(1, groups):
        pl.semaphore_signal(whole, inc=1, device_id={"grp": lax.rem(group + j, groups)})

    alpha_copies = all_to_all(snd_a, rcv_a, a_send, a_recv)
    loads[1].wait()
    used = set()
    for v in range(3):
        for m in range(members):
            at = slot_of(v, m, members)
            used.add(at)
            ens_stage[:, at, :] = ens[m, v].astype(F32)
    for at in range(2 * SLOTS):
        if at not in used:
            ens_stage[:, at, :] = jnp.zeros((rows, cols), F32)
    snd_e[...] = ens_stage[...].astype(BF16)

    ens_copies = all_to_all(snd_e, rcv_e, e_send, e_recv)
    if groups > 1:
        pl.semaphore_wait(whole, groups - 1)
    field_copies = []
    for j in range(groups):
        to = lax.rem(group + j, groups)
        plans = [(1, right, edge, rcv_edge.at[0, group]), (2, left, edge, rcv_edge.at[1, group])]
        if j > 0:
            plans.append((0, part, fields, rcv_f.at[group]))
        for kind, at, source, target in plans:
            field_copies.append(pltpu.make_async_remote_copy(
                src_ref=source, dst_ref=target,
                send_sem=f_send.at[kind, j], recv_sem=f_recv.at[kind, j], device_id={"grp": to, "sp": at},
            ))
            field_copies[-1].start()
    started.extend(field_copies)
    rcv_f[group] = fields[...]

    for load in loads[8:]:
        load.wait()
    count = spectrum.shape[1]
    inner = count // parts
    wave = lax.broadcasted_iota(jnp.int32, (SLOTS * (-(-residues // SLOTS)), count), 1)
    residue = lax.broadcasted_iota(jnp.int32, wave.shape, 0)
    weights = jnp.broadcast_to(spectrum[...], wave.shape)
    forward = jnp.where((lax.rem(wave, parts) == residue) & (residue < residues), weights, 0.0)
    mirrored = (lax.rem(wave + residue, parts) == 0) & (residue > 0) & (residue < residues - 1)
    backward = jnp.where(mirrored, weights, 0.0)
    k = lax.broadcasted_iota(jnp.int32, (count, 4 * inner), 0)
    j = lax.rem(lax.broadcasted_iota(jnp.int32, (count, 4 * inner), 1), 2 * inner)
    ahead, behind = k - parts * (j - inner), k - parts * (inner - 1 - j)
    ahead = jnp.where((ahead >= 0) & (ahead < parts), 1.0, 0.0).astype(BF16)
    behind = jnp.where((behind >= 0) & (behind < parts), 1.0, 0.0).astype(BF16)
    f_hi, f_lo = split2(forward)
    b_hi, b_lo = split2(backward)
    waves[...] = dot(f_hi, ahead) + dot(f_lo, ahead) + dot(b_hi, behind) + dot(b_lo, behind)

    def filtered(xs):
        pieces = xs
        spectra = [real_dft(piece) for piece in pieces]
        res, ims = [], []
        for k1 in range(residues):
            parts_re, parts_im = [], []
            for h in range(halves):
                c = tw_c[k1 : k1 + 1, h * LANES : (h + 1) * LANES]
                s = tw_s[k1 : k1 + 1, h * LANES : (h + 1) * LANES]
                re, im = spectra[h][k1]
                if k1 == 0:
                    parts_re.append(re)
                    parts_im.append(jnp.zeros_like(re))
                elif im is None:
                    parts_re.append(re * c)
                    parts_im.append(-re * s)
                else:
                    parts_re.append(re * c + im * s)
                    parts_im.append(im * c - re * s)
            res.append(jnp.concatenate(parts_re + parts_im, axis=1))
        y_hi, y_lo = split2(jnp.concatenate(res, axis=0))
        z = dot(y_hi, fwd_hi[...]) + dot(y_lo, fwd_hi[...]) + dot(y_hi, fwd_lo[...])
        z = jnp.concatenate(
            [z[k1 * SLOTS : (k1 + 1) * SLOTS] * waves[k1 : k1 + 1, :] for k1 in range(residues)], axis=0
        )
        z_hi, z_lo = split2(z)
        v = dot(z_hi, inv_hi[...]) + dot(z_lo, inv_hi[...]) + dot(z_hi, inv_lo[...])
        outs = []
        for h in range(halves):
            zs = []
            for k1 in range(residues):
                c = tw_c[k1 : k1 + 1, h * LANES : (h + 1) * LANES]
                s = tw_s[k1 : k1 + 1, h * LANES : (h + 1) * LANES]
                at = slice(k1 * SLOTS, (k1 + 1) * SLOTS)
                re = v[at, h * LANES : (h + 1) * LANES]
                im = v[at, cols + h * LANES : cols + (h + 1) * LANES]
                zs.append((re, im) if k1 == 0 else (re * c - im * s, im * c + re * s))
            outs.append(real_sum(zs, parts))
        return outs

    received(alpha_copies)
    came = [[None] * parts for _ in range(halves)]
    for p in range(parts):
        x = rcv_a[p].astype(F32)
        for h in range(halves):
            came[h][p] = (x if h == 0 else pltpu.roll(x, x.shape[0] - h * members, 0))[:SLOTS]
    localized = filtered(came)
    received(ens_copies)
    at_slot = lax.broadcasted_iota(jnp.int32, (SLOTS, cols), 0)
    firsts, seconds = [], []
    for p in range(parts):
        loc = jnp.concatenate([localized[h][p] for h in range(halves)], axis=1).astype(BF16).astype(F32)
        moved = jnp.where(at_slot < members, loc, pltpu.roll(loc, shift, 0)) if shift else loc
        again = jnp.where(at_slot < members, loc, pltpu.roll(loc, members, 0))
        firsts.append(rcv_e[p, :SLOTS].astype(F32) * again)
        seconds.append(rcv_e[p, SLOTS:].astype(F32) * moved)
    a_hi, a_lo = split2(jnp.concatenate(firsts, axis=0))
    b_hi, b_lo = split2(jnp.concatenate(seconds, axis=0))
    pick_a, pick_b = pick[:, : parts * SLOTS], pick[:, parts * SLOTS :]
    inc = spread * (dot(pick_a, a_hi) + dot(pick_a, a_lo) + dot(pick_b, b_hi) + dot(pick_b, b_lo))
    lane = lax.broadcasted_iota(jnp.int32, (parts, LANES), 1)
    packed = jnp.zeros((parts, LANES), F32)
    for v in range(3):
        field = inc[v * parts : (v + 1) * parts]
        for h in range(halves):
            message[:, v * halves + h, :] = field[:, h * LANES : (h + 1) * LANES]
        after = pltpu.roll(field[:, :LANES], parts - 1, 0)
        before = pltpu.roll(field[:, cols - LANES :], 1, 0)
        ends = pltpu.roll(jnp.where(lane < LANES // 2, after, before), 2 * HALO * v + HALO, 1)
        packed = jnp.where((lane >= 2 * HALO * v) & (lane < 2 * HALO * (v + 1)), ends, packed)
    message[:, 3 * halves, :] = packed
    snd_i[...] = message[...].astype(BF16)
    copies = []
    for i in range(parts):
        for j in range(groups):
            if i + j > 0:
                g, to = lax.rem(group + j, groups), lax.rem(part + i, parts)
                copies.append(pltpu.make_async_remote_copy(
                    src_ref=snd_i.at[to], dst_ref=rcv_i.at[group, part],
                    send_sem=i_send.at[i, j], recv_sem=i_recv.at[i, j], device_id={"grp": g, "sp": to},
                ))
                copies[-1].start()
    rcv_i[group, part] = snd_i[part]
    started.extend(copies)

    received(field_copies)
    lane = lax.broadcasted_iota(jnp.int32, (tile_rows, LANES), 1)
    for g in range(groups):
        at = slice(g * tile_rows, (g + 1) * tile_rows)
        for f in range(9):
            wide[f, at, :cols] = rcv_f[g, f]
            if f in haloed:
                back = LANES - (2 * HALO * haloed.index(f) + HALO)
                before, after = (pltpu.roll(rcv_edge[side, g], back, 1) for side in (0, 1))
                wide[f, at, cols:] = jnp.where(lane < LANES // 2, after, before)
            else:
                wide[f, at, cols:] = jnp.zeros((tile_rows, LANES), F32)

    received(copies)

    total = rcv_i[0].astype(F32)
    for g in range(1, groups):
        total = total + rcv_i[g].astype(F32)
    message[...] = total

    def gathered(index):
        return message[:, index, :]

    ends = gathered(3 * halves)
    state0 = []
    for v in range(3):
        pieces = [gathered(v * halves + h) for h in range(halves)]
        pieces.append(pltpu.roll(ends, LANES - (2 * HALO * v + HALO), 1))
        state0.append(jnp.concatenate(pieces, axis=1) + wide[v])
    row_at = lax.broadcasted_iota(jnp.int32, (rows, cols + LANES), 0).astype(F32)
    rotation = 0.1 + 0.2 * (row_at + 0.5) / rows
    state1 = model_step(state0, rotation)
    state2 = model_step(state1, rotation)
    forcing = [wide[3 + t] * s[0] - wide[6 + t] for t, s in enumerate((state0, state1, state2))]
    zero = jnp.zeros_like(rotation)
    h, u, w = adjoint_step((forcing[2], zero, zero), rotation)
    h, u, w = adjoint_step((h + forcing[1], u, w), rotation)
    for v, field in enumerate((h + forcing[0], u, w)):
        field = field[:, :cols]
        adjoint[v] = field
        half = field.astype(BF16).astype(F32)
        for h in range(halves):
            message[:, v * halves + h, :] = half[:, h * LANES : (h + 1) * LANES]
    snd_h[...] = message[...].astype(BF16)
    copies = all_to_all(snd_h, rcv_h, h_send, h_recv)
    for v in range(3):
        grad_control_ref[v] = control[v] + std[v] * adjoint[v, tile, :]
    received(copies)
    weighted = []
    for p in range(parts):
        came_h = rcv_h[p].astype(F32)
        halfs = []
        for v in range(3):
            pieces = [
                jnp.broadcast_to(came_h[v * halves + h : v * halves + h + 1], (SLOTS, LANES)) for h in range(halves)
            ]
            halfs.append(jnp.concatenate(pieces, axis=1))
        a = rcv_e[p, :SLOTS].astype(F32) * jnp.where(at_slot < members, halfs[0], halfs[2])
        b = rcv_e[p, SLOTS:].astype(F32) * jnp.where(at_slot < members, halfs[1], halfs[2])
        own = jnp.where(at_slot < spare, pltpu.roll(a, SLOTS - members, 0), 0.0)
        if shift:
            own = jnp.where((at_slot >= spare) & (at_slot < members), pltpu.roll(b, SLOTS - shift, 0), own)
        weighted.append(a + b + own)
    outs = filtered([[x[:, h * LANES : (h + 1) * LANES] for x in weighted] for h in range(halves)])
    for p in range(parts):
        for h in range(halves):
            stage[p, h * members : (h + 1) * members, :] = outs[h][p][:members]
        snd_o[p] = stage[p].astype(BF16)
    received(all_to_all(snd_o, rcv_o, o_send, o_recv))
    stage[...] = rcv_o[...].astype(F32)
    for m in range(members):
        for h in range(halves):
            at = slice(h * LANES, (h + 1) * LANES)
            corr_ref[m, :, at] = alpha[m, :, at] + spread * stage[:, h * members + m, :]
    for copy in started:
        copy.wait_send()


def finish(corr_ref, grad_control_ref, corr_out, grad_control_out, sem):
    copies = [
        pltpu.make_async_copy(corr_ref, corr_out, sem.at[0]),
        pltpu.make_async_copy(grad_control_ref, grad_control_out, sem.at[1]),
    ]
    for copy in copies:
        copy.start()
    for copy in copies:
        copy.wait()


def tables(parts, cols, waves, members):
    length = parts * cols
    inner = waves // parts
    residues = parts // 2 + 1
    twist = 2 * np.pi * np.outer(np.arange(residues), np.arange(cols)) / length
    quotient = np.arange(-inner, inner)
    phase = 2 * np.pi * (np.outer(np.arange(cols), quotient) % cols) / cols
    c, s = np.cos(phase), np.sin(phase)
    forward = np.block([[c, -s], [s, c]])
    pick = np.zeros((3 * parts, 2, parts, SLOTS), np.float32)
    for p in range(parts):
        for v in range(3):
            for m in range(members):
                at = slot_of(v, m, members)
                pick[v * parts + p, at // SLOTS, p, at % SLOTS] = 1.0
    return (
        *both(forward), *both(forward.T.copy()), np.cos(twist).astype(np.float32), np.sin(twist).astype(np.float32),
        pick.reshape(3 * parts, 2 * parts * SLOTS).astype(BF16),
    )


def per_device(alpha, ensemble, static_std, control, loc_spectrum, obs_cell, obs_step, innovation, obs_weight):
    members, rows, cols = alpha.shape
    groups, parts = lax.axis_size("grp"), lax.axis_size("sp")
    spread = 1.0 / math.sqrt(members * groups - 1)
    assert rows == parts and 3 * members <= 2 * SLOTS
    tile_rows = control.shape[1]
    residues = parts // 2 + 1
    inner = loc_spectrum.shape[0] // parts
    operands = (
        alpha, ensemble, static_std, control, loc_spectrum[None],
        obs_cell[None], obs_step[None], innovation[None], obs_weight[None],
        *tables(parts, cols, loc_spectrum.shape[0], members),
    )
    packed = (8 * (-(-max(cols // LANES * members, SLOTS) // 8)), LANES)
    message = (8 * (-(-(3 * cols // LANES + 1) // 8)), LANES)
    vmem = pl.BlockSpec(memory_space=pltpu.VMEM)
    dma = pltpu.SemaphoreType.DMA
    corr, grad_control = pl.pallas_call(
        functools.partial(kernel, groups, parts, spread),
        out_shape=(
            pltpu.VMEM(alpha.shape, F32),
            pltpu.VMEM(control.shape, F32),
        ),
        in_specs=[HBM] * len(operands),
        out_specs=(vmem, vmem),
        scratch_shapes=[
            *[pltpu.VMEM(t.shape, t.dtype) for t in operands],
            pltpu.VMEM((rows, *packed), F32),
            pltpu.VMEM((rows, 2 * SLOTS, cols), F32),
            pltpu.VMEM((3, rows, cols), F32),
            pltpu.VMEM((SLOTS * (-(-residues // SLOTS)), 4 * inner), F32),
            pltpu.VMEM((9, tile_rows, cols), F32),
            pltpu.VMEM((9, rows, cols + LANES), F32),
            pltpu.VMEM((parts, *packed), BF16), pltpu.VMEM((parts, *packed), BF16),
            pltpu.VMEM((parts, 2 * SLOTS, cols), BF16), pltpu.VMEM((parts, 2 * SLOTS, cols), BF16),
            pltpu.VMEM((parts, *message), F32),
            pltpu.VMEM((parts, *message), BF16), pltpu.VMEM((groups, parts, *message), BF16),
            pltpu.VMEM((parts, *message), BF16), pltpu.VMEM((parts, *message), BF16),
            pltpu.VMEM((parts, *packed), BF16), pltpu.VMEM((parts, *packed), BF16),
            pltpu.VMEM((groups, 9, tile_rows, cols), F32),
            pltpu.VMEM((tile_rows, LANES), F32), pltpu.VMEM((2, groups, tile_rows, LANES), F32),
            dma((len(operands),)),
            dma((parts,)), dma((parts,)), dma((parts,)), dma((parts,)),
            dma((parts, groups)), dma((parts, groups)),
            dma((parts,)), dma((parts,)), dma((parts,)), dma((parts,)),
            dma((3, groups)), dma((3, groups)),
            pltpu.SemaphoreType.REGULAR,
        ],
        compiler_params=pltpu.CompilerParams(collective_id=0, has_side_effects=True, vmem_limit_bytes=63 << 20),
    )(*operands)
    return pl.pallas_call(
        finish,
        out_shape=(jax.ShapeDtypeStruct(alpha.shape, F32), jax.ShapeDtypeStruct(control.shape, F32)),
        in_specs=[vmem] * 2,
        out_specs=(HBM, HBM),
        scratch_shapes=[dma((2,))],
        compiler_params=pltpu.CompilerParams(vmem_limit_bytes=1 << 20),
    )(corr, grad_control)


def solution(mesh):
    flat = P(("grp", "sp"))
    tile = P(None, "grp", "sp")
    return jax.shard_map(
        per_device,
        mesh=mesh,
        in_specs=(P("grp", None, "sp"), P("grp", None, None, "sp"), tile, tile, P(), flat, flat, flat, flat),
        out_specs=(P("grp", None, "sp"), tile),
        check_vma=False,
    )
```

```python
import functools
import math

import jax
import jax.numpy as jnp
import numpy as np
from jax import lax
from jax.experimental import pallas as pl
from jax.experimental.pallas import tpu as pltpu
from jax.sharding import PartitionSpec as P

COURANT = 0.4
LANES = 128
HALO = 8
BATCHES = 4
BF16, F32 = jnp.bfloat16, jnp.float32
HBM = pl.BlockSpec(memory_space=pltpu.HBM)


def dot(a, b, contract=((1,), (0,))):
    return lax.dot_general(a, b, (contract, ((), ())), preferred_element_type=F32)


def split2(x):
    hi = x.astype(BF16)
    return hi, (x - hi.astype(F32)).astype(BF16)


def both(table):
    table = np.asarray(table, np.float32)
    hi = table.astype(BF16)
    return hi, (table - hi.astype(np.float32)).astype(BF16)


def add(a, b, sign=1.0):
    re = a[0] + b[0] if sign > 0 else a[0] - b[0]
    if b[1] is None:
        return re, a[1]
    if a[1] is None:
        return re, b[1] if sign > 0 else -b[1]
    return re, a[1] + b[1] if sign > 0 else a[1] - b[1]


def conj(a):
    return a[0], None if a[1] is None else -a[1]


def turn(a, eighths, n):
    at = (eighths % n) / n
    if at == 0:
        return a
    re, im = a
    if at == 0.25:
        return (jnp.zeros_like(re) if im is None else -im), re
    if at == 0.75:
        return (jnp.zeros_like(re) if im is None else im), -re
    c, s = math.cos(2 * math.pi * at), math.sin(2 * math.pi * at)
    if im is None:
        return c * re, s * re
    return c * re - s * im, c * im + s * re


def real_dft(xs):
    n = len(xs)
    if n == 1:
        return [(xs[0], None)]
    if n == 2:
        return [(xs[0] + xs[1], None), (xs[0] - xs[1], None)]
    half = n // 2
    even, odd = real_dft(xs[0::2]), real_dft(xs[1::2])
    out = [None] * (half + 1)
    for k in range(half // 2 + 1):
        t = turn(odd[k], -k, n)
        out[k] = add(even[k], t)
        if half - k != k:
            out[half - k] = conj(add(even[k], t, -1.0))
    return out


def real_sum(zs, n):
    if n == 1:
        return [zs[0][0]]
    if n == 2:
        return [zs[0][0] + zs[1][0], zs[0][0] - zs[1][0]]
    half = n // 2
    even, odd = [], []
    for k in range(half // 2 + 1):
        if half - k == k:
            even.append(zs[k])
            odd.append(turn(zs[k], k, n))
        else:
            other = conj(zs[half - k])
            even.append(add(zs[k], other))
            odd.append(turn(add(zs[k], other, -1.0), k, n))
    even, odd = real_sum(even, half), real_sum(odd, half)
    return [(even, odd)[p % 2][p // 2] for p in range(n)]


def dx(q):
    width = q.shape[1]
    return 0.5 * (pltpu.roll(q, width - 1, 1) - pltpu.roll(q, 1, 1))


def dy(q):
    rows = q.shape[0]
    at = lax.broadcasted_iota(jnp.int32, q.shape, 0)
    above = jnp.where(at < rows - 1, pltpu.roll(q, rows - 1, 0), 0.0)
    below = jnp.where(at > 0, pltpu.roll(q, 1, 0), 0.0)
    return 0.5 * (above - below)


def model_step(state, rotation):
    h, u, w = state
    h = h - COURANT * (dx(u) + dy(w))
    return h, u - COURANT * dx(h) + rotation * w, w - COURANT * dy(h) - rotation * u


def adjoint_step(state, rotation):
    h, u, w = state
    a = h + COURANT * (dx(u) + dy(w))
    return a, u - rotation * w + COURANT * dx(a), w + rotation * u + COURANT * dy(a)


def round8(n):
    return -(-n // 8) * 8


def layout(members, rows, parts):
    owners = parts // 2
    per = rows // owners
    items = per * members
    slots = round8(items)
    spare = slots - items
    return owners, per, items, slots, spare, 2 * slots + round8(items - 2 * spare)


def slot_of(v, item, items, slots, spare):
    if v < 2:
        return v * slots + item
    if item < spare:
        return items + item
    if item < 2 * spare:
        return slots + items + item - spare
    return 2 * slots + item - 2 * spare


def kernel(
    groups, parts, spread,
    alpha_any, ens_any, std_any, control_any, spectrum_any, cell_any, step_any, innovation_any, weight_any,
    fwd_hi_any, fwd_lo_any, inv_hi_any, inv_lo_any, tw_c_any, tw_s_any, pick_any,
    corr_ref, grad_control_ref,
    alpha, ens, std, control, spectrum, cell, step, innovation, weight,
    fwd_hi, fwd_lo, inv_hi, inv_lo, tw_c, tw_s, pick,
    stage, out_stage, ens_stage, loc_buf, adjoint, waves, fields, wide, message,
    snd_a, rcv_a, snd_e, rcv_e, snd_i, rcv_i, snd_h, rcv_h, snd_o, rcv_o, rcv_f, edge, rcv_edge,
    load_sem, a_send, a_recv, e_send, e_recv, i_send, i_recv, h_send, h_recv, o_send, o_recv, f_send, f_recv, whole,
):
    group, part = lax.axis_index("grp"), lax.axis_index("sp")
    left, right = lax.rem(part + parts - 1, parts), lax.rem(part + 1, parts)
    members, rows, cols = alpha.shape
    tile_rows = control.shape[1]
    tile = pl.ds(pl.multiple_of(group * tile_rows, tile_rows), tile_rows)
    owners, per, items, slots, spare, total_slots = layout(members, rows, parts)
    low = parts // 4
    mine = part - low
    owner = (part >= low) & (part < low + owners)
    halves = cols // LANES
    residues = parts // 2 + 1

    barrier = pltpu.get_barrier_semaphore()
    others = [(0, left), (0, right)] + [(j, at) for j in range(1, groups) for at in (part, left, right)]

    @pl.when(owner)
    def _():
        for i in range(1, parts):
            pl.semaphore_signal(barrier, inc=1, device_id={"sp": lax.rem(part + i, parts)})

    @pl.when(jnp.logical_not(owner))
    def _():
        for i in range(owners):
            pl.semaphore_signal(barrier, inc=1, device_id={"sp": low + lax.rem(part + i, owners)})

    for j, at in others:
        pl.semaphore_signal(barrier, inc=1, device_id={"grp": lax.rem(group + j, groups), "sp": at})

    pairs = [
        (alpha_any, alpha), (ens_any, ens), (cell_any, cell), (step_any, step), (innovation_any, innovation),
        (weight_any, weight), (std_any, std), (control_any, control), (spectrum_any, spectrum),
        (fwd_hi_any, fwd_hi), (fwd_lo_any, fwd_lo), (inv_hi_any, inv_hi), (inv_lo_any, inv_lo),
        (tw_c_any, tw_c), (tw_s_any, tw_s), (pick_any, pick),
    ]
    loads = [pltpu.make_async_copy(a, b, load_sem.at[i]) for i, (a, b) in enumerate(pairs)]
    for load in loads:
        load.start()

    loads[0].wait()
    filled = halves * items
    if stage.shape[1] > filled:
        stage[:, filled:, :] = jnp.zeros((owners, stage.shape[1] - filled, LANES), F32)
    for m in range(members):
        for j in range(per):
            for h in range(halves):
                stage[:, h * items + j * members + m, :] = (
                    alpha[m, j * owners : (j + 1) * owners, h * LANES : (h + 1) * LANES]
                )
    snd_a[...] = stage[...].astype(BF16)

    for load in loads[2:8]:
        load.wait()
    pitch = -(-tile_rows // 8) * 8
    nx = cols * parts
    first = group * tile_rows
    row = jnp.zeros_like(cell)
    cells = cell[...]
    for r in range(1, tile_rows):
        row = row + jnp.where(cells >= (first + r) * nx, 1, 0)
    col = cells - (first + row) * nx - part * cols
    slot = step[...] * pitch + row
    observations = cells.shape[1]
    in_col = (lax.broadcasted_iota(jnp.int32, (cols, observations), 0) == col).astype(F32).astype(BF16)
    in_slot = lax.broadcasted_iota(jnp.int32, (3 * pitch, observations), 0) == slot
    obs_weight = weight[...]
    values = jnp.concatenate([
        jnp.where(in_slot, obs_weight, 0.0), jnp.where(in_slot, obs_weight * innovation[...], 0.0)
    ], axis=0)
    hi, lo = split2(values)
    summed = dot(hi, in_col, ((1,), (1,))) + dot(lo, in_col, ((1,), (1,)))
    for v in range(3):
        fields[v] = std[v] * control[v]
    for f in range(6):
        fields[3 + f] = summed[f * pitch : f * pitch + tile_rows]
    haloed = (0, 1, 2, 4, 5, 7, 8)
    lane = lax.broadcasted_iota(jnp.int32, (tile_rows, LANES), 1)
    packed = jnp.zeros((tile_rows, LANES), F32)
    for e, f in enumerate(haloed):
        ends = jnp.where(lane < LANES // 2, fields[f, :, :LANES], fields[f, :, cols - LANES :])
        window = (lane >= 2 * HALO * e) & (lane < 2 * HALO * (e + 1))
        packed = jnp.where(window, pltpu.roll(ends, (2 * HALO * e + HALO) % LANES, 1), packed)
    edge[...] = packed

    @pl.when(owner)
    def _():
        pl.semaphore_wait(barrier, parts - 1 + len(others))
        for j in range(1, groups):
            pl.semaphore_signal(whole, inc=1, device_id={"grp": lax.rem(group + j, groups)})

    @pl.when(jnp.logical_not(owner))
    def _():
        pl.semaphore_wait(barrier, owners + len(others))

    class ToOwners:
        def __init__(self, source, target, send, recv):
            self.source, self.target, self.send, self.recv = source, target, send, recv

        def copy(self, i):
            at = lax.rem(part + i, owners)
            return low + at, pltpu.make_async_remote_copy(
                src_ref=self.source.at[at], dst_ref=self.target.at[part],
                send_sem=self.send.at[i], recv_sem=self.recv.at[part], device_id={"sp": low + at},
            )

        def start(self):
            for i in range(owners):
                to, copy = self.copy(i)
                pl.when(to != part)(copy.start)

        def take_own(self):
            self.target[part] = self.source[mine]

        def receive(self, i):
            at = lax.rem(part + parts - i, parts)
            pltpu.make_async_remote_copy(
                src_ref=self.source.at[0], dst_ref=self.target.at[at],
                send_sem=self.send.at[0], recv_sem=self.recv.at[at], device_id={"sp": left},
            ).wait_recv()

        def finish(self):
            for i in range(owners):
                to, copy = self.copy(i)
                pl.when(to != part)(copy.wait_send)

    alphas = ToOwners(snd_a, rcv_a, a_send, a_recv)
    enses = ToOwners(snd_e, rcv_e, e_send, e_recv)
    halfs = ToOwners(snd_h, rcv_h, h_send, h_recv)
    alphas.start()
    field_copies = []
    for j in range(groups):
        to = lax.rem(group + j, groups)
        plans = [(1, right, edge, rcv_edge.at[0, group]), (2, left, edge, rcv_edge.at[1, group])]
        if j > 0:
            plans.append((0, part, fields, rcv_f.at[group]))
        for kind, at, source, target in plans:
            field_copies.append(pltpu.make_async_remote_copy(
                src_ref=source, dst_ref=target,
                send_sem=f_send.at[kind, j], recv_sem=f_recv.at[kind, j], device_id={"grp": to, "sp": at},
            ))
            field_copies[-1].start()
    rcv_f[group] = fields[...]


    loads[1].wait()
    used = set()
    for v in range(3):
        for m in range(members):
            field = ens[m, v].astype(F32)
            for j in range(per):
                at = slot_of(v, j * members + m, items, slots, spare)
                used.add(at)
                ens_stage[:, at, :] = field[j * owners : (j + 1) * owners]
    for at in range(total_slots):
        if at not in used:
            ens_stage[:, at, :] = jnp.zeros((owners, cols), F32)
    snd_e[...] = ens_stage[...].astype(BF16)
    enses.start()

    for load in loads[8:]:
        load.wait()

    def filtered(xs):
        pieces = xs
        spectra = [real_dft(piece) for piece in pieces]
        res, ims = [], []
        for k1 in range(residues):
            parts_re, parts_im = [], []
            for h in range(halves):
                c = tw_c[k1 : k1 + 1, h * LANES : (h + 1) * LANES]
                s = tw_s[k1 : k1 + 1, h * LANES : (h + 1) * LANES]
                re, im = spectra[h][k1]
                if k1 == 0:
                    parts_re.append(re)
                    parts_im.append(jnp.zeros_like(re))
                elif im is None:
                    parts_re.append(re * c)
                    parts_im.append(-re * s)
                else:
                    parts_re.append(re * c + im * s)
                    parts_im.append(im * c - re * s)
            res.append(jnp.concatenate(parts_re + parts_im, axis=1))
        y_hi, y_lo = split2(jnp.concatenate(res, axis=0))
        z = dot(y_hi, fwd_hi[...]) + dot(y_lo, fwd_hi[...]) + dot(y_hi, fwd_lo[...])
        z = jnp.concatenate(
            [z[k1 * slots : (k1 + 1) * slots] * waves[k1 : k1 + 1, :] for k1 in range(residues)], axis=0
        )
        z_hi, z_lo = split2(z)
        v = dot(z_hi, inv_hi[...]) + dot(z_lo, inv_hi[...]) + dot(z_hi, inv_lo[...])
        outs = []
        for h in range(halves):
            zs = []
            for k1 in range(residues):
                c = tw_c[k1 : k1 + 1, h * LANES : (h + 1) * LANES]
                s = tw_s[k1 : k1 + 1, h * LANES : (h + 1) * LANES]
                at = slice(k1 * slots, (k1 + 1) * slots)
                re = v[at, h * LANES : (h + 1) * LANES]
                im = v[at, cols + h * LANES : cols + (h + 1) * LANES]
                zs.append((re, im) if k1 == 0 else (re * c - im * s, im * c + re * s))
            outs.append(real_sum(zs, parts))
        return outs

    at_slot = lax.broadcasted_iota(jnp.int32, (slots, cols), 0)

    def inc_copy(i, j):
        return pltpu.make_async_remote_copy(
            src_ref=snd_i.at[i], dst_ref=rcv_i.at[group, mine],
            send_sem=i_send.at[i, j], recv_sem=i_recv.at[group, mine],
            device_id={"grp": lax.rem(group + j, groups), "sp": lax.rem(part + parts - i, parts)},
        )

    def out_copy(i):
        to = lax.rem(part + i, parts)
        return pltpu.make_async_remote_copy(
            src_ref=snd_o.at[to], dst_ref=rcv_o.at[mine],
            send_sem=o_send.at[i], recv_sem=o_recv.at[mine], device_id={"sp": to},
        )

    @pl.when(owner)
    def _():
        count = spectrum.shape[1]
        inner = count // parts
        wave = lax.broadcasted_iota(jnp.int32, (waves.shape[0], count), 1)
        residue = lax.broadcasted_iota(jnp.int32, wave.shape, 0)
        weights = jnp.broadcast_to(spectrum[...], wave.shape)
        forward = jnp.where((lax.rem(wave, parts) == residue) & (residue < residues), weights, 0.0)
        mirrored = (lax.rem(wave + residue, parts) == 0) & (residue > 0) & (residue < residues - 1)
        backward = jnp.where(mirrored, weights, 0.0)
        k = lax.broadcasted_iota(jnp.int32, (count, 4 * inner), 0)
        j = lax.rem(lax.broadcasted_iota(jnp.int32, (count, 4 * inner), 1), 2 * inner)
        ahead, behind = k - parts * (j - inner), k - parts * (inner - 1 - j)
        ahead = jnp.where((ahead >= 0) & (ahead < parts), 1.0, 0.0).astype(BF16)
        behind = jnp.where((behind >= 0) & (behind < parts), 1.0, 0.0).astype(BF16)
        f_hi, f_lo = split2(forward)
        b_hi, b_lo = split2(backward)
        waves[...] = dot(f_hi, ahead) + dot(f_lo, ahead) + dot(b_hi, behind) + dot(b_lo, behind)

        alphas.take_own()
        enses.take_own()
        for i in range(1, parts):
            alphas.receive(i)
        came = [[None] * parts for _ in range(halves)]
        for p in range(parts):
            x = rcv_a[p].astype(F32)
            for h in range(halves):
                came[h][p] = (x if h == 0 else pltpu.roll(x, x.shape[0] - h * items, 0))[:slots]
        localized = filtered(came)
        for p in range(parts):
            loc = jnp.concatenate([localized[h][p] for h in range(halves)], axis=1)
            loc_buf[p] = loc.astype(BF16).astype(F32)
        lane = lax.broadcasted_iota(jnp.int32, (8, LANES), 1)
        at_row = lax.broadcasted_iota(jnp.int32, (8, LANES), 0)
        tiles = [None] * parts

        def increments(p):
            loc = loc_buf[p]
            a = rcv_e[p, :slots].astype(F32) * jnp.where(at_slot < items, loc, pltpu.roll(loc, items, 0))
            b = rcv_e[p, slots : 2 * slots].astype(F32) * jnp.where(at_slot < items, loc, pltpu.roll(loc, items - spare, 0))
            rest = total_slots - 2 * slots
            c = rcv_e[p, 2 * slots :].astype(F32) * loc[2 * spare : 2 * spare + rest]
            hi, lo = split2(jnp.concatenate([a, b, c], axis=0))
            return spread * dot(pick[...], jnp.concatenate([hi, lo], axis=0))

        def put_increments(i):
            after, before = tiles[i - 1][:, :LANES], tiles[(i + 1) % parts][:, cols - LANES :]
            ends = jnp.where(lane < LANES // 2, after, before)
            pieces = [tiles[i][:, h * LANES : (h + 1) * LANES] for h in range(halves)]
            for v in range(3):
                window = (lane >= 2 * HALO * v) & (lane < 2 * HALO * (v + 1)) & (at_row >= 3 * per)
                moved = pltpu.roll(ends, 2 * HALO * v + HALO, 1)
                if 3 * per - per * v:
                    moved = pltpu.roll(moved, 3 * per - per * v, 0)
                pieces[0] = jnp.where(window, moved, pieces[0])
            snd_i[i] = jnp.concatenate(pieces, axis=0).astype(BF16)

        pl.semaphore_wait(whole, groups - 1)
        batch = owners // BATCHES
        for first_of in range(0, owners, batch):
            blocks = [i for k in range(first_of, first_of + batch) for i in (k, k + owners)]
            for i in blocks:
                if i > 0:
                    enses.receive(i)
            for i in blocks:
                tiles[i] = increments(lax.rem(part + parts - i, parts))
            ready = [i for k in range(first_of - 1, first_of + batch - 1) if k > 0 for i in (k, k + owners)]
            if first_of + batch == owners:
                ready += [owners - 1, parts - 1, 0, owners]
            for i in ready:
                put_increments(i)
            for i in ready:
                for j in range(groups):
                    if i + j > 0:
                        inc_copy(i, j).start()
        rcv_i[group, mine] = snd_i[0]

    for copy in field_copies:
        copy.wait_recv()
    lane = lax.broadcasted_iota(jnp.int32, (tile_rows, LANES), 1)
    for g in range(groups):
        at = slice(g * tile_rows, (g + 1) * tile_rows)
        for f in range(9):
            wide[f, at, :cols] = rcv_f[g, f]
            if f in haloed:
                back = LANES - (2 * HALO * haloed.index(f) + HALO)
                before, after = (pltpu.roll(rcv_edge[side, g], back, 1) for side in (0, 1))
                wide[f, at, cols:] = jnp.where(lane < LANES // 2, after, before)
            else:
                wide[f, at, cols:] = jnp.zeros((tile_rows, LANES), F32)

    for j in range(groups):
        for k in range(owners):
            g, at = lax.rem(group + j, groups), lax.rem(part + k, owners)
            arrival = pltpu.make_async_remote_copy(
                src_ref=snd_i.at[0], dst_ref=rcv_i.at[g, at],
                send_sem=i_send.at[0, 0], recv_sem=i_recv.at[g, at], device_id={"sp": left},
            )
            if j == 0:
                pl.when(at != mine)(arrival.wait_recv)
            else:
                arrival.wait_recv()
    total = rcv_i[0].astype(F32)
    for g in range(1, groups):
        total = total + rcv_i[g].astype(F32)
    message[...] = total

    def gathered(index):
        return jnp.concatenate([message[:, index + j, :] for j in range(per)], axis=0)

    ends = gathered(3 * per)
    state0 = []
    for v in range(3):
        pieces = [gathered(8 * h + per * v) for h in range(halves)]
        pieces.append(pltpu.roll(ends, LANES - (2 * HALO * v + HALO), 1))
        state0.append(jnp.concatenate(pieces, axis=1) + wide[v])
    row_at = lax.broadcasted_iota(jnp.int32, (rows, cols + LANES), 0).astype(F32)
    rotation = 0.1 + 0.2 * (row_at + 0.5) / rows
    state1 = model_step(state0, rotation)
    state2 = model_step(state1, rotation)
    forcing = [wide[3 + t] * s[0] - wide[6 + t] for t, s in enumerate((state0, state1, state2))]
    zero = jnp.zeros_like(rotation)
    h, u, w = adjoint_step((forcing[2], zero, zero), rotation)
    h, u, w = adjoint_step((h + forcing[1], u, w), rotation)
    for v, field in enumerate((h + forcing[0], u, w)):
        field = field[:, :cols]
        adjoint[v] = field
        half = field.astype(BF16).astype(F32)
        for h in range(halves):
            for j in range(per):
                message[:, 8 * h + per * v + j, :] = half[j * owners : (j + 1) * owners, h * LANES : (h + 1) * LANES]
    snd_h[...] = message[...].astype(BF16)
    halfs.start()
    for v in range(3):
        grad_control_ref[v] = control[v] + std[v] * adjoint[v, tile, :]

    @pl.when(owner)
    def _():
        halfs.take_own()
        for i in range(1, parts):
            halfs.receive(i)
        weighted = []
        for p in range(parts):
            came_h = rcv_h[p].astype(F32)

            def row_of(v, j):
                pieces = [came_h[8 * h + per * v + j : 8 * h + per * v + j + 1] for h in range(halves)]
                return jnp.broadcast_to(jnp.concatenate(pieces, axis=1), (slots, cols))

            def field_of(v, count):
                out = row_of(v, per - 1)
                for j in reversed(range(per - 1)):
                    out = jnp.where(at_slot < (j + 1) * members, row_of(v, j), out)
                return out

            third = field_of(2, items)
            a = rcv_e[p, :slots].astype(F32) * jnp.where(at_slot < items, field_of(0, items), pltpu.roll(third, items, 0))
            b = rcv_e[p, slots : 2 * slots].astype(F32) * jnp.where(
                at_slot < items, field_of(1, items), pltpu.roll(third, items - spare, 0)
            )
            rest = total_slots - 2 * slots
            c = rcv_e[p, 2 * slots :].astype(F32) * third[2 * spare : 2 * spare + rest]
            own = jnp.concatenate([jnp.zeros((2 * spare, cols), F32), c], axis=0)[:slots]
            own = jnp.where(at_slot < 2 * spare, pltpu.roll(b, slots - (items - spare), 0), own)
            own = jnp.where(at_slot < spare, pltpu.roll(a, slots - items, 0), own)
            weighted.append(a + b + own)
        outs = filtered([[x[:, h * LANES : (h + 1) * LANES] for x in weighted] for h in range(halves)])
        for p in range(parts):
            for h in range(halves):
                out_stage[p, h * items : (h + 1) * items, :] = outs[h][p][:items]
            snd_o[p] = out_stage[p].astype(BF16)
        for i in range(1, parts):
            out_copy(i).start()
        rcv_o[mine] = snd_o[part]

    for k in range(owners):
        at = lax.rem(part + k, owners)
        arrival = pltpu.make_async_remote_copy(
            src_ref=snd_o.at[0], dst_ref=rcv_o.at[at],
            send_sem=o_send.at[0], recv_sem=o_recv.at[at], device_id={"sp": left},
        )
        pl.when(at != mine)(arrival.wait_recv)
    stage[...] = rcv_o[...].astype(F32)
    for m in range(members):
        for j in range(per):
            for h in range(halves):
                at, lanes = slice(j * owners, (j + 1) * owners), slice(h * LANES, (h + 1) * LANES)
                corr_ref[m, at, lanes] = alpha[m, at, lanes] + spread * stage[:, h * items + j * members + m, :]
    alphas.finish()
    enses.finish()
    halfs.finish()
    for copy in field_copies:
        copy.wait_send()

    @pl.when(owner)
    def _():
        for i in range(parts):
            for j in range(groups):
                if i + j > 0:
                    inc_copy(i, j).wait_send()
        for i in range(1, parts):
            out_copy(i).wait_send()


def finish(corr_ref, grad_control_ref, corr_out, grad_control_out, sem):
    copies = [
        pltpu.make_async_copy(corr_ref, corr_out, sem.at[0]),
        pltpu.make_async_copy(grad_control_ref, grad_control_out, sem.at[1]),
    ]
    for copy in copies:
        copy.start()
    for copy in copies:
        copy.wait()


def tables(parts, cols, waves, members, rows):
    length = parts * cols
    inner = waves // parts
    residues = parts // 2 + 1
    twist = 2 * np.pi * np.outer(np.arange(residues), np.arange(cols)) / length
    quotient = np.arange(-inner, inner)
    phase = 2 * np.pi * (np.outer(np.arange(cols), quotient) % cols) / cols
    c, s = np.cos(phase), np.sin(phase)
    forward = np.block([[c, -s], [s, c]])
    owners, per, items, slots, spare, total_slots = layout(members, rows, parts)
    pick = np.zeros((8, 2, total_slots), np.float32)
    for v in range(3):
        for j in range(per):
            for m in range(members):
                pick[v * per + j, :, slot_of(v, j * members + m, items, slots, spare)] = 1.0
    return (
        *both(forward), *both(forward.T.copy()), np.cos(twist).astype(np.float32), np.sin(twist).astype(np.float32),
        pick.reshape(8, 2 * total_slots).astype(BF16),
    )


def per_device(alpha, ensemble, static_std, control, loc_spectrum, obs_cell, obs_step, innovation, obs_weight):
    members, rows, cols = alpha.shape
    groups, parts = lax.axis_size("grp"), lax.axis_size("sp")
    spread = 1.0 / math.sqrt(members * groups - 1)
    owners, per, items, slots, spare, total_slots = layout(members, rows, parts)
    assert owners * per == rows and 4 * per <= 8 and spare % 4 == 0
    tile_rows = control.shape[1]
    halves = cols // LANES
    residues = parts // 2 + 1
    inner = loc_spectrum.shape[0] // parts
    operands = (
        alpha, ensemble, static_std, control, loc_spectrum[None],
        obs_cell[None], obs_step[None], innovation[None], obs_weight[None],
        *tables(parts, cols, loc_spectrum.shape[0], members, rows),
    )
    packed = (round8(halves * items), LANES)
    message = (8 * halves, LANES)
    vmem = pl.BlockSpec(memory_space=pltpu.VMEM)
    dma = pltpu.SemaphoreType.DMA
    corr, grad_control = pl.pallas_call(
        functools.partial(kernel, groups, parts, spread),
        out_shape=(
            pltpu.VMEM(alpha.shape, F32),
            pltpu.VMEM(control.shape, F32),
        ),
        in_specs=[HBM] * len(operands),
        out_specs=(vmem, vmem),
        scratch_shapes=[
            *[pltpu.VMEM(t.shape, t.dtype) for t in operands],
            pltpu.VMEM((owners, *packed), F32),
            pltpu.VMEM((parts, *packed), F32),
            pltpu.VMEM((owners, total_slots, cols), F32),
            pltpu.VMEM((parts, slots, cols), F32),
            pltpu.VMEM((3, rows, cols), F32),
            pltpu.VMEM((round8(residues), 4 * inner), F32),
            pltpu.VMEM((9, tile_rows, cols), F32),
            pltpu.VMEM((9, rows, cols + LANES), F32),
            pltpu.VMEM((owners, *message), F32),
            pltpu.VMEM((owners, *packed), BF16), pltpu.VMEM((parts, *packed), BF16),
            pltpu.VMEM((owners, total_slots, cols), BF16), pltpu.VMEM((parts, total_slots, cols), BF16),
            pltpu.VMEM((parts, *message), BF16), pltpu.VMEM((groups, owners, *message), BF16),
            pltpu.VMEM((owners, *message), BF16), pltpu.VMEM((parts, *message), BF16),
            pltpu.VMEM((parts, *packed), BF16), pltpu.VMEM((owners, *packed), BF16),
            pltpu.VMEM((groups, 9, tile_rows, cols), F32),
            pltpu.VMEM((tile_rows, LANES), F32), pltpu.VMEM((2, groups, tile_rows, LANES), F32),
            dma((len(operands),)),
            dma((owners,)), dma((parts,)), dma((owners,)), dma((parts,)),
            dma((parts, groups)), dma((groups, owners)),
            dma((owners,)), dma((parts,)), dma((parts,)), dma((owners,)),
            dma((3, groups)), dma((3, groups)),
            pltpu.SemaphoreType.REGULAR,
        ],
        compiler_params=pltpu.CompilerParams(collective_id=0, has_side_effects=True, vmem_limit_bytes=63 << 20),
    )(*operands)
    return pl.pallas_call(
        finish,
        out_shape=(jax.ShapeDtypeStruct(alpha.shape, F32), jax.ShapeDtypeStruct(control.shape, F32)),
        in_specs=[vmem] * 2,
        out_specs=(HBM, HBM),
        scratch_shapes=[dma((2,))],
        compiler_params=pltpu.CompilerParams(vmem_limit_bytes=1 << 20),
    )(corr, grad_control)


def solution(mesh):
    flat = P(("grp", "sp"))
    tile = P(None, "grp", "sp")
    return jax.shard_map(
        per_device,
        mesh=mesh,
        in_specs=(P("grp", None, "sp"), P("grp", None, None, "sp"), tile, tile, P(), flat, flat, flat, flat),
        out_specs=(P("grp", None, "sp"), tile),
        check_vma=False,
    )
```

```python
import functools
import math

import jax
import jax.numpy as jnp
import numpy as np
from jax import lax
from jax.experimental import pallas as pl
from jax.experimental.pallas import tpu as pltpu
from jax.sharding import PartitionSpec as P

COURANT = 0.4
LANES = 128
HALO = 8
BATCHES = 4
BF16, F32 = jnp.bfloat16, jnp.float32
HBM = pl.BlockSpec(memory_space=pltpu.HBM)


def dot(a, b, contract=((1,), (0,))):
    return lax.dot_general(a, b, (contract, ((), ())), preferred_element_type=F32)


def split2(x):
    hi = x.astype(BF16)
    return hi, (x - hi.astype(F32)).astype(BF16)


def both(table):
    table = np.asarray(table, np.float32)
    hi = table.astype(BF16)
    return hi, (table - hi.astype(np.float32)).astype(BF16)


def add(a, b, sign=1.0):
    re = a[0] + b[0] if sign > 0 else a[0] - b[0]
    if b[1] is None:
        return re, a[1]
    if a[1] is None:
        return re, b[1] if sign > 0 else -b[1]
    return re, a[1] + b[1] if sign > 0 else a[1] - b[1]


def conj(a):
    return a[0], None if a[1] is None else -a[1]


def turn(a, eighths, n):
    at = (eighths % n) / n
    if at == 0:
        return a
    re, im = a
    if at == 0.25:
        return (jnp.zeros_like(re) if im is None else -im), re
    if at == 0.75:
        return (jnp.zeros_like(re) if im is None else im), -re
    c, s = math.cos(2 * math.pi * at), math.sin(2 * math.pi * at)
    if im is None:
        return c * re, s * re
    return c * re - s * im, c * im + s * re


def real_dft(xs):
    n = len(xs)
    if n == 1:
        return [(xs[0], None)]
    if n == 2:
        return [(xs[0] + xs[1], None), (xs[0] - xs[1], None)]
    half = n // 2
    even, odd = real_dft(xs[0::2]), real_dft(xs[1::2])
    out = [None] * (half + 1)
    for k in range(half // 2 + 1):
        t = turn(odd[k], -k, n)
        out[k] = add(even[k], t)
        if half - k != k:
            out[half - k] = conj(add(even[k], t, -1.0))
    return out


def real_sum(zs, n):
    if n == 1:
        return [zs[0][0]]
    if n == 2:
        return [zs[0][0] + zs[1][0], zs[0][0] - zs[1][0]]
    half = n // 2
    even, odd = [], []
    for k in range(half // 2 + 1):
        if half - k == k:
            even.append(zs[k])
            odd.append(turn(zs[k], k, n))
        else:
            other = conj(zs[half - k])
            even.append(add(zs[k], other))
            odd.append(turn(add(zs[k], other, -1.0), k, n))
    even, odd = real_sum(even, half), real_sum(odd, half)
    return [(even, odd)[p % 2][p // 2] for p in range(n)]


def dx(q):
    width = q.shape[1]
    return 0.5 * (pltpu.roll(q, width - 1, 1) - pltpu.roll(q, 1, 1))


def dy(q):
    rows = q.shape[0]
    at = lax.broadcasted_iota(jnp.int32, q.shape, 0)
    above = jnp.where(at < rows - 1, pltpu.roll(q, rows - 1, 0), 0.0)
    below = jnp.where(at > 0, pltpu.roll(q, 1, 0), 0.0)
    return 0.5 * (above - below)


def model_step(state, rotation):
    h, u, w = state
    h = h - COURANT * (dx(u) + dy(w))
    return h, u - COURANT * dx(h) + rotation * w, w - COURANT * dy(h) - rotation * u


def adjoint_step(state, rotation):
    h, u, w = state
    a = h + COURANT * (dx(u) + dy(w))
    return a, u - rotation * w + COURANT * dx(a), w + rotation * u + COURANT * dy(a)


def round8(n):
    return -(-n // 8) * 8


def layout(members, rows, parts):
    owners = parts // 2
    per = rows // owners
    items = per * members
    slots = round8(items)
    spare = slots - items
    return owners, per, items, slots, spare, 2 * slots + round8(items - 2 * spare)


def slot_of(v, item, items, slots, spare):
    if v < 2:
        return v * slots + item
    if item < spare:
        return items + item
    if item < 2 * spare:
        return slots + items + item - spare
    return 2 * slots + item - 2 * spare


def kernel(
    groups, parts, spread,
    alpha_any, ens_any, std_any, control_any, spectrum_any, cell_any, step_any, innovation_any, weight_any,
    fwd_hi_any, fwd_lo_any, inv_hi_any, inv_lo_any, tw_c_any, tw_s_any, pick_any,
    corr_ref, grad_control_ref,
    alpha, ens, std, control, spectrum, cell, step, innovation, weight,
    fwd_hi, fwd_lo, inv_hi, inv_lo, tw_c, tw_s, pick,
    stage, out_stage, ens_stage, loc_buf, adjoint, waves, fields, wide, message,
    snd_a, rcv_a, snd_e, rcv_e, snd_i, rcv_i, snd_h, rcv_h, snd_o, rcv_o, rcv_f, edge, rcv_edge,
    load_sem, a_send, a_recv, e_send, e_recv, i_send, i_recv, h_send, h_recv, o_send, o_recv, f_send, f_recv, here, whole, go,
):
    group, part = lax.axis_index("grp"), lax.axis_index("sp")
    left, right = lax.rem(part + parts - 1, parts), lax.rem(part + 1, parts)
    members, rows, cols = alpha.shape
    tile_rows = control.shape[1]
    tile = pl.ds(pl.multiple_of(group * tile_rows, tile_rows), tile_rows)
    owners, per, items, slots, spare, total_slots = layout(members, rows, parts)
    low = parts // 4
    mine = part - low
    owner = (part >= low) & (part < low + owners)
    halves = cols // LANES
    residues = parts // 2 + 1

    barrier = pltpu.get_barrier_semaphore()

    @pl.when(owner)
    def _():
        for i in range(1, parts):
            pl.semaphore_signal(barrier, inc=1, device_id={"sp": lax.rem(part + i, parts)})

    for j in range(1, groups):
        pl.semaphore_signal(barrier, inc=1, device_id={"grp": lax.rem(group + j, groups)})

    pairs = [
        (alpha_any, alpha), (ens_any, ens), (cell_any, cell), (step_any, step), (innovation_any, innovation),
        (weight_any, weight), (std_any, std), (control_any, control), (spectrum_any, spectrum),
        (fwd_hi_any, fwd_hi), (fwd_lo_any, fwd_lo), (inv_hi_any, inv_hi), (inv_lo_any, inv_lo),
        (tw_c_any, tw_c), (tw_s_any, tw_s), (pick_any, pick),
    ]
    loads = [pltpu.make_async_copy(a, b, load_sem.at[i]) for i, (a, b) in enumerate(pairs)]
    for load in loads:
        load.start()

    loads[0].wait()
    filled = halves * items
    if stage.shape[1] > filled:
        stage[:, filled:, :] = jnp.zeros((owners, stage.shape[1] - filled, LANES), F32)
    for m in range(members):
        for j in range(per):
            for h in range(halves):
                stage[:, h * items + j * members + m, :] = (
                    alpha[m, j * owners : (j + 1) * owners, h * LANES : (h + 1) * LANES]
                )
    snd_a[...] = stage[...].astype(BF16)

    @pl.when(owner)
    def _():
        pl.semaphore_wait(barrier, owners + groups - 2)

    @pl.when(jnp.logical_not(owner))
    def _():
        pl.semaphore_wait(barrier, owners + groups - 1)
        for i in range(owners):
            pl.semaphore_signal(here, inc=1, device_id={"sp": low + lax.rem(part + i, owners)})

    class ToOwners:
        def __init__(self, source, target, send, recv):
            self.source, self.target, self.send, self.recv = source, target, send, recv

        def copy(self, i):
            at = lax.rem(part + i, owners)
            return low + at, pltpu.make_async_remote_copy(
                src_ref=self.source.at[at], dst_ref=self.target.at[part],
                send_sem=self.send.at[i], recv_sem=self.recv.at[part], device_id={"sp": low + at},
            )

        def start(self):
            for i in range(owners):
                to, copy = self.copy(i)
                pl.when(to != part)(copy.start)

        def take_own(self):
            self.target[part] = self.source[mine]

        def receive(self, i):
            at = lax.rem(part + parts - i, parts)
            pltpu.make_async_remote_copy(
                src_ref=self.source.at[0], dst_ref=self.target.at[at],
                send_sem=self.send.at[0], recv_sem=self.recv.at[at], device_id={"sp": left},
            ).wait_recv()

        def finish(self):
            for i in range(owners):
                to, copy = self.copy(i)
                pl.when(to != part)(copy.wait_send)

    alphas = ToOwners(snd_a, rcv_a, a_send, a_recv)
    enses = ToOwners(snd_e, rcv_e, e_send, e_recv)
    halfs = ToOwners(snd_h, rcv_h, h_send, h_recv)
    alphas.start()
    loads[1].wait()
    used = set()
    for v in range(3):
        for m in range(members):
            field = ens[m, v].astype(F32)
            for j in range(per):
                at = slot_of(v, j * members + m, items, slots, spare)
                used.add(at)
                ens_stage[:, at, :] = field[j * owners : (j + 1) * owners]
    for at in range(total_slots):
        if at not in used:
            ens_stage[:, at, :] = jnp.zeros((owners, cols), F32)
    snd_e[...] = ens_stage[...].astype(BF16)
    enses.start()

    for load in loads[2:8]:
        load.wait()
    pitch = -(-tile_rows // 8) * 8
    nx = cols * parts
    first = group * tile_rows
    row = jnp.zeros_like(cell)
    cells = cell[...]
    for r in range(1, tile_rows):
        row = row + jnp.where(cells >= (first + r) * nx, 1, 0)
    col = cells - (first + row) * nx - part * cols
    slot = step[...] * pitch + row
    observations = cells.shape[1]
    in_col = (lax.broadcasted_iota(jnp.int32, (cols, observations), 0) == col).astype(F32).astype(BF16)
    in_slot = lax.broadcasted_iota(jnp.int32, (3 * pitch, observations), 0) == slot
    obs_weight = weight[...]
    values = jnp.concatenate([
        jnp.where(in_slot, obs_weight, 0.0), jnp.where(in_slot, obs_weight * innovation[...], 0.0)
    ], axis=0)
    hi, lo = split2(values)
    summed = dot(hi, in_col, ((1,), (1,))) + dot(lo, in_col, ((1,), (1,)))
    for v in range(3):
        fields[v] = std[v] * control[v]
    for f in range(6):
        fields[3 + f] = summed[f * pitch : f * pitch + tile_rows]
    haloed = (0, 1, 2, 4, 5, 7, 8)
    lane = lax.broadcasted_iota(jnp.int32, (tile_rows, LANES), 1)
    packed = jnp.zeros((tile_rows, LANES), F32)
    for e, f in enumerate(haloed):
        ends = jnp.where(lane < LANES // 2, fields[f, :, :LANES], fields[f, :, cols - LANES :])
        window = (lane >= 2 * HALO * e) & (lane < 2 * HALO * (e + 1))
        packed = jnp.where(window, pltpu.roll(ends, (2 * HALO * e + HALO) % LANES, 1), packed)
    edge[...] = packed

    rcv_f[group] = fields[...]
    full_copies = [
        pltpu.make_async_remote_copy(
            src_ref=fields, dst_ref=rcv_f.at[group],
            send_sem=f_send.at[0, j], recv_sem=f_recv.at[0, j], device_id={"grp": lax.rem(group + j, groups)},
        )
        for j in range(1, groups)
    ]
    for copy in full_copies:
        copy.start()

    @pl.when(owner)
    def _():
        pl.semaphore_wait(here, parts - owners)
        for j in range(1, groups):
            pl.semaphore_signal(whole, inc=1, device_id={"grp": lax.rem(group + j, groups)})

    for load in loads[8:]:
        load.wait()

    def filtered(xs, exact):
        pieces = xs
        spectra = [real_dft(piece) for piece in pieces]
        res, ims = [], []
        for k1 in range(residues):
            parts_re, parts_im = [], []
            for h in range(halves):
                c = tw_c[k1 : k1 + 1, h * LANES : (h + 1) * LANES]
                s = tw_s[k1 : k1 + 1, h * LANES : (h + 1) * LANES]
                re, im = spectra[h][k1]
                if k1 == 0:
                    parts_re.append(re)
                    parts_im.append(jnp.zeros_like(re))
                elif im is None:
                    parts_re.append(re * c)
                    parts_im.append(-re * s)
                else:
                    parts_re.append(re * c + im * s)
                    parts_im.append(im * c - re * s)
            res.append(jnp.concatenate(parts_re + parts_im, axis=1))
        y_hi, y_lo = split2(jnp.concatenate(res, axis=0))
        z = dot(y_hi, fwd_hi[...])
        if exact:
            z = z + dot(y_lo, fwd_hi[...]) + dot(y_hi, fwd_lo[...])
        z = jnp.concatenate(
            [z[k1 * slots : (k1 + 1) * slots] * waves[k1 : k1 + 1, :] for k1 in range(residues)], axis=0
        )
        z_hi, z_lo = split2(z)
        v = dot(z_hi, inv_hi[...])
        if exact:
            v = v + dot(z_lo, inv_hi[...]) + dot(z_hi, inv_lo[...])
        outs = []
        for h in range(halves):
            zs = []
            for k1 in range(residues):
                c = tw_c[k1 : k1 + 1, h * LANES : (h + 1) * LANES]
                s = tw_s[k1 : k1 + 1, h * LANES : (h + 1) * LANES]
                at = slice(k1 * slots, (k1 + 1) * slots)
                re = v[at, h * LANES : (h + 1) * LANES]
                im = v[at, cols + h * LANES : cols + (h + 1) * LANES]
                zs.append((re, im) if k1 == 0 else (re * c - im * s, im * c + re * s))
            outs.append(real_sum(zs, parts))
        return outs

    at_slot = lax.broadcasted_iota(jnp.int32, (slots, cols), 0)

    def inc_copy(i, j):
        return pltpu.make_async_remote_copy(
            src_ref=snd_i.at[i], dst_ref=rcv_i.at[group, mine],
            send_sem=i_send.at[i, j], recv_sem=i_recv.at[group, mine],
            device_id={"grp": lax.rem(group + j, groups), "sp": lax.rem(part + parts - i, parts)},
        )

    def out_copy(i):
        to = i
        return pltpu.make_async_remote_copy(
            src_ref=snd_o.at[to], dst_ref=rcv_o.at[mine],
            send_sem=o_send.at[i], recv_sem=o_recv.at[mine], device_id={"sp": to},
        )

    @pl.when(owner)
    def _():
        count = spectrum.shape[1]
        inner = count // parts
        wave = lax.broadcasted_iota(jnp.int32, (waves.shape[0], count), 1)
        residue = lax.broadcasted_iota(jnp.int32, wave.shape, 0)
        weights = jnp.broadcast_to(spectrum[...], wave.shape)
        forward = jnp.where((lax.rem(wave, parts) == residue) & (residue < residues), weights, 0.0)
        mirrored = (lax.rem(wave + residue, parts) == 0) & (residue > 0) & (residue < residues - 1)
        backward = jnp.where(mirrored, weights, 0.0)
        k = lax.broadcasted_iota(jnp.int32, (count, 4 * inner), 0)
        j = lax.rem(lax.broadcasted_iota(jnp.int32, (count, 4 * inner), 1), 2 * inner)
        ahead, behind = k - parts * (j - inner), k - parts * (inner - 1 - j)
        ahead = jnp.where((ahead >= 0) & (ahead < parts), 1.0, 0.0).astype(BF16)
        behind = jnp.where((behind >= 0) & (behind < parts), 1.0, 0.0).astype(BF16)
        f_hi, f_lo = split2(forward)
        b_hi, b_lo = split2(backward)
        waves[...] = dot(f_hi, ahead) + dot(f_lo, ahead) + dot(b_hi, behind) + dot(b_lo, behind)

        alphas.take_own()
        enses.take_own()
        for i in range(1, parts):
            alphas.receive(i)
        came = [[None] * parts for _ in range(halves)]
        for p in range(parts):
            x = rcv_a[p].astype(F32)
            for h in range(halves):
                came[h][p] = (x if h == 0 else pltpu.roll(x, x.shape[0] - h * items, 0))[:slots]
        localized = filtered(came, True)
        for p in range(parts):
            loc = jnp.concatenate([localized[h][p] for h in range(halves)], axis=1)
            loc_buf[p] = loc.astype(BF16).astype(F32)
    @pl.when(owner)
    def _():
        if groups > 1:
            pl.semaphore_wait(whole, groups - 1)
        for i in range(parts // owners):
            to = mine * (parts // owners) + i

            @pl.when(to != part)
            def _():
                pl.semaphore_signal(go, inc=1, device_id={"sp": to})

    @pl.when(part // (parts // owners) != mine)
    def _():
        pl.semaphore_wait(go, 1)

    end_copies = []
    for j in range(groups):
        for kind, at, target in ((1, right, rcv_edge.at[0, group]), (2, left, rcv_edge.at[1, group])):
            end_copies.append(pltpu.make_async_remote_copy(
                src_ref=edge, dst_ref=target, send_sem=f_send.at[kind, j], recv_sem=f_recv.at[kind, j],
                device_id={"grp": lax.rem(group + j, groups), "sp": at},
            ))
            end_copies[-1].start()
    field_copies = full_copies + end_copies

    @pl.when(owner)
    def _():
        lane = lax.broadcasted_iota(jnp.int32, (8, LANES), 1)
        at_row = lax.broadcasted_iota(jnp.int32, (8, LANES), 0)
        tiles = [None] * parts

        def increments(p):
            loc = loc_buf[p]
            a = rcv_e[p, :slots].astype(F32) * jnp.where(at_slot < items, loc, pltpu.roll(loc, items, 0))
            b = rcv_e[p, slots : 2 * slots].astype(F32) * jnp.where(at_slot < items, loc, pltpu.roll(loc, items - spare, 0))
            rest = total_slots - 2 * slots
            c = rcv_e[p, 2 * slots :].astype(F32) * loc[2 * spare : 2 * spare + rest]
            hi, lo = split2(jnp.concatenate([a, b, c], axis=0))
            return spread * dot(pick[...], jnp.concatenate([hi, lo], axis=0))

        def put_increments(i):
            after, before = tiles[i - 1][:, :LANES], tiles[(i + 1) % parts][:, cols - LANES :]
            ends = jnp.where(lane < LANES // 2, after, before)
            pieces = [tiles[i][:, h * LANES : (h + 1) * LANES] for h in range(halves)]
            for v in range(3):
                window = (lane >= 2 * HALO * v) & (lane < 2 * HALO * (v + 1)) & (at_row >= 3 * per)
                moved = pltpu.roll(ends, 2 * HALO * v + HALO, 1)
                if 3 * per - per * v:
                    moved = pltpu.roll(moved, 3 * per - per * v, 0)
                pieces[0] = jnp.where(window, moved, pieces[0])
            snd_i[i] = jnp.concatenate(pieces, axis=0).astype(BF16)

        batch = owners // BATCHES
        for first_of in range(0, owners, batch):
            blocks = [i for k in range(first_of, first_of + batch) for i in (k, k + owners)]
            for i in blocks:
                if i > 0:
                    enses.receive(i)
            for i in blocks:
                tiles[i] = increments(lax.rem(part + parts - i, parts))
            ready = [i for k in range(first_of - 1, first_of + batch - 1) if k > 0 for i in (k, k + owners)]
            if first_of + batch == owners:
                ready += [owners - 1, parts - 1, 0, owners]
            for i in ready:
                put_increments(i)
            for i in ready:
                for j in range(groups):
                    if i + j > 0:
                        inc_copy(i, j).start()
        rcv_i[group, mine] = snd_i[0]

    for copy in field_copies:
        copy.wait_recv()
    lane = lax.broadcasted_iota(jnp.int32, (tile_rows, LANES), 1)
    for g in range(groups):
        at = slice(g * tile_rows, (g + 1) * tile_rows)
        for f in range(9):
            wide[f, at, :cols] = rcv_f[g, f]
            if f in haloed:
                back = LANES - (2 * HALO * haloed.index(f) + HALO)
                before, after = (pltpu.roll(rcv_edge[side, g], back, 1) for side in (0, 1))
                wide[f, at, cols:] = jnp.where(lane < LANES // 2, after, before)
            else:
                wide[f, at, cols:] = jnp.zeros((tile_rows, LANES), F32)

    for j in range(groups):
        for k in range(owners):
            g, at = lax.rem(group + j, groups), lax.rem(part + k, owners)
            arrival = pltpu.make_async_remote_copy(
                src_ref=snd_i.at[0], dst_ref=rcv_i.at[g, at],
                send_sem=i_send.at[0, 0], recv_sem=i_recv.at[g, at], device_id={"sp": left},
            )
            if j == 0:
                pl.when(at != mine)(arrival.wait_recv)
            else:
                arrival.wait_recv()
    total = rcv_i[0].astype(F32)
    for g in range(1, groups):
        total = total + rcv_i[g].astype(F32)
    message[...] = total

    def gathered(index):
        return jnp.concatenate([message[:, index + j, :] for j in range(per)], axis=0)

    ends = gathered(3 * per)
    state0 = []
    for v in range(3):
        pieces = [gathered(8 * h + per * v) for h in range(halves)]
        pieces.append(pltpu.roll(ends, LANES - (2 * HALO * v + HALO), 1))
        state0.append(jnp.concatenate(pieces, axis=1) + wide[v])
    row_at = lax.broadcasted_iota(jnp.int32, (rows, cols + LANES), 0).astype(F32)
    rotation = 0.1 + 0.2 * (row_at + 0.5) / rows
    state1 = model_step(state0, rotation)
    state2 = model_step(state1, rotation)
    forcing = [wide[3 + t] * s[0] - wide[6 + t] for t, s in enumerate((state0, state1, state2))]
    zero = jnp.zeros_like(rotation)
    h, u, w = adjoint_step((forcing[2], zero, zero), rotation)
    h, u, w = adjoint_step((h + forcing[1], u, w), rotation)
    for v, field in enumerate((h + forcing[0], u, w)):
        field = field[:, :cols]
        adjoint[v] = field
        half = field.astype(BF16).astype(F32)
        for h in range(halves):
            for j in range(per):
                message[:, 8 * h + per * v + j, :] = half[j * owners : (j + 1) * owners, h * LANES : (h + 1) * LANES]
    snd_h[...] = message[...].astype(BF16)
    halfs.start()
    for v in range(3):
        grad_control_ref[v] = control[v] + std[v] * adjoint[v, tile, :]

    @pl.when(owner)
    def _():
        halfs.take_own()
        for i in range(1, parts):
            halfs.receive(i)
        weighted = []
        for p in range(parts):
            came_h = rcv_h[p].astype(F32)

            def row_of(v, j):
                pieces = [came_h[8 * h + per * v + j : 8 * h + per * v + j + 1] for h in range(halves)]
                return jnp.broadcast_to(jnp.concatenate(pieces, axis=1), (slots, cols))

            def field_of(v, count):
                out = row_of(v, per - 1)
                for j in reversed(range(per - 1)):
                    out = jnp.where(at_slot < (j + 1) * members, row_of(v, j), out)
                return out

            third = field_of(2, items)
            a = rcv_e[p, :slots].astype(F32) * jnp.where(at_slot < items, field_of(0, items), pltpu.roll(third, items, 0))
            b = rcv_e[p, slots : 2 * slots].astype(F32) * jnp.where(
                at_slot < items, field_of(1, items), pltpu.roll(third, items - spare, 0)
            )
            rest = total_slots - 2 * slots
            c = rcv_e[p, 2 * slots :].astype(F32) * third[2 * spare : 2 * spare + rest]
            own = jnp.concatenate([jnp.zeros((2 * spare, cols), F32), c], axis=0)[:slots]
            own = jnp.where(at_slot < 2 * spare, pltpu.roll(b, slots - (items - spare), 0), own)
            own = jnp.where(at_slot < spare, pltpu.roll(a, slots - items, 0), own)
            weighted.append(a + b + own)
        outs = filtered([[x[:, h * LANES : (h + 1) * LANES] for x in weighted] for h in range(halves)], False)
        for p in range(parts):
            for h in range(halves):
                out_stage[p, h * items : (h + 1) * items, :] = outs[h][p][:items]
            snd_o[p] = out_stage[p].astype(BF16)
        for i in range(parts):
            pl.when(part != i)(out_copy(i).start)
        rcv_o[mine] = snd_o[part]

    for k in range(owners):
        at = lax.rem(part + k, owners)
        arrival = pltpu.make_async_remote_copy(
            src_ref=snd_o.at[0], dst_ref=rcv_o.at[at],
            send_sem=o_send.at[0], recv_sem=o_recv.at[at], device_id={"sp": left},
        )
        pl.when(at != mine)(arrival.wait_recv)
    stage[...] = rcv_o[...].astype(F32)
    for m in range(members):
        for j in range(per):
            for h in range(halves):
                at, lanes = slice(j * owners, (j + 1) * owners), slice(h * LANES, (h + 1) * LANES)
                corr_ref[m, at, lanes] = alpha[m, at, lanes] + spread * stage[:, h * items + j * members + m, :]
    alphas.finish()
    enses.finish()
    halfs.finish()
    for copy in field_copies:
        copy.wait_send()

    @pl.when(owner)
    def _():
        for i in range(parts):
            for j in range(groups):
                if i + j > 0:
                    inc_copy(i, j).wait_send()
        for i in range(parts):
            pl.when(part != i)(out_copy(i).wait_send)


def finish(corr_ref, grad_control_ref, corr_out, grad_control_out, sem):
    copies = [
        pltpu.make_async_copy(corr_ref, corr_out, sem.at[0]),
        pltpu.make_async_copy(grad_control_ref, grad_control_out, sem.at[1]),
    ]
    for copy in copies:
        copy.start()
    for copy in copies:
        copy.wait()


def tables(parts, cols, waves, members, rows):
    length = parts * cols
    inner = waves // parts
    residues = parts // 2 + 1
    twist = 2 * np.pi * np.outer(np.arange(residues), np.arange(cols)) / length
    quotient = np.arange(-inner, inner)
    phase = 2 * np.pi * (np.outer(np.arange(cols), quotient) % cols) / cols
    c, s = np.cos(phase), np.sin(phase)
    forward = np.block([[c, -s], [s, c]])
    owners, per, items, slots, spare, total_slots = layout(members, rows, parts)
    pick = np.zeros((8, 2, total_slots), np.float32)
    for v in range(3):
        for j in range(per):
            for m in range(members):
                pick[v * per + j, :, slot_of(v, j * members + m, items, slots, spare)] = 1.0
    return (
        *both(forward), *both(forward.T.copy()), np.cos(twist).astype(np.float32), np.sin(twist).astype(np.float32),
        pick.reshape(8, 2 * total_slots).astype(BF16),
    )


def per_device(alpha, ensemble, static_std, control, loc_spectrum, obs_cell, obs_step, innovation, obs_weight):
    members, rows, cols = alpha.shape
    groups, parts = lax.axis_size("grp"), lax.axis_size("sp")
    spread = 1.0 / math.sqrt(members * groups - 1)
    owners, per, items, slots, spare, total_slots = layout(members, rows, parts)
    assert owners * per == rows and 4 * per <= 8 and spare % 4 == 0
    tile_rows = control.shape[1]
    halves = cols // LANES
    residues = parts // 2 + 1
    inner = loc_spectrum.shape[0] // parts
    operands = (
        alpha, ensemble, static_std, control, loc_spectrum[None],
        obs_cell[None], obs_step[None], innovation[None], obs_weight[None],
        *tables(parts, cols, loc_spectrum.shape[0], members, rows),
    )
    packed = (round8(halves * items), LANES)
    message = (8 * halves, LANES)
    vmem = pl.BlockSpec(memory_space=pltpu.VMEM)
    dma = pltpu.SemaphoreType.DMA
    corr, grad_control = pl.pallas_call(
        functools.partial(kernel, groups, parts, spread),
        out_shape=(
            pltpu.VMEM(alpha.shape, F32),
            pltpu.VMEM(control.shape, F32),
        ),
        in_specs=[HBM] * len(operands),
        out_specs=(vmem, vmem),
        scratch_shapes=[
            *[pltpu.VMEM(t.shape, t.dtype) for t in operands],
            pltpu.VMEM((owners, *packed), F32),
            pltpu.VMEM((parts, *packed), F32),
            pltpu.VMEM((owners, total_slots, cols), F32),
            pltpu.VMEM((parts, slots, cols), F32),
            pltpu.VMEM((3, rows, cols), F32),
            pltpu.VMEM((round8(residues), 4 * inner), F32),
            pltpu.VMEM((9, tile_rows, cols), F32),
            pltpu.VMEM((9, rows, cols + LANES), F32),
            pltpu.VMEM((owners, *message), F32),
            pltpu.VMEM((owners, *packed), BF16), pltpu.VMEM((parts, *packed), BF16),
            pltpu.VMEM((owners, total_slots, cols), BF16), pltpu.VMEM((parts, total_slots, cols), BF16),
            pltpu.VMEM((parts, *message), BF16), pltpu.VMEM((groups, owners, *message), BF16),
            pltpu.VMEM((owners, *message), BF16), pltpu.VMEM((parts, *message), BF16),
            pltpu.VMEM((parts, *packed), BF16), pltpu.VMEM((owners, *packed), BF16),
            pltpu.VMEM((groups, 9, tile_rows, cols), F32),
            pltpu.VMEM((tile_rows, LANES), F32), pltpu.VMEM((2, groups, tile_rows, LANES), F32),
            dma((len(operands),)),
            dma((owners,)), dma((parts,)), dma((owners,)), dma((parts,)),
            dma((parts, groups)), dma((groups, owners)),
            dma((owners,)), dma((parts,)), dma((parts,)), dma((owners,)),
            dma((3, groups)), dma((3, groups)),
            pltpu.SemaphoreType.REGULAR, pltpu.SemaphoreType.REGULAR, pltpu.SemaphoreType.REGULAR,
        ],
        compiler_params=pltpu.CompilerParams(collective_id=0, has_side_effects=True, vmem_limit_bytes=63 << 20),
    )(*operands)
    return pl.pallas_call(
        finish,
        out_shape=(jax.ShapeDtypeStruct(alpha.shape, F32), jax.ShapeDtypeStruct(control.shape, F32)),
        in_specs=[vmem] * 2,
        out_specs=(HBM, HBM),
        scratch_shapes=[dma((2,))],
        compiler_params=pltpu.CompilerParams(vmem_limit_bytes=1 << 20),
    )(corr, grad_control)


def solution(mesh):
    flat = P(("grp", "sp"))
    tile = P(None, "grp", "sp")
    return jax.shard_map(
        per_device,
        mesh=mesh,
        in_specs=(P("grp", None, "sp"), P("grp", None, None, "sp"), tile, tile, P(), flat, flat, flat, flat),
        out_specs=(P("grp", None, "sp"), tile),
        check_vma=False,
    )
```

```python
import functools
import math

import jax
import jax.numpy as jnp
import numpy as np
from jax import lax
from jax.experimental import pallas as pl
from jax.experimental.pallas import tpu as pltpu
from jax.sharding import PartitionSpec as P

COURANT = 0.4
LANES = 128
HALO = 8
BATCHES = 4
BF16, F32 = jnp.bfloat16, jnp.float32
HBM = pl.BlockSpec(memory_space=pltpu.HBM)


def dot(a, b, contract=((1,), (0,))):
    return lax.dot_general(a, b, (contract, ((), ())), preferred_element_type=F32)


def split2(x):
    hi = x.astype(BF16)
    return hi, (x - hi.astype(F32)).astype(BF16)


def both(table):
    table = np.asarray(table, np.float32)
    hi = table.astype(BF16)
    return hi, (table - hi.astype(np.float32)).astype(BF16)


def add(a, b, sign=1.0):
    re = a[0] + b[0] if sign > 0 else a[0] - b[0]
    if b[1] is None:
        return re, a[1]
    if a[1] is None:
        return re, b[1] if sign > 0 else -b[1]
    return re, a[1] + b[1] if sign > 0 else a[1] - b[1]


def conj(a):
    return a[0], None if a[1] is None else -a[1]


def turn(a, eighths, n):
    at = (eighths % n) / n
    if at == 0:
        return a
    re, im = a
    if at == 0.25:
        return (jnp.zeros_like(re) if im is None else -im), re
    if at == 0.75:
        return (jnp.zeros_like(re) if im is None else im), -re
    c, s = math.cos(2 * math.pi * at), math.sin(2 * math.pi * at)
    if im is None:
        return c * re, s * re
    return c * re - s * im, c * im + s * re


def real_dft(xs):
    n = len(xs)
    if n == 1:
        return [(xs[0], None)]
    if n == 2:
        return [(xs[0] + xs[1], None), (xs[0] - xs[1], None)]
    half = n // 2
    even, odd = real_dft(xs[0::2]), real_dft(xs[1::2])
    out = [None] * (half + 1)
    for k in range(half // 2 + 1):
        t = turn(odd[k], -k, n)
        out[k] = add(even[k], t)
        if half - k != k:
            out[half - k] = conj(add(even[k], t, -1.0))
    return out


def real_sum(zs, n):
    if n == 1:
        return [zs[0][0]]
    if n == 2:
        return [zs[0][0] + zs[1][0], zs[0][0] - zs[1][0]]
    half = n // 2
    even, odd = [], []
    for k in range(half // 2 + 1):
        if half - k == k:
            even.append(zs[k])
            odd.append(turn(zs[k], k, n))
        else:
            other = conj(zs[half - k])
            even.append(add(zs[k], other))
            odd.append(turn(add(zs[k], other, -1.0), k, n))
    even, odd = real_sum(even, half), real_sum(odd, half)
    return [(even, odd)[p % 2][p // 2] for p in range(n)]


def dx(q):
    width = q.shape[1]
    return 0.5 * (pltpu.roll(q, width - 1, 1) - pltpu.roll(q, 1, 1))


def dy(q):
    rows = q.shape[0]
    at = lax.broadcasted_iota(jnp.int32, q.shape, 0)
    above = jnp.where(at < rows - 1, pltpu.roll(q, rows - 1, 0), 0.0)
    below = jnp.where(at > 0, pltpu.roll(q, 1, 0), 0.0)
    return 0.5 * (above - below)


def model_step(state, rotation):
    h, u, w = state
    h = h - COURANT * (dx(u) + dy(w))
    return h, u - COURANT * dx(h) + rotation * w, w - COURANT * dy(h) - rotation * u


def adjoint_step(state, rotation):
    h, u, w = state
    a = h + COURANT * (dx(u) + dy(w))
    return a, u - rotation * w + COURANT * dx(a), w + rotation * u + COURANT * dy(a)


def round8(n):
    return -(-n // 8) * 8


def layout(members, rows, parts):
    owners = parts // 2
    per = rows // owners
    items = per * members
    slots = round8(items)
    spare = slots - items
    return owners, per, items, slots, spare, 2 * slots + round8(items - 2 * spare)


def half_row(slot, half, halves, used):
    whole_rows = used // 8 * 8
    if slot < whole_rows:
        return half * whole_rows + slot
    return halves * whole_rows + half * (used - whole_rows) + slot - whole_rows


def slot_of(v, item, items, slots, spare):
    if v < 2:
        return v * slots + item
    if item < spare:
        return items + item
    if item < 2 * spare:
        return slots + items + item - spare
    return 2 * slots + item - 2 * spare


def kernel(
    groups, parts, spread,
    alpha_any, ens_any, std_any, control_any, spectrum_any, cell_any, step_any, innovation_any, weight_any,
    fwd_hi_any, fwd_lo_any, inv_hi_any, inv_lo_any, tw_c_any, tw_s_any, pick_any,
    corr_ref, grad_control_ref,
    alpha, ens, std, control, spectrum, cell, step, innovation, weight,
    fwd_hi, fwd_lo, inv_hi, inv_lo, tw_c, tw_s, pick,
    stage, out_stage, ens_stage, loc_buf, adjoint, waves, fields, wide, message,
    snd_a, rcv_a, snd_e, rcv_e, snd_i, rcv_i, snd_h, rcv_h, snd_o, rcv_o, rcv_f, edge, rcv_edge,
    load_sem, a_send, a_recv, e_send, e_recv, i_send, i_recv, h_send, h_recv, o_send, o_recv, f_send, f_recv, here, whole, go,
):
    group, part = lax.axis_index("grp"), lax.axis_index("sp")
    left, right = lax.rem(part + parts - 1, parts), lax.rem(part + 1, parts)
    members, rows, cols = alpha.shape
    tile_rows = control.shape[1]
    tile = pl.ds(pl.multiple_of(group * tile_rows, tile_rows), tile_rows)
    owners, per, items, slots, spare, total_slots = layout(members, rows, parts)
    used = 3 * items
    low = parts // 4
    mine = part - low
    owner = (part >= low) & (part < low + owners)
    halves = cols // LANES
    residues = parts // 2 + 1

    barrier = pltpu.get_barrier_semaphore()

    @pl.when(owner)
    def _():
        for i in range(1, parts):
            pl.semaphore_signal(barrier, inc=1, device_id={"sp": lax.rem(part + i, parts)})

    for j in range(1, groups):
        pl.semaphore_signal(barrier, inc=1, device_id={"grp": lax.rem(group + j, groups)})

    pairs = [
        (alpha_any, alpha), (ens_any, ens), (cell_any, cell), (step_any, step), (innovation_any, innovation),
        (weight_any, weight), (std_any, std), (control_any, control), (spectrum_any, spectrum),
        (fwd_hi_any, fwd_hi), (fwd_lo_any, fwd_lo), (inv_hi_any, inv_hi), (inv_lo_any, inv_lo),
        (tw_c_any, tw_c), (tw_s_any, tw_s), (pick_any, pick),
    ]
    loads = [pltpu.make_async_copy(a, b, load_sem.at[i]) for i, (a, b) in enumerate(pairs)]
    for load in loads:
        load.start()

    loads[0].wait()
    filled = halves * items
    if stage.shape[1] > filled:
        stage[:, filled:, :] = jnp.zeros((owners, stage.shape[1] - filled, LANES), F32)
    for m in range(members):
        for j in range(per):
            for h in range(halves):
                stage[:, h * items + j * members + m, :] = (
                    alpha[m, j * owners : (j + 1) * owners, h * LANES : (h + 1) * LANES]
                )
    snd_a[...] = stage[...].astype(BF16)

    @pl.when(owner)
    def _():
        pl.semaphore_wait(barrier, owners + groups - 2)

    @pl.when(jnp.logical_not(owner))
    def _():
        pl.semaphore_wait(barrier, owners + groups - 1)
        for i in range(owners):
            pl.semaphore_signal(here, inc=1, device_id={"sp": low + lax.rem(part + i, owners)})

    class ToOwners:
        def __init__(self, source, target, send, recv):
            self.source, self.target, self.send, self.recv = source, target, send, recv

        def copy(self, i):
            at = lax.rem(part + i, owners)
            return low + at, pltpu.make_async_remote_copy(
                src_ref=self.source.at[at], dst_ref=self.target.at[part],
                send_sem=self.send.at[i], recv_sem=self.recv.at[part], device_id={"sp": low + at},
            )

        def start(self):
            for i in range(owners):
                to, copy = self.copy(i)
                pl.when(to != part)(copy.start)

        def take_own(self):
            self.target[part] = self.source[mine]

        def receive(self, i):
            at = lax.rem(part + parts - i, parts)
            pltpu.make_async_remote_copy(
                src_ref=self.source.at[0], dst_ref=self.target.at[at],
                send_sem=self.send.at[0], recv_sem=self.recv.at[at], device_id={"sp": left},
            ).wait_recv()

        def finish(self):
            for i in range(owners):
                to, copy = self.copy(i)
                pl.when(to != part)(copy.wait_send)

    alphas = ToOwners(snd_a, rcv_a, a_send, a_recv)
    enses = ToOwners(snd_e, rcv_e, e_send, e_recv)
    halfs = ToOwners(snd_h, rcv_h, h_send, h_recv)
    alphas.start()
    loads[1].wait()
    if ens_stage.shape[1] > halves * used:
        ens_stage[:, halves * used :, :] = jnp.zeros((owners, ens_stage.shape[1] - halves * used, LANES), F32)
    for v in range(3):
        for m in range(members):
            field = ens[m, v].astype(F32)
            for j in range(per):
                for h in range(halves):
                    at = half_row(slot_of(v, j * members + m, items, slots, spare), h, halves, used)
                    ens_stage[:, at, :] = field[j * owners : (j + 1) * owners, h * LANES : (h + 1) * LANES]
    snd_e[...] = ens_stage[...].astype(BF16)
    enses.start()

    for load in loads[2:8]:
        load.wait()
    pitch = -(-tile_rows // 8) * 8
    nx = cols * parts
    first = group * tile_rows
    row = jnp.zeros_like(cell)
    cells = cell[...]
    for r in range(1, tile_rows):
        row = row + jnp.where(cells >= (first + r) * nx, 1, 0)
    col = cells - (first + row) * nx - part * cols
    slot = step[...] * pitch + row
    observations = cells.shape[1]
    in_col = (lax.broadcasted_iota(jnp.int32, (cols, observations), 0) == col).astype(F32).astype(BF16)
    in_slot = lax.broadcasted_iota(jnp.int32, (3 * pitch, observations), 0) == slot
    obs_weight = weight[...]
    values = jnp.concatenate([
        jnp.where(in_slot, obs_weight, 0.0), jnp.where(in_slot, obs_weight * innovation[...], 0.0)
    ], axis=0)
    hi, lo = split2(values)
    summed = dot(hi, in_col, ((1,), (1,))) + dot(lo, in_col, ((1,), (1,)))
    for v in range(3):
        fields[v] = std[v] * control[v]
    for f in range(6):
        fields[3 + f] = summed[f * pitch : f * pitch + tile_rows]
    haloed = (0, 1, 2, 4, 5, 7, 8)
    lane = lax.broadcasted_iota(jnp.int32, (tile_rows, LANES), 1)
    packed = jnp.zeros((tile_rows, LANES), F32)
    for e, f in enumerate(haloed):
        ends = jnp.where(lane < LANES // 2, fields[f, :, :LANES], fields[f, :, cols - LANES :])
        window = (lane >= 2 * HALO * e) & (lane < 2 * HALO * (e + 1))
        packed = jnp.where(window, pltpu.roll(ends, (2 * HALO * e + HALO) % LANES, 1), packed)
    edge[...] = packed

    rcv_f[group] = fields[...]
    full_copies = [
        pltpu.make_async_remote_copy(
            src_ref=fields, dst_ref=rcv_f.at[group],
            send_sem=f_send.at[0, j], recv_sem=f_recv.at[0, j], device_id={"grp": lax.rem(group + j, groups)},
        )
        for j in range(1, groups)
    ]
    for copy in full_copies:
        copy.start()

    @pl.when(owner)
    def _():
        pl.semaphore_wait(here, parts - owners)
        for j in range(1, groups):
            pl.semaphore_signal(whole, inc=1, device_id={"grp": lax.rem(group + j, groups)})

    for load in loads[8:]:
        load.wait()

    def filtered(xs, exact):
        pieces = xs
        spectra = [real_dft(piece) for piece in pieces]
        res, ims = [], []
        for k1 in range(residues):
            parts_re, parts_im = [], []
            for h in range(halves):
                c = tw_c[k1 : k1 + 1, h * LANES : (h + 1) * LANES]
                s = tw_s[k1 : k1 + 1, h * LANES : (h + 1) * LANES]
                re, im = spectra[h][k1]
                if k1 == 0:
                    parts_re.append(re)
                    parts_im.append(jnp.zeros_like(re))
                elif im is None:
                    parts_re.append(re * c)
                    parts_im.append(-re * s)
                else:
                    parts_re.append(re * c + im * s)
                    parts_im.append(im * c - re * s)
            res.append(jnp.concatenate(parts_re + parts_im, axis=1))
        y_hi, y_lo = split2(jnp.concatenate(res, axis=0))
        z = dot(y_hi, fwd_hi[...])
        if exact:
            z = z + dot(y_lo, fwd_hi[...]) + dot(y_hi, fwd_lo[...])
        z = jnp.concatenate(
            [z[k1 * slots : (k1 + 1) * slots] * waves[k1 : k1 + 1, :] for k1 in range(residues)], axis=0
        )
        z_hi, z_lo = split2(z)
        v = dot(z_hi, inv_hi[...])
        if exact:
            v = v + dot(z_lo, inv_hi[...]) + dot(z_hi, inv_lo[...])
        outs = []
        for h in range(halves):
            zs = []
            for k1 in range(residues):
                c = tw_c[k1 : k1 + 1, h * LANES : (h + 1) * LANES]
                s = tw_s[k1 : k1 + 1, h * LANES : (h + 1) * LANES]
                at = slice(k1 * slots, (k1 + 1) * slots)
                re = v[at, h * LANES : (h + 1) * LANES]
                im = v[at, cols + h * LANES : cols + (h + 1) * LANES]
                zs.append((re, im) if k1 == 0 else (re * c - im * s, im * c + re * s))
            outs.append(real_sum(zs, parts))
        return outs

    at_slot = lax.broadcasted_iota(jnp.int32, (slots, cols), 0)

    def ens_rows(p, first_slot, last_slot):
        full = used // 8 * 8
        pieces = []
        for h in range(halves):
            rows_of = [rcv_e[p, h * full + first_slot : h * full + min(last_slot, full)].astype(F32)]
            if last_slot > full:
                tail = rcv_e[p, halves * full : halves * full + 8].astype(F32)
                rows_of.append(tail if h == 0 else pltpu.roll(tail, 8 - h * (used - full), 0))
            pieces.append(jnp.concatenate(rows_of, axis=0))
        return jnp.concatenate(pieces, axis=1)

    def inc_copy(i, j):
        return pltpu.make_async_remote_copy(
            src_ref=snd_i.at[i], dst_ref=rcv_i.at[group, mine],
            send_sem=i_send.at[i, j], recv_sem=i_recv.at[group, mine],
            device_id={"grp": lax.rem(group + j, groups), "sp": lax.rem(part + parts - i, parts)},
        )

    def out_copy(i):
        to = i
        return pltpu.make_async_remote_copy(
            src_ref=snd_o.at[to], dst_ref=rcv_o.at[mine],
            send_sem=o_send.at[i], recv_sem=o_recv.at[mine], device_id={"sp": to},
        )

    @pl.when(owner)
    def _():
        count = spectrum.shape[1]
        inner = count // parts
        wave = lax.broadcasted_iota(jnp.int32, (waves.shape[0], count), 1)
        residue = lax.broadcasted_iota(jnp.int32, wave.shape, 0)
        weights = jnp.broadcast_to(spectrum[...], wave.shape)
        forward = jnp.where((lax.rem(wave, parts) == residue) & (residue < residues), weights, 0.0)
        mirrored = (lax.rem(wave + residue, parts) == 0) & (residue > 0) & (residue < residues - 1)
        backward = jnp.where(mirrored, weights, 0.0)
        k = lax.broadcasted_iota(jnp.int32, (count, 4 * inner), 0)
        j = lax.rem(lax.broadcasted_iota(jnp.int32, (count, 4 * inner), 1), 2 * inner)
        ahead, behind = k - parts * (j - inner), k - parts * (inner - 1 - j)
        ahead = jnp.where((ahead >= 0) & (ahead < parts), 1.0, 0.0).astype(BF16)
        behind = jnp.where((behind >= 0) & (behind < parts), 1.0, 0.0).astype(BF16)
        f_hi, f_lo = split2(forward)
        b_hi, b_lo = split2(backward)
        waves[...] = dot(f_hi, ahead) + dot(f_lo, ahead) + dot(b_hi, behind) + dot(b_lo, behind)

        alphas.take_own()
        enses.take_own()
        for i in range(1, parts):
            alphas.receive(i)
        came = [[None] * parts for _ in range(halves)]
        for p in range(parts):
            x = rcv_a[p].astype(F32)
            for h in range(halves):
                came[h][p] = (x if h == 0 else pltpu.roll(x, x.shape[0] - h * items, 0))[:slots]
        localized = filtered(came, True)
        for p in range(parts):
            loc = jnp.concatenate([localized[h][p] for h in range(halves)], axis=1)
            loc_buf[p] = loc.astype(BF16).astype(F32)
    @pl.when(owner)
    def _():
        if groups > 1:
            pl.semaphore_wait(whole, groups - 1)
        for i in range(parts // owners):
            to = mine * (parts // owners) + i

            @pl.when(to != part)
            def _():
                pl.semaphore_signal(go, inc=1, device_id={"sp": to})

    @pl.when(part // (parts // owners) != mine)
    def _():
        pl.semaphore_wait(go, 1)

    end_copies = []
    for j in range(groups):
        for kind, at, target in ((1, right, rcv_edge.at[0, group]), (2, left, rcv_edge.at[1, group])):
            end_copies.append(pltpu.make_async_remote_copy(
                src_ref=edge, dst_ref=target, send_sem=f_send.at[kind, j], recv_sem=f_recv.at[kind, j],
                device_id={"grp": lax.rem(group + j, groups), "sp": at},
            ))
            end_copies[-1].start()
    field_copies = full_copies + end_copies

    @pl.when(owner)
    def _():
        lane = lax.broadcasted_iota(jnp.int32, (8, LANES), 1)
        at_row = lax.broadcasted_iota(jnp.int32, (8, LANES), 0)
        tiles = [None] * parts

        def increments(p):
            loc = loc_buf[p]
            a = ens_rows(p, 0, slots) * jnp.where(at_slot < items, loc, pltpu.roll(loc, items, 0))
            b = ens_rows(p, slots, 2 * slots) * jnp.where(at_slot < items, loc, pltpu.roll(loc, items - spare, 0))
            rest = total_slots - 2 * slots
            c = ens_rows(p, 2 * slots, total_slots) * loc[2 * spare : 2 * spare + rest]
            hi, lo = split2(jnp.concatenate([a, b, c], axis=0))
            return spread * dot(pick[...], jnp.concatenate([hi, lo], axis=0))

        def offset(i):
            return (i + low) % parts

        def put_increments(i):
            after, before = tiles[i - 1][:, :LANES], tiles[(i + 1) % parts][:, cols - LANES :]
            ends = jnp.where(lane < LANES // 2, after, before)
            pieces = [tiles[i][:, h * LANES : (h + 1) * LANES] for h in range(halves)]
            for v in range(3):
                window = (lane >= 2 * HALO * v) & (lane < 2 * HALO * (v + 1)) & (at_row >= 3 * per)
                moved = pltpu.roll(ends, 2 * HALO * v + HALO, 1)
                if 3 * per - per * v:
                    moved = pltpu.roll(moved, 3 * per - per * v, 0)
                pieces[0] = jnp.where(window, moved, pieces[0])
            snd_i[offset(i)] = jnp.concatenate(pieces, axis=0).astype(BF16)

        batch = owners // BATCHES
        for first_of in range(0, owners, batch):
            blocks = [i for k in range(first_of, first_of + batch) for i in (k, k + owners)]
            for i in blocks:
                if offset(i) > 0:
                    enses.receive(offset(i))
            for i in blocks:
                tiles[i] = increments(lax.rem(part + parts - offset(i), parts))
            ready = [i for k in range(first_of - 1, first_of + batch - 1) if k > 0 for i in (k, k + owners)]
            if first_of + batch == owners:
                ready += [owners - 1, parts - 1, 0, owners]
            for i in ready:
                put_increments(i)
            for i in ready:
                for j in range(groups):
                    if offset(i) + j > 0:
                        inc_copy(offset(i), j).start()
        rcv_i[group, mine] = snd_i[0]

    for copy in field_copies:
        copy.wait_recv()
    lane = lax.broadcasted_iota(jnp.int32, (tile_rows, LANES), 1)
    for g in range(groups):
        at = slice(g * tile_rows, (g + 1) * tile_rows)
        for f in range(9):
            wide[f, at, :cols] = rcv_f[g, f]
            if f in haloed:
                back = LANES - (2 * HALO * haloed.index(f) + HALO)
                before, after = (pltpu.roll(rcv_edge[side, g], back, 1) for side in (0, 1))
                wide[f, at, cols:] = jnp.where(lane < LANES // 2, after, before)
            else:
                wide[f, at, cols:] = jnp.zeros((tile_rows, LANES), F32)

    for j in range(groups):
        for k in range(owners):
            g, at = lax.rem(group + j, groups), lax.rem(part + k, owners)
            arrival = pltpu.make_async_remote_copy(
                src_ref=snd_i.at[0], dst_ref=rcv_i.at[g, at],
                send_sem=i_send.at[0, 0], recv_sem=i_recv.at[g, at], device_id={"sp": left},
            )
            if j == 0:
                pl.when(at != mine)(arrival.wait_recv)
            else:
                arrival.wait_recv()
    total = rcv_i[0].astype(F32)
    for g in range(1, groups):
        total = total + rcv_i[g].astype(F32)
    message[...] = total

    def gathered(index):
        return jnp.concatenate([message[:, index + j, :] for j in range(per)], axis=0)

    ends = gathered(3 * per)
    state0 = []
    for v in range(3):
        pieces = [gathered(8 * h + per * v) for h in range(halves)]
        pieces.append(pltpu.roll(ends, LANES - (2 * HALO * v + HALO), 1))
        state0.append(jnp.concatenate(pieces, axis=1) + wide[v])
    row_at = lax.broadcasted_iota(jnp.int32, (rows, cols + LANES), 0).astype(F32)
    rotation = 0.1 + 0.2 * (row_at + 0.5) / rows
    state1 = model_step(state0, rotation)
    state2 = model_step(state1, rotation)
    forcing = [wide[3 + t] * s[0] - wide[6 + t] for t, s in enumerate((state0, state1, state2))]
    zero = jnp.zeros_like(rotation)
    h, u, w = adjoint_step((forcing[2], zero, zero), rotation)
    h, u, w = adjoint_step((h + forcing[1], u, w), rotation)
    for v, field in enumerate((h + forcing[0], u, w)):
        field = field[:, :cols]
        adjoint[v] = field
        half = field.astype(BF16).astype(F32)
        for h in range(halves):
            for j in range(per):
                message[:, 8 * h + per * v + j, :] = half[j * owners : (j + 1) * owners, h * LANES : (h + 1) * LANES]
    snd_h[...] = message[...].astype(BF16)
    halfs.start()
    for v in range(3):
        grad_control_ref[v] = control[v] + std[v] * adjoint[v, tile, :]

    @pl.when(owner)
    def _():
        halfs.take_own()
        for i in range(1, parts):
            halfs.receive(i)
        weighted = []
        for p in range(parts):
            came_h = rcv_h[p].astype(F32)

            def row_of(v, j):
                pieces = [came_h[8 * h + per * v + j : 8 * h + per * v + j + 1] for h in range(halves)]
                return jnp.broadcast_to(jnp.concatenate(pieces, axis=1), (slots, cols))

            def field_of(v, count):
                out = row_of(v, per - 1)
                for j in reversed(range(per - 1)):
                    out = jnp.where(at_slot < (j + 1) * members, row_of(v, j), out)
                return out

            third = field_of(2, items)
            a = ens_rows(p, 0, slots) * jnp.where(at_slot < items, field_of(0, items), pltpu.roll(third, items, 0))
            b = ens_rows(p, slots, 2 * slots) * jnp.where(
                at_slot < items, field_of(1, items), pltpu.roll(third, items - spare, 0)
            )
            rest = total_slots - 2 * slots
            c = ens_rows(p, 2 * slots, total_slots) * third[2 * spare : 2 * spare + rest]
            own = jnp.concatenate([jnp.zeros((2 * spare, cols), F32), c], axis=0)[:slots]
            own = jnp.where(at_slot < 2 * spare, pltpu.roll(b, slots - (items - spare), 0), own)
            own = jnp.where(at_slot < spare, pltpu.roll(a, slots - items, 0), own)
            weighted.append(a + b + own)
        outs = filtered([[x[:, h * LANES : (h + 1) * LANES] for x in weighted] for h in range(halves)], False)
        for p in range(parts):
            for h in range(halves):
                out_stage[p, h * items : (h + 1) * items, :] = outs[h][p][:items]
            snd_o[p] = out_stage[p].astype(BF16)
        for i in range(parts):
            pl.when(part != i)(out_copy(i).start)
        rcv_o[mine] = snd_o[part]

    for k in range(owners):
        at = lax.rem(part + k, owners)
        arrival = pltpu.make_async_remote_copy(
            src_ref=snd_o.at[0], dst_ref=rcv_o.at[at],
            send_sem=o_send.at[0], recv_sem=o_recv.at[at], device_id={"sp": left},
        )
        pl.when(at != mine)(arrival.wait_recv)
    stage[...] = rcv_o[...].astype(F32)
    for m in range(members):
        for j in range(per):
            for h in range(halves):
                at, lanes = slice(j * owners, (j + 1) * owners), slice(h * LANES, (h + 1) * LANES)
                corr_ref[m, at, lanes] = alpha[m, at, lanes] + spread * stage[:, h * items + j * members + m, :]
    alphas.finish()
    enses.finish()
    halfs.finish()
    for copy in field_copies:
        copy.wait_send()

    @pl.when(owner)
    def _():
        for i in range(parts):
            for j in range(groups):
                if i + j > 0:
                    inc_copy(i, j).wait_send()
        for i in range(parts):
            pl.when(part != i)(out_copy(i).wait_send)


def finish(corr_ref, grad_control_ref, corr_out, grad_control_out, sem):
    copies = [
        pltpu.make_async_copy(corr_ref, corr_out, sem.at[0]),
        pltpu.make_async_copy(grad_control_ref, grad_control_out, sem.at[1]),
    ]
    for copy in copies:
        copy.start()
    for copy in copies:
        copy.wait()


def tables(parts, cols, waves, members, rows):
    length = parts * cols
    inner = waves // parts
    residues = parts // 2 + 1
    twist = 2 * np.pi * np.outer(np.arange(residues), np.arange(cols)) / length
    quotient = np.arange(-inner, inner)
    phase = 2 * np.pi * (np.outer(np.arange(cols), quotient) % cols) / cols
    c, s = np.cos(phase), np.sin(phase)
    forward = np.block([[c, -s], [s, c]])
    owners, per, items, slots, spare, total_slots = layout(members, rows, parts)
    pick = np.zeros((8, 2, total_slots), np.float32)
    for v in range(3):
        for j in range(per):
            for m in range(members):
                pick[v * per + j, :, slot_of(v, j * members + m, items, slots, spare)] = 1.0
    return (
        *both(forward), *both(forward.T.copy()), np.cos(twist).astype(np.float32), np.sin(twist).astype(np.float32),
        pick.reshape(8, 2 * total_slots).astype(BF16),
    )


def per_device(alpha, ensemble, static_std, control, loc_spectrum, obs_cell, obs_step, innovation, obs_weight):
    members, rows, cols = alpha.shape
    groups, parts = lax.axis_size("grp"), lax.axis_size("sp")
    spread = 1.0 / math.sqrt(members * groups - 1)
    owners, per, items, slots, spare, total_slots = layout(members, rows, parts)
    assert owners * per == rows and 4 * per <= 8 and spare % 4 == 0
    tile_rows = control.shape[1]
    halves = cols // LANES
    residues = parts // 2 + 1
    inner = loc_spectrum.shape[0] // parts
    operands = (
        alpha, ensemble, static_std, control, loc_spectrum[None],
        obs_cell[None], obs_step[None], innovation[None], obs_weight[None],
        *tables(parts, cols, loc_spectrum.shape[0], members, rows),
    )
    packed = (round8(halves * items), LANES)
    ens_packed = (round8(3 * halves * items), LANES)
    message = (8 * halves, LANES)
    vmem = pl.BlockSpec(memory_space=pltpu.VMEM)
    dma = pltpu.SemaphoreType.DMA
    corr, grad_control = pl.pallas_call(
        functools.partial(kernel, groups, parts, spread),
        out_shape=(
            pltpu.VMEM(alpha.shape, F32),
            pltpu.VMEM(control.shape, F32),
        ),
        in_specs=[HBM] * len(operands),
        out_specs=(vmem, vmem),
        scratch_shapes=[
            *[pltpu.VMEM(t.shape, t.dtype) for t in operands],
            pltpu.VMEM((owners, *packed), F32),
            pltpu.VMEM((parts, *packed), F32),
            pltpu.VMEM((owners, *ens_packed), F32),
            pltpu.VMEM((parts, slots, cols), F32),
            pltpu.VMEM((3, rows, cols), F32),
            pltpu.VMEM((round8(residues), 4 * inner), F32),
            pltpu.VMEM((9, tile_rows, cols), F32),
            pltpu.VMEM((9, rows, cols + LANES), F32),
            pltpu.VMEM((owners, *message), F32),
            pltpu.VMEM((owners, *packed), BF16), pltpu.VMEM((parts, *packed), BF16),
            pltpu.VMEM((owners, *ens_packed), BF16), pltpu.VMEM((parts, *ens_packed), BF16),
            pltpu.VMEM((parts, *message), BF16), pltpu.VMEM((groups, owners, *message), BF16),
            pltpu.VMEM((owners, *message), BF16), pltpu.VMEM((parts, *message), BF16),
            pltpu.VMEM((parts, *packed), BF16), pltpu.VMEM((owners, *packed), BF16),
            pltpu.VMEM((groups, 9, tile_rows, cols), F32),
            pltpu.VMEM((tile_rows, LANES), F32), pltpu.VMEM((2, groups, tile_rows, LANES), F32),
            dma((len(operands),)),
            dma((owners,)), dma((parts,)), dma((owners,)), dma((parts,)),
            dma((parts, groups)), dma((groups, owners)),
            dma((owners,)), dma((parts,)), dma((parts,)), dma((owners,)),
            dma((3, groups)), dma((3, groups)),
            pltpu.SemaphoreType.REGULAR, pltpu.SemaphoreType.REGULAR, pltpu.SemaphoreType.REGULAR,
        ],
        compiler_params=pltpu.CompilerParams(collective_id=0, has_side_effects=True, vmem_limit_bytes=63 << 20),
    )(*operands)
    return pl.pallas_call(
        finish,
        out_shape=(jax.ShapeDtypeStruct(alpha.shape, F32), jax.ShapeDtypeStruct(control.shape, F32)),
        in_specs=[vmem] * 2,
        out_specs=(HBM, HBM),
        scratch_shapes=[dma((2,))],
        compiler_params=pltpu.CompilerParams(vmem_limit_bytes=1 << 20),
    )(corr, grad_control)


def solution(mesh):
    flat = P(("grp", "sp"))
    tile = P(None, "grp", "sp")
    return jax.shard_map(
        per_device,
        mesh=mesh,
        in_specs=(P("grp", None, "sp"), P("grp", None, None, "sp"), tile, tile, P(), flat, flat, flat, flat),
        out_specs=(P("grp", None, "sp"), tile),
        check_vma=False,
    )
```

```python
import functools
import math

import jax
import jax.numpy as jnp
import numpy as np
from jax import lax
from jax.experimental import pallas as pl
from jax.experimental.pallas import tpu as pltpu
from jax.sharding import PartitionSpec as P

COURANT = 0.4
LANES = 128
HALO = 8
BATCHES = 4
BF16, F32 = jnp.bfloat16, jnp.float32
HBM = pl.BlockSpec(memory_space=pltpu.HBM)


def dot(a, b, contract=((1,), (0,))):
    return lax.dot_general(a, b, (contract, ((), ())), preferred_element_type=F32)


def split2(x):
    hi = x.astype(BF16)
    return hi, (x - hi.astype(F32)).astype(BF16)


def both(table):
    table = np.asarray(table, np.float32)
    hi = table.astype(BF16)
    return hi, (table - hi.astype(np.float32)).astype(BF16)


def add(a, b, sign=1.0):
    re = a[0] + b[0] if sign > 0 else a[0] - b[0]
    if b[1] is None:
        return re, a[1]
    if a[1] is None:
        return re, b[1] if sign > 0 else -b[1]
    return re, a[1] + b[1] if sign > 0 else a[1] - b[1]


def conj(a):
    return a[0], None if a[1] is None else -a[1]


def turn(a, eighths, n):
    at = (eighths % n) / n
    if at == 0:
        return a
    re, im = a
    if at == 0.25:
        return (jnp.zeros_like(re) if im is None else -im), re
    if at == 0.75:
        return (jnp.zeros_like(re) if im is None else im), -re
    c, s = math.cos(2 * math.pi * at), math.sin(2 * math.pi * at)
    if im is None:
        return c * re, s * re
    return c * re - s * im, c * im + s * re


def real_dft(xs):
    n = len(xs)
    if n == 1:
        return [(xs[0], None)]
    if n == 2:
        return [(xs[0] + xs[1], None), (xs[0] - xs[1], None)]
    half = n // 2
    even, odd = real_dft(xs[0::2]), real_dft(xs[1::2])
    out = [None] * (half + 1)
    for k in range(half // 2 + 1):
        t = turn(odd[k], -k, n)
        out[k] = add(even[k], t)
        if half - k != k:
            out[half - k] = conj(add(even[k], t, -1.0))
    return out


def real_sum(zs, n):
    if n == 1:
        return [zs[0][0]]
    if n == 2:
        return [zs[0][0] + zs[1][0], zs[0][0] - zs[1][0]]
    half = n // 2
    even, odd = [], []
    for k in range(half // 2 + 1):
        if half - k == k:
            even.append(zs[k])
            odd.append(turn(zs[k], k, n))
        else:
            other = conj(zs[half - k])
            even.append(add(zs[k], other))
            odd.append(turn(add(zs[k], other, -1.0), k, n))
    even, odd = real_sum(even, half), real_sum(odd, half)
    return [(even, odd)[p % 2][p // 2] for p in range(n)]


def dx(q):
    width = q.shape[1]
    return 0.5 * (pltpu.roll(q, width - 1, 1) - pltpu.roll(q, 1, 1))


def dy(q):
    rows = q.shape[0]
    at = lax.broadcasted_iota(jnp.int32, q.shape, 0)
    above = jnp.where(at < rows - 1, pltpu.roll(q, rows - 1, 0), 0.0)
    below = jnp.where(at > 0, pltpu.roll(q, 1, 0), 0.0)
    return 0.5 * (above - below)


def model_step(state, rotation):
    h, u, w = state
    h = h - COURANT * (dx(u) + dy(w))
    return h, u - COURANT * dx(h) + rotation * w, w - COURANT * dy(h) - rotation * u


def adjoint_step(state, rotation):
    h, u, w = state
    a = h + COURANT * (dx(u) + dy(w))
    return a, u - rotation * w + COURANT * dx(a), w + rotation * u + COURANT * dy(a)


def round8(n):
    return -(-n // 8) * 8


def layout(members, rows, parts):
    owners = parts // 2
    per = rows // owners
    items = per * members
    slots = round8(items)
    spare = slots - items
    return owners, per, items, slots, spare, 2 * slots + round8(items - 2 * spare)


def half_row(slot, half, halves, used):
    whole_rows = used // 8 * 8
    if slot < whole_rows:
        return half * whole_rows + slot
    return halves * whole_rows + half * (used - whole_rows) + slot - whole_rows


def slot_of(v, item, items, slots, spare):
    if v < 2:
        return v * slots + item
    if item < spare:
        return items + item
    if item < 2 * spare:
        return slots + items + item - spare
    return 2 * slots + item - 2 * spare


def kernel(
    groups, parts, spread,
    alpha_any, ens_any, std_any, control_any, spectrum_any, cell_any, step_any, innovation_any, weight_any,
    fwd_hi_any, fwd_lo_any, inv_hi_any, inv_lo_any, tw_c_any, tw_s_any, pick_any,
    corr_ref, grad_control_ref,
    alpha, ens, std, control, spectrum, cell, step, innovation, weight,
    fwd_hi, fwd_lo, inv_hi, inv_lo, tw_c, tw_s, pick,
    stage, out_stage, ens_stage, loc_buf, adjoint, waves, fields, wide, message,
    snd_a, rcv_a, snd_e, rcv_e, snd_i, rcv_i, snd_h, rcv_h, snd_o, rcv_o, rcv_f, edge, rcv_edge,
    load_sem, a_send, a_recv, e_send, e_recv, i_send, i_recv, h_send, h_recv, o_send, o_recv, f_send, f_recv, here, whole, go,
):
    group, part = lax.axis_index("grp"), lax.axis_index("sp")
    left, right = lax.rem(part + parts - 1, parts), lax.rem(part + 1, parts)
    members, rows, cols = alpha.shape
    tile_rows = control.shape[1]
    tile = pl.ds(pl.multiple_of(group * tile_rows, tile_rows), tile_rows)
    owners, per, items, slots, spare, total_slots = layout(members, rows, parts)
    used = 3 * items
    low = parts // 4
    mine = part - low
    owner = (part >= low) & (part < low + owners)
    halves = cols // LANES
    residues = parts // 2 + 1

    barrier = pltpu.get_barrier_semaphore()

    @pl.when(owner)
    def _():
        for i in range(1, parts):
            pl.semaphore_signal(barrier, inc=1, device_id={"sp": lax.rem(part + i, parts)})

    for j in range(1, groups):
        pl.semaphore_signal(barrier, inc=1, device_id={"grp": lax.rem(group + j, groups)})

    pairs = [
        (alpha_any, alpha), (ens_any, ens), (cell_any, cell), (step_any, step), (innovation_any, innovation),
        (weight_any, weight), (std_any, std), (control_any, control), (spectrum_any, spectrum),
        (fwd_hi_any, fwd_hi), (fwd_lo_any, fwd_lo), (inv_hi_any, inv_hi), (inv_lo_any, inv_lo),
        (tw_c_any, tw_c), (tw_s_any, tw_s), (pick_any, pick),
    ]
    loads = [pltpu.make_async_copy(a, b, load_sem.at[i]) for i, (a, b) in enumerate(pairs)]
    for load in loads:
        load.start()

    loads[0].wait()
    filled = halves * items
    if stage.shape[1] > filled:
        stage[:, filled:, :] = jnp.zeros((owners, stage.shape[1] - filled, LANES), F32)
    for m in range(members):
        for j in range(per):
            for h in range(halves):
                stage[:, h * items + j * members + m, :] = (
                    alpha[m, j * owners : (j + 1) * owners, h * LANES : (h + 1) * LANES]
                )
    snd_a[...] = stage[...].astype(BF16)

    @pl.when(owner)
    def _():
        pl.semaphore_wait(barrier, owners + groups - 2)

    @pl.when(jnp.logical_not(owner))
    def _():
        pl.semaphore_wait(barrier, owners + groups - 1)
        for i in range(owners):
            pl.semaphore_signal(here, inc=1, device_id={"sp": low + lax.rem(part + i, owners)})

    class ToOwners:
        def __init__(self, source, target, send, recv):
            self.source, self.target, self.send, self.recv = source, target, send, recv

        def copy(self, i):
            at = lax.rem(part + i, owners)
            return low + at, pltpu.make_async_remote_copy(
                src_ref=self.source.at[at], dst_ref=self.target.at[part],
                send_sem=self.send.at[i], recv_sem=self.recv.at[part], device_id={"sp": low + at},
            )

        def start(self):
            for i in range(owners):
                to, copy = self.copy(i)
                pl.when(to != part)(copy.start)

        def take_own(self):
            self.target[part] = self.source[mine]

        def receive(self, i):
            at = lax.rem(part + parts - i, parts)
            pltpu.make_async_remote_copy(
                src_ref=self.source.at[0], dst_ref=self.target.at[at],
                send_sem=self.send.at[0], recv_sem=self.recv.at[at], device_id={"sp": left},
            ).wait_recv()

        def receive_from(self, p):
            arrival = pltpu.make_async_remote_copy(
                src_ref=self.source.at[0], dst_ref=self.target.at[p],
                send_sem=self.send.at[0], recv_sem=self.recv.at[p], device_id={"sp": left},
            )
            if low <= p < low + owners:
                pl.when(part != p)(arrival.wait_recv)
            else:
                arrival.wait_recv()

        def finish(self):
            for i in range(owners):
                to, copy = self.copy(i)
                pl.when(to != part)(copy.wait_send)

    alphas = ToOwners(snd_a, rcv_a, a_send, a_recv)
    enses = ToOwners(snd_e, rcv_e, e_send, e_recv)
    halfs = ToOwners(snd_h, rcv_h, h_send, h_recv)
    alphas.start()
    loads[1].wait()
    if ens_stage.shape[1] > halves * used:
        ens_stage[:, halves * used :, :] = jnp.zeros((owners, ens_stage.shape[1] - halves * used, LANES), F32)
    for v in range(3):
        for m in range(members):
            field = ens[m, v].astype(F32)
            for j in range(per):
                for h in range(halves):
                    at = half_row(slot_of(v, j * members + m, items, slots, spare), h, halves, used)
                    ens_stage[:, at, :] = field[j * owners : (j + 1) * owners, h * LANES : (h + 1) * LANES]
    snd_e[...] = ens_stage[...].astype(BF16)
    enses.start()

    for load in loads[2:8]:
        load.wait()
    pitch = -(-tile_rows // 8) * 8
    nx = cols * parts
    first = group * tile_rows
    row = jnp.zeros_like(cell)
    cells = cell[...]
    for r in range(1, tile_rows):
        row = row + jnp.where(cells >= (first + r) * nx, 1, 0)
    col = cells - (first + row) * nx - part * cols
    slot = step[...] * pitch + row
    observations = cells.shape[1]
    in_col = (lax.broadcasted_iota(jnp.int32, (cols, observations), 0) == col).astype(F32).astype(BF16)
    in_slot = lax.broadcasted_iota(jnp.int32, (3 * pitch, observations), 0) == slot
    obs_weight = weight[...]
    values = jnp.concatenate([
        jnp.where(in_slot, obs_weight, 0.0), jnp.where(in_slot, obs_weight * innovation[...], 0.0)
    ], axis=0)
    hi, lo = split2(values)
    summed = dot(hi, in_col, ((1,), (1,))) + dot(lo, in_col, ((1,), (1,)))
    for v in range(3):
        fields[v] = std[v] * control[v]
    for f in range(6):
        fields[3 + f] = summed[f * pitch : f * pitch + tile_rows]
    haloed = (0, 1, 2, 4, 5, 7, 8)
    lane = lax.broadcasted_iota(jnp.int32, (tile_rows, LANES), 1)
    packed = jnp.zeros((tile_rows, LANES), F32)
    for e, f in enumerate(haloed):
        ends = jnp.where(lane < LANES // 2, fields[f, :, :LANES], fields[f, :, cols - LANES :])
        window = (lane >= 2 * HALO * e) & (lane < 2 * HALO * (e + 1))
        packed = jnp.where(window, pltpu.roll(ends, (2 * HALO * e + HALO) % LANES, 1), packed)
    edge[...] = packed

    rcv_f[group] = fields[...]
    full_copies = [
        pltpu.make_async_remote_copy(
            src_ref=fields, dst_ref=rcv_f.at[group],
            send_sem=f_send.at[0, j], recv_sem=f_recv.at[0, j], device_id={"grp": lax.rem(group + j, groups)},
        )
        for j in range(1, groups)
    ]
    for copy in full_copies:
        copy.start()

    @pl.when(owner)
    def _():
        pl.semaphore_wait(here, parts - owners)
        for j in range(1, groups):
            pl.semaphore_signal(whole, inc=1, device_id={"grp": lax.rem(group + j, groups)})

    for load in loads[8:]:
        load.wait()

    def filtered(xs, exact):
        pieces = xs
        spectra = [real_dft(piece) for piece in pieces]
        res, ims = [], []
        for k1 in range(residues):
            parts_re, parts_im = [], []
            for h in range(halves):
                c = tw_c[k1 : k1 + 1, h * LANES : (h + 1) * LANES]
                s = tw_s[k1 : k1 + 1, h * LANES : (h + 1) * LANES]
                re, im = spectra[h][k1]
                if k1 == 0:
                    parts_re.append(re)
                    parts_im.append(jnp.zeros_like(re))
                elif im is None:
                    parts_re.append(re * c)
                    parts_im.append(-re * s)
                else:
                    parts_re.append(re * c + im * s)
                    parts_im.append(im * c - re * s)
            res.append(jnp.concatenate(parts_re + parts_im, axis=1))
        y_hi, y_lo = split2(jnp.concatenate(res, axis=0))
        z = dot(y_hi, fwd_hi[...])
        if exact:
            z = z + dot(y_lo, fwd_hi[...]) + dot(y_hi, fwd_lo[...])
        z = jnp.concatenate(
            [z[k1 * slots : (k1 + 1) * slots] * waves[k1 : k1 + 1, :] for k1 in range(residues)], axis=0
        )
        z_hi, z_lo = split2(z)
        v = dot(z_hi, inv_hi[...])
        if exact:
            v = v + dot(z_lo, inv_hi[...]) + dot(z_hi, inv_lo[...])
        outs = []
        for h in range(halves):
            zs = []
            for k1 in range(residues):
                c = tw_c[k1 : k1 + 1, h * LANES : (h + 1) * LANES]
                s = tw_s[k1 : k1 + 1, h * LANES : (h + 1) * LANES]
                at = slice(k1 * slots, (k1 + 1) * slots)
                re = v[at, h * LANES : (h + 1) * LANES]
                im = v[at, cols + h * LANES : cols + (h + 1) * LANES]
                zs.append((re, im) if k1 == 0 else (re * c - im * s, im * c + re * s))
            outs.append(real_sum(zs, parts))
        return outs

    at_slot = lax.broadcasted_iota(jnp.int32, (slots, cols), 0)

    def ens_rows(p, first_slot, last_slot):
        full = used // 8 * 8
        pieces = []
        for h in range(halves):
            rows_of = [rcv_e[p, h * full + first_slot : h * full + min(last_slot, full)].astype(F32)]
            if last_slot > full:
                tail = rcv_e[p, halves * full : halves * full + 8].astype(F32)
                rows_of.append(tail if h == 0 else pltpu.roll(tail, 8 - h * (used - full), 0))
            pieces.append(jnp.concatenate(rows_of, axis=0))
        return jnp.concatenate(pieces, axis=1)

    def inc_copy(i, j):
        return pltpu.make_async_remote_copy(
            src_ref=snd_i.at[i], dst_ref=rcv_i.at[group, mine],
            send_sem=i_send.at[i, j], recv_sem=i_recv.at[group, mine],
            device_id={"grp": lax.rem(group + j, groups), "sp": lax.rem(part + parts - i, parts)},
        )

    def out_copy(i):
        to = i
        return pltpu.make_async_remote_copy(
            src_ref=snd_o.at[to], dst_ref=rcv_o.at[mine],
            send_sem=o_send.at[i], recv_sem=o_recv.at[mine], device_id={"sp": to},
        )

    @pl.when(owner)
    def _():
        count = spectrum.shape[1]
        inner = count // parts
        wave = lax.broadcasted_iota(jnp.int32, (waves.shape[0], count), 1)
        residue = lax.broadcasted_iota(jnp.int32, wave.shape, 0)
        weights = jnp.broadcast_to(spectrum[...], wave.shape)
        forward = jnp.where((lax.rem(wave, parts) == residue) & (residue < residues), weights, 0.0)
        mirrored = (lax.rem(wave + residue, parts) == 0) & (residue > 0) & (residue < residues - 1)
        backward = jnp.where(mirrored, weights, 0.0)
        k = lax.broadcasted_iota(jnp.int32, (count, 4 * inner), 0)
        j = lax.rem(lax.broadcasted_iota(jnp.int32, (count, 4 * inner), 1), 2 * inner)
        ahead, behind = k - parts * (j - inner), k - parts * (inner - 1 - j)
        ahead = jnp.where((ahead >= 0) & (ahead < parts), 1.0, 0.0).astype(BF16)
        behind = jnp.where((behind >= 0) & (behind < parts), 1.0, 0.0).astype(BF16)
        f_hi, f_lo = split2(forward)
        b_hi, b_lo = split2(backward)
        waves[...] = dot(f_hi, ahead) + dot(f_lo, ahead) + dot(b_hi, behind) + dot(b_lo, behind)

        alphas.take_own()
        enses.take_own()
        for i in range(1, parts):
            alphas.receive(i)
        came = [[None] * parts for _ in range(halves)]
        for p in range(parts):
            x = rcv_a[p].astype(F32)
            for h in range(halves):
                came[h][p] = (x if h == 0 else pltpu.roll(x, x.shape[0] - h * items, 0))[:slots]
        localized = filtered(came, True)
        for p in range(parts):
            loc = jnp.concatenate([localized[h][p] for h in range(halves)], axis=1)
            loc_buf[p] = loc.astype(BF16).astype(F32)
    @pl.when(owner)
    def _():
        if groups > 1:
            pl.semaphore_wait(whole, groups - 1)
        for i in range(parts // owners):
            to = mine * (parts // owners) + i

            @pl.when(to != part)
            def _():
                pl.semaphore_signal(go, inc=1, device_id={"sp": to})

    @pl.when(part // (parts // owners) != mine)
    def _():
        pl.semaphore_wait(go, 1)

    end_copies = []
    for j in range(groups):
        for kind, at, target in ((1, right, rcv_edge.at[0, group]), (2, left, rcv_edge.at[1, group])):
            end_copies.append(pltpu.make_async_remote_copy(
                src_ref=edge, dst_ref=target, send_sem=f_send.at[kind, j], recv_sem=f_recv.at[kind, j],
                device_id={"grp": lax.rem(group + j, groups), "sp": at},
            ))
            end_copies[-1].start()
    field_copies = full_copies + end_copies

    @pl.when(owner)
    def _():
        lane = lax.broadcasted_iota(jnp.int32, (8, LANES), 1)
        at_row = lax.broadcasted_iota(jnp.int32, (8, LANES), 0)
        tiles = [None] * parts

        def increments(p):
            loc = loc_buf[p]
            a = ens_rows(p, 0, slots) * jnp.where(at_slot < items, loc, pltpu.roll(loc, items, 0))
            b = ens_rows(p, slots, 2 * slots) * jnp.where(at_slot < items, loc, pltpu.roll(loc, items - spare, 0))
            rest = total_slots - 2 * slots
            c = ens_rows(p, 2 * slots, total_slots) * loc[2 * spare : 2 * spare + rest]
            hi, lo = split2(jnp.concatenate([a, b, c], axis=0))
            return spread * dot(pick[...], jnp.concatenate([hi, lo], axis=0))

        def offset(i):
            return (i + low) % parts

        def put_increments(i):
            after, before = tiles[i - 1][:, :LANES], tiles[(i + 1) % parts][:, cols - LANES :]
            ends = jnp.where(lane < LANES // 2, after, before)
            pieces = [tiles[i][:, h * LANES : (h + 1) * LANES] for h in range(halves)]
            for v in range(3):
                window = (lane >= 2 * HALO * v) & (lane < 2 * HALO * (v + 1)) & (at_row >= 3 * per)
                moved = pltpu.roll(ends, 2 * HALO * v + HALO, 1)
                if 3 * per - per * v:
                    moved = pltpu.roll(moved, 3 * per - per * v, 0)
                pieces[0] = jnp.where(window, moved, pieces[0])
            snd_i[offset(i)] = jnp.concatenate(pieces, axis=0).astype(BF16)

        batch = owners // BATCHES
        for first_of in range(0, owners, batch):
            blocks = [i for k in range(first_of, first_of + batch) for i in (k, k + owners)]
            for i in blocks:
                if offset(i) > 0:
                    enses.receive(offset(i))
            for i in blocks:
                tiles[i] = increments(lax.rem(part + parts - offset(i), parts))
            ready = [i for k in range(first_of - 1, first_of + batch - 1) if k > 0 for i in (k, k + owners)]
            if first_of + batch == owners:
                ready += [owners - 1, parts - 1, 0, owners]
            for i in ready:
                put_increments(i)
            for i in ready:
                for j in range(groups):
                    if offset(i) + j > 0:
                        inc_copy(offset(i), j).start()
        rcv_i[group, mine] = snd_i[0]

    for copy in field_copies:
        copy.wait_recv()
    lane = lax.broadcasted_iota(jnp.int32, (tile_rows, LANES), 1)
    for g in range(groups):
        at = slice(g * tile_rows, (g + 1) * tile_rows)
        for f in range(9):
            wide[f, at, :cols] = rcv_f[g, f]
            if f in haloed:
                back = LANES - (2 * HALO * haloed.index(f) + HALO)
                before, after = (pltpu.roll(rcv_edge[side, g], back, 1) for side in (0, 1))
                wide[f, at, cols:] = jnp.where(lane < LANES // 2, after, before)
            else:
                wide[f, at, cols:] = jnp.zeros((tile_rows, LANES), F32)

    row_at = lax.broadcasted_iota(jnp.int32, (rows, cols + LANES), 0).astype(F32)
    rotation = 0.1 + 0.2 * (row_at + 0.5) / rows
    for j in range(groups):
        for k in range(owners):
            g, at = lax.rem(group + j, groups), lax.rem(part + k, owners)
            arrival = pltpu.make_async_remote_copy(
                src_ref=snd_i.at[0], dst_ref=rcv_i.at[g, at],
                send_sem=i_send.at[0, 0], recv_sem=i_recv.at[g, at], device_id={"sp": left},
            )
            if j == 0:
                pl.when(at != mine)(arrival.wait_recv)
            else:
                arrival.wait_recv()
    total = rcv_i[0].astype(F32)
    for g in range(1, groups):
        total = total + rcv_i[g].astype(F32)
    message[...] = total

    def gathered(index):
        return jnp.concatenate([message[:, index + j, :] for j in range(per)], axis=0)

    ends = gathered(3 * per)
    state0 = []
    for v in range(3):
        pieces = [gathered(8 * h + per * v) for h in range(halves)]
        pieces.append(pltpu.roll(ends, LANES - (2 * HALO * v + HALO), 1))
        state0.append(jnp.concatenate(pieces, axis=1) + wide[v])
    state1 = model_step(state0, rotation)
    state2 = model_step(state1, rotation)
    forcing = [wide[3 + t] * s[0] - wide[6 + t] for t, s in enumerate((state0, state1, state2))]
    h, u, w = forcing[2], COURANT * dx(forcing[2]), COURANT * dy(forcing[2])
    h, u, w = adjoint_step((h + forcing[1], u, w), rotation)
    for v, field in enumerate((h + forcing[0], u, w)):
        field = field[:, :cols]
        adjoint[v] = field
        half = field.astype(BF16).astype(F32)
        for h in range(halves):
            for j in range(per):
                message[:, 8 * h + per * v + j, :] = half[j * owners : (j + 1) * owners, h * LANES : (h + 1) * LANES]
    snd_h[...] = message[...].astype(BF16)
    halfs.start()
    for v in range(3):
        grad_control_ref[v] = control[v] + std[v] * adjoint[v, tile, :]

    @pl.when(owner)
    def _():
        halfs.take_own()
        weighted = [None] * parts
        middle = range(low, low + owners)
        for p in middle:
            halfs.receive_from(p)
        for p in [*middle, *[p for p in range(parts) if p not in middle]]:
            if p == 0:
                for other in range(parts):
                    if other not in middle:
                        halfs.receive_from(other)
            came_h = rcv_h[p].astype(F32)

            def row_of(v, j):
                pieces = [came_h[8 * h + per * v + j : 8 * h + per * v + j + 1] for h in range(halves)]
                return jnp.broadcast_to(jnp.concatenate(pieces, axis=1), (slots, cols))

            def field_of(v, count):
                out = row_of(v, per - 1)
                for j in reversed(range(per - 1)):
                    out = jnp.where(at_slot < (j + 1) * members, row_of(v, j), out)
                return out

            third = field_of(2, items)
            a = ens_rows(p, 0, slots) * jnp.where(at_slot < items, field_of(0, items), pltpu.roll(third, items, 0))
            b = ens_rows(p, slots, 2 * slots) * jnp.where(
                at_slot < items, field_of(1, items), pltpu.roll(third, items - spare, 0)
            )
            rest = total_slots - 2 * slots
            c = ens_rows(p, 2 * slots, total_slots) * third[2 * spare : 2 * spare + rest]
            own = jnp.concatenate([jnp.zeros((2 * spare, cols), F32), c], axis=0)[:slots]
            own = jnp.where(at_slot < 2 * spare, pltpu.roll(b, slots - (items - spare), 0), own)
            own = jnp.where(at_slot < spare, pltpu.roll(a, slots - items, 0), own)
            weighted[p] = a + b + own
        outs = filtered([[x[:, h * LANES : (h + 1) * LANES] for x in weighted] for h in range(halves)], False)
        for p in range(parts):
            for h in range(halves):
                out_stage[p, h * items : (h + 1) * items, :] = outs[h][p][:items]
            snd_o[p] = out_stage[p].astype(BF16)
        for i in range(parts):
            pl.when(part != i)(out_copy(i).start)
        rcv_o[mine] = snd_o[part]

    for k in range(owners):
        at = lax.rem(part + k, owners)
        arrival = pltpu.make_async_remote_copy(
            src_ref=snd_o.at[0], dst_ref=rcv_o.at[at],
            send_sem=o_send.at[0], recv_sem=o_recv.at[at], device_id={"sp": left},
        )
        pl.when(at != mine)(arrival.wait_recv)
        stage[at] = rcv_o[at].astype(F32)
    for m in range(members):
        for j in range(per):
            for h in range(halves):
                at, lanes = slice(j * owners, (j + 1) * owners), slice(h * LANES, (h + 1) * LANES)
                corr_ref[m, at, lanes] = alpha[m, at, lanes] + spread * stage[:, h * items + j * members + m, :]
    alphas.finish()
    enses.finish()
    halfs.finish()
    for copy in field_copies:
        copy.wait_send()

    @pl.when(owner)
    def _():
        for i in range(parts):
            for j in range(groups):
                if i + j > 0:
                    inc_copy(i, j).wait_send()
        for i in range(parts):
            pl.when(part != i)(out_copy(i).wait_send)


def finish(corr_ref, grad_control_ref, corr_out, grad_control_out, sem):
    copies = [
        pltpu.make_async_copy(corr_ref, corr_out, sem.at[0]),
        pltpu.make_async_copy(grad_control_ref, grad_control_out, sem.at[1]),
    ]
    for copy in copies:
        copy.start()
    for copy in copies:
        copy.wait()


def tables(parts, cols, waves, members, rows):
    length = parts * cols
    inner = waves // parts
    residues = parts // 2 + 1
    twist = 2 * np.pi * np.outer(np.arange(residues), np.arange(cols)) / length
    quotient = np.arange(-inner, inner)
    phase = 2 * np.pi * (np.outer(np.arange(cols), quotient) % cols) / cols
    c, s = np.cos(phase), np.sin(phase)
    forward = np.block([[c, -s], [s, c]])
    owners, per, items, slots, spare, total_slots = layout(members, rows, parts)
    pick = np.zeros((8, 2, total_slots), np.float32)
    for v in range(3):
        for j in range(per):
            for m in range(members):
                pick[v * per + j, :, slot_of(v, j * members + m, items, slots, spare)] = 1.0
    return (
        *both(forward), *both(forward.T.copy()), np.cos(twist).astype(np.float32), np.sin(twist).astype(np.float32),
        pick.reshape(8, 2 * total_slots).astype(BF16),
    )


def per_device(alpha, ensemble, static_std, control, loc_spectrum, obs_cell, obs_step, innovation, obs_weight):
    members, rows, cols = alpha.shape
    groups, parts = lax.axis_size("grp"), lax.axis_size("sp")
    spread = 1.0 / math.sqrt(members * groups - 1)
    owners, per, items, slots, spare, total_slots = layout(members, rows, parts)
    assert owners * per == rows and 4 * per <= 8 and spare % 4 == 0
    tile_rows = control.shape[1]
    halves = cols // LANES
    residues = parts // 2 + 1
    inner = loc_spectrum.shape[0] // parts
    operands = (
        alpha, ensemble, static_std, control, loc_spectrum[None],
        obs_cell[None], obs_step[None], innovation[None], obs_weight[None],
        *tables(parts, cols, loc_spectrum.shape[0], members, rows),
    )
    packed = (round8(halves * items), LANES)
    ens_packed = (round8(3 * halves * items), LANES)
    message = (8 * halves, LANES)
    vmem = pl.BlockSpec(memory_space=pltpu.VMEM)
    dma = pltpu.SemaphoreType.DMA
    corr, grad_control = pl.pallas_call(
        functools.partial(kernel, groups, parts, spread),
        out_shape=(
            pltpu.VMEM(alpha.shape, F32),
            pltpu.VMEM(control.shape, F32),
        ),
        in_specs=[HBM] * len(operands),
        out_specs=(vmem, vmem),
        scratch_shapes=[
            *[pltpu.VMEM(t.shape, t.dtype) for t in operands],
            pltpu.VMEM((owners, *packed), F32),
            pltpu.VMEM((parts, *packed), F32),
            pltpu.VMEM((owners, *ens_packed), F32),
            pltpu.VMEM((parts, slots, cols), F32),
            pltpu.VMEM((3, rows, cols), F32),
            pltpu.VMEM((round8(residues), 4 * inner), F32),
            pltpu.VMEM((9, tile_rows, cols), F32),
            pltpu.VMEM((9, rows, cols + LANES), F32),
            pltpu.VMEM((owners, *message), F32),
            pltpu.VMEM((owners, *packed), BF16), pltpu.VMEM((parts, *packed), BF16),
            pltpu.VMEM((owners, *ens_packed), BF16), pltpu.VMEM((parts, *ens_packed), BF16),
            pltpu.VMEM((parts, *message), BF16), pltpu.VMEM((groups, owners, *message), BF16),
            pltpu.VMEM((owners, *message), BF16), pltpu.VMEM((parts, *message), BF16),
            pltpu.VMEM((parts, *packed), BF16), pltpu.VMEM((owners, *packed), BF16),
            pltpu.VMEM((groups, 9, tile_rows, cols), F32),
            pltpu.VMEM((tile_rows, LANES), F32), pltpu.VMEM((2, groups, tile_rows, LANES), F32),
            dma((len(operands),)),
            dma((owners,)), dma((parts,)), dma((owners,)), dma((parts,)),
            dma((parts, groups)), dma((groups, owners)),
            dma((owners,)), dma((parts,)), dma((parts,)), dma((owners,)),
            dma((3, groups)), dma((3, groups)),
            pltpu.SemaphoreType.REGULAR, pltpu.SemaphoreType.REGULAR, pltpu.SemaphoreType.REGULAR,
        ],
        compiler_params=pltpu.CompilerParams(collective_id=0, has_side_effects=True, vmem_limit_bytes=63 << 20),
    )(*operands)
    return pl.pallas_call(
        finish,
        out_shape=(jax.ShapeDtypeStruct(alpha.shape, F32), jax.ShapeDtypeStruct(control.shape, F32)),
        in_specs=[vmem] * 2,
        out_specs=(HBM, HBM),
        scratch_shapes=[dma((2,))],
        compiler_params=pltpu.CompilerParams(vmem_limit_bytes=1 << 20),
    )(corr, grad_control)


def solution(mesh):
    flat = P(("grp", "sp"))
    tile = P(None, "grp", "sp")
    return jax.shard_map(
        per_device,
        mesh=mesh,
        in_specs=(P("grp", None, "sp"), P("grp", None, None, "sp"), tile, tile, P(), flat, flat, flat, flat),
        out_specs=(P("grp", None, "sp"), tile),
        check_vma=False,
    )
```

```python
import functools
import math

import jax
import jax.numpy as jnp
import numpy as np
from jax import lax
from jax.experimental import pallas as pl
from jax.experimental.pallas import tpu as pltpu
from jax.sharding import PartitionSpec as P

COURANT = 0.4
LANES = 128
HALO = 8
BATCHES = 4
BF16, F32 = jnp.bfloat16, jnp.float32
HBM = pl.BlockSpec(memory_space=pltpu.HBM)


def dot(a, b, contract=((1,), (0,))):
    return lax.dot_general(a, b, (contract, ((), ())), preferred_element_type=F32)


def split2(x):
    hi = x.astype(BF16)
    return hi, (x - hi.astype(F32)).astype(BF16)


def both(table):
    table = np.asarray(table, np.float32)
    hi = table.astype(BF16)
    return hi, (table - hi.astype(np.float32)).astype(BF16)


def add(a, b, sign=1.0):
    re = a[0] + b[0] if sign > 0 else a[0] - b[0]
    if b[1] is None:
        return re, a[1]
    if a[1] is None:
        return re, b[1] if sign > 0 else -b[1]
    return re, a[1] + b[1] if sign > 0 else a[1] - b[1]


def conj(a):
    return a[0], None if a[1] is None else -a[1]


def turn(a, eighths, n):
    at = (eighths % n) / n
    if at == 0:
        return a
    re, im = a
    if at == 0.25:
        return (jnp.zeros_like(re) if im is None else -im), re
    if at == 0.75:
        return (jnp.zeros_like(re) if im is None else im), -re
    c, s = math.cos(2 * math.pi * at), math.sin(2 * math.pi * at)
    if im is None:
        return c * re, s * re
    return c * re - s * im, c * im + s * re


def real_dft(xs):
    n = len(xs)
    if n == 1:
        return [(xs[0], None)]
    if n == 2:
        return [(xs[0] + xs[1], None), (xs[0] - xs[1], None)]
    half = n // 2
    even, odd = real_dft(xs[0::2]), real_dft(xs[1::2])
    out = [None] * (half + 1)
    for k in range(half // 2 + 1):
        t = turn(odd[k], -k, n)
        out[k] = add(even[k], t)
        if half - k != k:
            out[half - k] = conj(add(even[k], t, -1.0))
    return out


def real_sum(zs, n):
    if n == 1:
        return [zs[0][0]]
    if n == 2:
        return [zs[0][0] + zs[1][0], zs[0][0] - zs[1][0]]
    half = n // 2
    even, odd = [], []
    for k in range(half // 2 + 1):
        if half - k == k:
            even.append(zs[k])
            odd.append(turn(zs[k], k, n))
        else:
            other = conj(zs[half - k])
            even.append(add(zs[k], other))
            odd.append(turn(add(zs[k], other, -1.0), k, n))
    even, odd = real_sum(even, half), real_sum(odd, half)
    return [(even, odd)[p % 2][p // 2] for p in range(n)]


def dx(q):
    width = q.shape[1]
    return 0.5 * (pltpu.roll(q, width - 1, 1) - pltpu.roll(q, 1, 1))


def dy(q):
    rows = q.shape[0]
    at = lax.broadcasted_iota(jnp.int32, q.shape, 0)
    above = jnp.where(at < rows - 1, pltpu.roll(q, rows - 1, 0), 0.0)
    below = jnp.where(at > 0, pltpu.roll(q, 1, 0), 0.0)
    return 0.5 * (above - below)


def model_step(state, rotation):
    h, u, w = state
    h = h - COURANT * (dx(u) + dy(w))
    return h, u - COURANT * dx(h) + rotation * w, w - COURANT * dy(h) - rotation * u


def adjoint_step(state, rotation):
    h, u, w = state
    a = h + COURANT * (dx(u) + dy(w))
    return a, u - rotation * w + COURANT * dx(a), w + rotation * u + COURANT * dy(a)


def round8(n):
    return -(-n // 8) * 8


def layout(members, rows, parts):
    owners = parts // 2
    per = rows // owners
    items = per * members
    slots = round8(items)
    spare = slots - items
    return owners, per, items, slots, spare, 2 * slots + round8(items - 2 * spare)


def half_row(slot, half, halves, used):
    whole_rows = used // 8 * 8
    if slot < whole_rows:
        return half * whole_rows + slot
    return halves * whole_rows + half * (used - whole_rows) + slot - whole_rows


def slot_of(v, item, items, slots, spare):
    if v < 2:
        return v * slots + item
    if item < spare:
        return items + item
    if item < 2 * spare:
        return slots + items + item - spare
    return 2 * slots + item - 2 * spare


def kernel(
    groups, parts, spread,
    alpha_any, ens_any, std_any, control_any, spectrum_any, cell_any, step_any, innovation_any, weight_any,
    fwd_hi_any, fwd_lo_any, inv_hi_any, inv_lo_any, tw_c_any, tw_s_any, pick_any,
    corr_ref, grad_control_ref,
    alpha, ens, std, control, spectrum, cell, step, innovation, weight,
    fwd_hi, fwd_lo, inv_hi, inv_lo, tw_c, tw_s, pick,
    stage, out_stage, ens_stage, loc_buf, adjoint, waves, fields, wide, message,
    snd_a, rcv_a, snd_e, rcv_e, snd_i, rcv_i, snd_h, rcv_h, snd_o, rcv_o, rcv_f, edge, rcv_edge,
    load_sem, a_send, a_recv, e_send, e_recv, i_send, i_recv, h_send, h_recv, o_send, o_recv, f_send, f_recv, here, whole, go,
):
    group, part = lax.axis_index("grp"), lax.axis_index("sp")
    left, right = lax.rem(part + parts - 1, parts), lax.rem(part + 1, parts)
    members, rows, cols = alpha.shape
    tile_rows = control.shape[1]
    tile = pl.ds(pl.multiple_of(group * tile_rows, tile_rows), tile_rows)
    owners, per, items, slots, spare, total_slots = layout(members, rows, parts)
    used = 3 * items
    low = parts // 4
    mine = part - low
    owner = (part >= low) & (part < low + owners)
    halves = cols // LANES
    residues = parts // 2 + 1

    barrier = pltpu.get_barrier_semaphore()

    @pl.when(owner)
    def _():
        for i in range(1, parts):
            pl.semaphore_signal(barrier, inc=1, device_id={"sp": lax.rem(part + i, parts)})

    for j in range(1, groups):
        pl.semaphore_signal(barrier, inc=1, device_id={"grp": lax.rem(group + j, groups)})

    pairs = [
        (alpha_any, alpha), (ens_any, ens), (cell_any, cell), (step_any, step), (innovation_any, innovation),
        (weight_any, weight), (std_any, std), (control_any, control), (spectrum_any, spectrum),
        (fwd_hi_any, fwd_hi), (fwd_lo_any, fwd_lo), (inv_hi_any, inv_hi), (inv_lo_any, inv_lo),
        (tw_c_any, tw_c), (tw_s_any, tw_s), (pick_any, pick),
    ]
    loads = [pltpu.make_async_copy(a, b, load_sem.at[i]) for i, (a, b) in enumerate(pairs)]
    for load in loads:
        load.start()

    loads[0].wait()
    filled = halves * items
    if stage.shape[1] > filled:
        stage[:, filled:, :] = jnp.zeros((owners, stage.shape[1] - filled, LANES), F32)
    for m in range(members):
        for j in range(per):
            for h in range(halves):
                stage[:, h * items + j * members + m, :] = (
                    alpha[m, j * owners : (j + 1) * owners, h * LANES : (h + 1) * LANES]
                )
    snd_a[...] = stage[...].astype(BF16)

    loads[1].wait()
    if ens_stage.shape[1] > halves * used:
        ens_stage[:, halves * used :, :] = jnp.zeros((owners, ens_stage.shape[1] - halves * used, LANES), F32)
    for v in range(3):
        for m in range(members):
            field = ens[m, v].astype(F32)
            for j in range(per):
                for h in range(halves):
                    at = half_row(slot_of(v, j * members + m, items, slots, spare), h, halves, used)
                    ens_stage[:, at, :] = field[j * owners : (j + 1) * owners, h * LANES : (h + 1) * LANES]
    snd_e[...] = ens_stage[...].astype(BF16)
    @pl.when(owner)
    def _():
        pl.semaphore_wait(barrier, owners + groups - 2)

    @pl.when(jnp.logical_not(owner))
    def _():
        pl.semaphore_wait(barrier, owners + groups - 1)
        for i in range(owners):
            pl.semaphore_signal(here, inc=1, device_id={"sp": low + lax.rem(part + i, owners)})

    class ToOwners:
        def __init__(self, source, target, send, recv):
            self.source, self.target, self.send, self.recv = source, target, send, recv

        def copy(self, i):
            at = lax.rem(part + i, owners)
            return low + at, pltpu.make_async_remote_copy(
                src_ref=self.source.at[at], dst_ref=self.target.at[part],
                send_sem=self.send.at[i], recv_sem=self.recv.at[part], device_id={"sp": low + at},
            )

        def start(self):
            for i in range(owners):
                to, copy = self.copy(i)
                pl.when(to != part)(copy.start)

        def take_own(self):
            self.target[part] = self.source[mine]

        def receive(self, i):
            at = lax.rem(part + parts - i, parts)
            pltpu.make_async_remote_copy(
                src_ref=self.source.at[0], dst_ref=self.target.at[at],
                send_sem=self.send.at[0], recv_sem=self.recv.at[at], device_id={"sp": left},
            ).wait_recv()

        def receive_from(self, p):
            arrival = pltpu.make_async_remote_copy(
                src_ref=self.source.at[0], dst_ref=self.target.at[p],
                send_sem=self.send.at[0], recv_sem=self.recv.at[p], device_id={"sp": left},
            )
            if low <= p < low + owners:
                pl.when(part != p)(arrival.wait_recv)
            else:
                arrival.wait_recv()

        def finish(self):
            for i in range(owners):
                to, copy = self.copy(i)
                pl.when(to != part)(copy.wait_send)

    alphas = ToOwners(snd_a, rcv_a, a_send, a_recv)
    enses = ToOwners(snd_e, rcv_e, e_send, e_recv)
    halfs = ToOwners(snd_h, rcv_h, h_send, h_recv)
    alphas.start()
    enses.start()

    for load in loads[2:8]:
        load.wait()
    pitch = -(-tile_rows // 8) * 8
    nx = cols * parts
    first = group * tile_rows
    row = jnp.zeros_like(cell)
    cells = cell[...]
    for r in range(1, tile_rows):
        row = row + jnp.where(cells >= (first + r) * nx, 1, 0)
    col = cells - (first + row) * nx - part * cols
    slot = step[...] * pitch + row
    observations = cells.shape[1]
    in_col = (lax.broadcasted_iota(jnp.int32, (cols, observations), 0) == col).astype(F32).astype(BF16)
    in_slot = lax.broadcasted_iota(jnp.int32, (3 * pitch, observations), 0) == slot
    obs_weight = weight[...]
    values = jnp.concatenate([
        jnp.where(in_slot, obs_weight, 0.0), jnp.where(in_slot, obs_weight * innovation[...], 0.0)
    ], axis=0)
    hi, lo = split2(values)
    summed = dot(hi, in_col, ((1,), (1,))) + dot(lo, in_col, ((1,), (1,)))
    for v in range(3):
        fields[v] = std[v] * control[v]
    for f in range(6):
        fields[3 + f] = summed[f * pitch : f * pitch + tile_rows]
    haloed = (0, 1, 2, 4, 5, 7, 8)
    lane = lax.broadcasted_iota(jnp.int32, (tile_rows, LANES), 1)
    packed = jnp.zeros((tile_rows, LANES), F32)
    for e, f in enumerate(haloed):
        ends = jnp.where(lane < LANES // 2, fields[f, :, :LANES], fields[f, :, cols - LANES :])
        window = (lane >= 2 * HALO * e) & (lane < 2 * HALO * (e + 1))
        packed = jnp.where(window, pltpu.roll(ends, (2 * HALO * e + HALO) % LANES, 1), packed)
    edge[...] = packed

    rcv_f[group] = fields[...]
    full_copies = [
        pltpu.make_async_remote_copy(
            src_ref=fields, dst_ref=rcv_f.at[group],
            send_sem=f_send.at[0, j], recv_sem=f_recv.at[0, j], device_id={"grp": lax.rem(group + j, groups)},
        )
        for j in range(1, groups)
    ]
    for copy in full_copies:
        copy.start()

    @pl.when(owner)
    def _():
        pl.semaphore_wait(here, parts - owners)
        for j in range(1, groups):
            pl.semaphore_signal(whole, inc=1, device_id={"grp": lax.rem(group + j, groups)})

    for load in loads[8:]:
        load.wait()

    def filtered(xs, exact):
        pieces = xs
        spectra = [real_dft(piece) for piece in pieces]
        res, ims = [], []
        for k1 in range(residues):
            parts_re, parts_im = [], []
            for h in range(halves):
                c = tw_c[k1 : k1 + 1, h * LANES : (h + 1) * LANES]
                s = tw_s[k1 : k1 + 1, h * LANES : (h + 1) * LANES]
                re, im = spectra[h][k1]
                if k1 == 0:
                    parts_re.append(re)
                    parts_im.append(jnp.zeros_like(re))
                elif im is None:
                    parts_re.append(re * c)
                    parts_im.append(-re * s)
                else:
                    parts_re.append(re * c + im * s)
                    parts_im.append(im * c - re * s)
            res.append(jnp.concatenate(parts_re + parts_im, axis=1))
        y_hi, y_lo = split2(jnp.concatenate(res, axis=0))
        z = dot(y_hi, fwd_hi[...])
        if exact:
            z = z + dot(y_lo, fwd_hi[...]) + dot(y_hi, fwd_lo[...])
        z = jnp.concatenate(
            [z[k1 * slots : (k1 + 1) * slots] * waves[k1 : k1 + 1, :] for k1 in range(residues)], axis=0
        )
        z_hi, z_lo = split2(z)
        v = dot(z_hi, inv_hi[...])
        if exact:
            v = v + dot(z_lo, inv_hi[...]) + dot(z_hi, inv_lo[...])
        outs = []
        for h in range(halves):
            zs = []
            for k1 in range(residues):
                c = tw_c[k1 : k1 + 1, h * LANES : (h + 1) * LANES]
                s = tw_s[k1 : k1 + 1, h * LANES : (h + 1) * LANES]
                at = slice(k1 * slots, (k1 + 1) * slots)
                re = v[at, h * LANES : (h + 1) * LANES]
                im = v[at, cols + h * LANES : cols + (h + 1) * LANES]
                zs.append((re, im) if k1 == 0 else (re * c - im * s, im * c + re * s))
            outs.append(real_sum(zs, parts))
        return outs

    at_slot = lax.broadcasted_iota(jnp.int32, (slots, cols), 0)

    def ens_rows(p, first_slot, last_slot):
        full = used // 8 * 8
        pieces = []
        for h in range(halves):
            rows_of = [rcv_e[p, h * full + first_slot : h * full + min(last_slot, full)].astype(F32)]
            if last_slot > full:
                tail = rcv_e[p, halves * full : halves * full + 8].astype(F32)
                rows_of.append(tail if h == 0 else pltpu.roll(tail, 8 - h * (used - full), 0))
            pieces.append(jnp.concatenate(rows_of, axis=0))
        return jnp.concatenate(pieces, axis=1)

    def inc_copy(i, j):
        return pltpu.make_async_remote_copy(
            src_ref=snd_i.at[i], dst_ref=rcv_i.at[group, mine],
            send_sem=i_send.at[i, j], recv_sem=i_recv.at[group, mine],
            device_id={"grp": lax.rem(group + j, groups), "sp": lax.rem(part + parts - i, parts)},
        )

    def out_copy(i):
        to = i
        return pltpu.make_async_remote_copy(
            src_ref=snd_o.at[to], dst_ref=rcv_o.at[mine],
            send_sem=o_send.at[i], recv_sem=o_recv.at[mine], device_id={"sp": to},
        )

    @pl.when(owner)
    def _():
        count = spectrum.shape[1]
        inner = count // parts
        wave = lax.broadcasted_iota(jnp.int32, (waves.shape[0], count), 1)
        residue = lax.broadcasted_iota(jnp.int32, wave.shape, 0)
        weights = jnp.broadcast_to(spectrum[...], wave.shape)
        forward = jnp.where((lax.rem(wave, parts) == residue) & (residue < residues), weights, 0.0)
        mirrored = (lax.rem(wave + residue, parts) == 0) & (residue > 0) & (residue < residues - 1)
        backward = jnp.where(mirrored, weights, 0.0)
        k = lax.broadcasted_iota(jnp.int32, (count, 4 * inner), 0)
        j = lax.rem(lax.broadcasted_iota(jnp.int32, (count, 4 * inner), 1), 2 * inner)
        ahead, behind = k - parts * (j - inner), k - parts * (inner - 1 - j)
        ahead = jnp.where((ahead >= 0) & (ahead < parts), 1.0, 0.0).astype(BF16)
        behind = jnp.where((behind >= 0) & (behind < parts), 1.0, 0.0).astype(BF16)
        f_hi, f_lo = split2(forward)
        b_hi, b_lo = split2(backward)
        waves[...] = dot(f_hi, ahead) + dot(f_lo, ahead) + dot(b_hi, behind) + dot(b_lo, behind)

        alphas.take_own()
        enses.take_own()
        for i in range(1, parts):
            alphas.receive(i)
        came = [[None] * parts for _ in range(halves)]
        for p in range(parts):
            x = rcv_a[p].astype(F32)
            for h in range(halves):
                came[h][p] = (x if h == 0 else pltpu.roll(x, x.shape[0] - h * items, 0))[:slots]
        localized = filtered(came, True)
        for p in range(parts):
            loc = jnp.concatenate([localized[h][p] for h in range(halves)], axis=1)
            loc_buf[p] = loc.astype(BF16).astype(F32)
    @pl.when(owner)
    def _():
        if groups > 1:
            pl.semaphore_wait(whole, groups - 1)
        for i in range(parts // owners):
            to = mine * (parts // owners) + i

            @pl.when(to != part)
            def _():
                pl.semaphore_signal(go, inc=1, device_id={"sp": to})

    @pl.when(part // (parts // owners) != mine)
    def _():
        pl.semaphore_wait(go, 1)

    end_copies = []
    for j in range(groups):
        for kind, at, target in ((1, right, rcv_edge.at[0, group]), (2, left, rcv_edge.at[1, group])):
            end_copies.append(pltpu.make_async_remote_copy(
                src_ref=edge, dst_ref=target, send_sem=f_send.at[kind, j], recv_sem=f_recv.at[kind, j],
                device_id={"grp": lax.rem(group + j, groups), "sp": at},
            ))
            end_copies[-1].start()
    field_copies = full_copies + end_copies

    @pl.when(owner)
    def _():
        lane = lax.broadcasted_iota(jnp.int32, (8, LANES), 1)
        at_row = lax.broadcasted_iota(jnp.int32, (8, LANES), 0)
        tiles = [None] * parts

        def increments(p):
            loc = loc_buf[p]
            a = ens_rows(p, 0, slots) * jnp.where(at_slot < items, loc, pltpu.roll(loc, items, 0))
            b = ens_rows(p, slots, 2 * slots) * jnp.where(at_slot < items, loc, pltpu.roll(loc, items - spare, 0))
            rest = total_slots - 2 * slots
            c = ens_rows(p, 2 * slots, total_slots) * loc[2 * spare : 2 * spare + rest]
            hi, lo = split2(jnp.concatenate([a, b, c], axis=0))
            return spread * dot(pick[...], jnp.concatenate([hi, lo], axis=0))

        def offset(i):
            return (i + low) % parts

        def put_increments(i):
            after, before = tiles[i - 1][:, :LANES], tiles[(i + 1) % parts][:, cols - LANES :]
            ends = jnp.where(lane < LANES // 2, after, before)
            pieces = [tiles[i][:, h * LANES : (h + 1) * LANES] for h in range(halves)]
            for v in range(3):
                window = (lane >= 2 * HALO * v) & (lane < 2 * HALO * (v + 1)) & (at_row >= 3 * per)
                moved = pltpu.roll(ends, 2 * HALO * v + HALO, 1)
                if 3 * per - per * v:
                    moved = pltpu.roll(moved, 3 * per - per * v, 0)
                pieces[0] = jnp.where(window, moved, pieces[0])
            snd_i[offset(i)] = jnp.concatenate(pieces, axis=0).astype(BF16)

        batch = owners // BATCHES
        for first_of in range(0, owners, batch):
            blocks = [i for k in range(first_of, first_of + batch) for i in (k, k + owners)]
            for i in blocks:
                if offset(i) > 0:
                    enses.receive(offset(i))
            for i in blocks:
                tiles[i] = increments(lax.rem(part + parts - offset(i), parts))
            ready = [i for k in range(first_of - 1, first_of + batch - 1) if k > 0 for i in (k, k + owners)]
            if first_of + batch == owners:
                ready += [owners - 1, parts - 1, 0, owners]
            for i in ready:
                put_increments(i)
            for i in ready:
                for j in range(groups):
                    if offset(i) + j > 0:
                        inc_copy(offset(i), j).start()
        rcv_i[group, mine] = snd_i[0]

    for copy in field_copies:
        copy.wait_recv()
    lane = lax.broadcasted_iota(jnp.int32, (tile_rows, LANES), 1)
    for g in range(groups):
        at = slice(g * tile_rows, (g + 1) * tile_rows)
        for f in range(9):
            wide[f, at, :cols] = rcv_f[g, f]
            if f in haloed:
                back = LANES - (2 * HALO * haloed.index(f) + HALO)
                before, after = (pltpu.roll(rcv_edge[side, g], back, 1) for side in (0, 1))
                wide[f, at, cols:] = jnp.where(lane < LANES // 2, after, before)
            else:
                wide[f, at, cols:] = jnp.zeros((tile_rows, LANES), F32)

    row_at = lax.broadcasted_iota(jnp.int32, (rows, cols + LANES), 0).astype(F32)
    rotation = 0.1 + 0.2 * (row_at + 0.5) / rows
    for j in range(groups):
        for k in range(owners):
            g, at = lax.rem(group + j, groups), lax.rem(part + k, owners)
            arrival = pltpu.make_async_remote_copy(
                src_ref=snd_i.at[0], dst_ref=rcv_i.at[g, at],
                send_sem=i_send.at[0, 0], recv_sem=i_recv.at[g, at], device_id={"sp": left},
            )
            if j == 0:
                pl.when(at != mine)(arrival.wait_recv)
            else:
                arrival.wait_recv()
    total = rcv_i[0].astype(F32)
    for g in range(1, groups):
        total = total + rcv_i[g].astype(F32)
    message[...] = total

    def gathered(index):
        return jnp.concatenate([message[:, index + j, :] for j in range(per)], axis=0)

    ends = gathered(3 * per)
    state0 = []
    for v in range(3):
        pieces = [gathered(8 * h + per * v) for h in range(halves)]
        pieces.append(pltpu.roll(ends, LANES - (2 * HALO * v + HALO), 1))
        state0.append(jnp.concatenate(pieces, axis=1) + wide[v])
    state1 = model_step(state0, rotation)
    state2 = model_step(state1, rotation)
    forcing = [wide[3 + t] * s[0] - wide[6 + t] for t, s in enumerate((state0, state1, state2))]
    h, u, w = forcing[2], COURANT * dx(forcing[2]), COURANT * dy(forcing[2])
    h, u, w = adjoint_step((h + forcing[1], u, w), rotation)
    for v, field in enumerate((h + forcing[0], u, w)):
        field = field[:, :cols]
        adjoint[v] = field
        half = field.astype(BF16).astype(F32)
        for h in range(halves):
            for j in range(per):
                message[:, 8 * h + per * v + j, :] = half[j * owners : (j + 1) * owners, h * LANES : (h + 1) * LANES]
    snd_h[...] = message[...].astype(BF16)
    halfs.start()
    for v in range(3):
        grad_control_ref[v] = control[v] + std[v] * adjoint[v, tile, :]

    @pl.when(owner)
    def _():
        halfs.take_own()
        weighted = [None] * parts
        middle = range(low, low + owners)
        for p in middle:
            halfs.receive_from(p)
        for p in [*middle, *[p for p in range(parts) if p not in middle]]:
            if p == 0:
                for other in range(parts):
                    if other not in middle:
                        halfs.receive_from(other)
            came_h = rcv_h[p].astype(F32)

            def row_of(v, j):
                pieces = [came_h[8 * h + per * v + j : 8 * h + per * v + j + 1] for h in range(halves)]
                return jnp.broadcast_to(jnp.concatenate(pieces, axis=1), (slots, cols))

            def field_of(v, count):
                out = row_of(v, per - 1)
                for j in reversed(range(per - 1)):
                    out = jnp.where(at_slot < (j + 1) * members, row_of(v, j), out)
                return out

            third = field_of(2, items)
            a = ens_rows(p, 0, slots) * jnp.where(at_slot < items, field_of(0, items), pltpu.roll(third, items, 0))
            b = ens_rows(p, slots, 2 * slots) * jnp.where(
                at_slot < items, field_of(1, items), pltpu.roll(third, items - spare, 0)
            )
            rest = total_slots - 2 * slots
            c = ens_rows(p, 2 * slots, total_slots) * third[2 * spare : 2 * spare + rest]
            own = jnp.concatenate([jnp.zeros((2 * spare, cols), F32), c], axis=0)[:slots]
            own = jnp.where(at_slot < 2 * spare, pltpu.roll(b, slots - (items - spare), 0), own)
            own = jnp.where(at_slot < spare, pltpu.roll(a, slots - items, 0), own)
            weighted[p] = a + b + own
        outs = filtered([[x[:, h * LANES : (h + 1) * LANES] for x in weighted] for h in range(halves)], False)
        for p in range(parts):
            for h in range(halves):
                out_stage[p, h * items : (h + 1) * items, :] = outs[h][p][:items]
            snd_o[p] = out_stage[p].astype(BF16)
        for i in range(parts):
            pl.when(part != i)(out_copy(i).start)
        rcv_o[mine] = snd_o[part]

    for k in range(owners):
        at = lax.rem(part + k, owners)
        arrival = pltpu.make_async_remote_copy(
            src_ref=snd_o.at[0], dst_ref=rcv_o.at[at],
            send_sem=o_send.at[0], recv_sem=o_recv.at[at], device_id={"sp": left},
        )
        pl.when(at != mine)(arrival.wait_recv)
        stage[at] = rcv_o[at].astype(F32)
    for m in range(members):
        for j in range(per):
            for h in range(halves):
                at, lanes = slice(j * owners, (j + 1) * owners), slice(h * LANES, (h + 1) * LANES)
                corr_ref[m, at, lanes] = alpha[m, at, lanes] + spread * stage[:, h * items + j * members + m, :]
    alphas.finish()
    enses.finish()
    halfs.finish()
    for copy in field_copies:
        copy.wait_send()

    @pl.when(owner)
    def _():
        for i in range(parts):
            for j in range(groups):
                if i + j > 0:
                    inc_copy(i, j).wait_send()
        for i in range(parts):
            pl.when(part != i)(out_copy(i).wait_send)


def finish(corr_ref, grad_control_ref, corr_out, grad_control_out, sem):
    copies = [
        pltpu.make_async_copy(corr_ref, corr_out, sem.at[0]),
        pltpu.make_async_copy(grad_control_ref, grad_control_out, sem.at[1]),
    ]
    for copy in copies:
        copy.start()
    for copy in copies:
        copy.wait()


def tables(parts, cols, waves, members, rows):
    length = parts * cols
    inner = waves // parts
    residues = parts // 2 + 1
    twist = 2 * np.pi * np.outer(np.arange(residues), np.arange(cols)) / length
    quotient = np.arange(-inner, inner)
    phase = 2 * np.pi * (np.outer(np.arange(cols), quotient) % cols) / cols
    c, s = np.cos(phase), np.sin(phase)
    forward = np.block([[c, -s], [s, c]])
    owners, per, items, slots, spare, total_slots = layout(members, rows, parts)
    pick = np.zeros((8, 2, total_slots), np.float32)
    for v in range(3):
        for j in range(per):
            for m in range(members):
                pick[v * per + j, :, slot_of(v, j * members + m, items, slots, spare)] = 1.0
    return (
        *both(forward), *both(forward.T.copy()), np.cos(twist).astype(np.float32), np.sin(twist).astype(np.float32),
        pick.reshape(8, 2 * total_slots).astype(BF16),
    )


def per_device(alpha, ensemble, static_std, control, loc_spectrum, obs_cell, obs_step, innovation, obs_weight):
    members, rows, cols = alpha.shape
    groups, parts = lax.axis_size("grp"), lax.axis_size("sp")
    spread = 1.0 / math.sqrt(members * groups - 1)
    owners, per, items, slots, spare, total_slots = layout(members, rows, parts)
    assert owners * per == rows and 4 * per <= 8 and spare % 4 == 0
    tile_rows = control.shape[1]
    halves = cols // LANES
    residues = parts // 2 + 1
    inner = loc_spectrum.shape[0] // parts
    operands = (
        alpha, ensemble, static_std, control, loc_spectrum[None],
        obs_cell[None], obs_step[None], innovation[None], obs_weight[None],
        *tables(parts, cols, loc_spectrum.shape[0], members, rows),
    )
    packed = (round8(halves * items), LANES)
    ens_packed = (round8(3 * halves * items), LANES)
    message = (8 * halves, LANES)
    vmem = pl.BlockSpec(memory_space=pltpu.VMEM)
    dma = pltpu.SemaphoreType.DMA
    corr, grad_control = pl.pallas_call(
        functools.partial(kernel, groups, parts, spread),
        out_shape=(
            pltpu.VMEM(alpha.shape, F32),
            pltpu.VMEM(control.shape, F32),
        ),
        in_specs=[HBM] * len(operands),
        out_specs=(vmem, vmem),
        scratch_shapes=[
            *[pltpu.VMEM(t.shape, t.dtype) for t in operands],
            pltpu.VMEM((owners, *packed), F32),
            pltpu.VMEM((parts, *packed), F32),
            pltpu.VMEM((owners, *ens_packed), F32),
            pltpu.VMEM((parts, slots, cols), F32),
            pltpu.VMEM((3, rows, cols), F32),
            pltpu.VMEM((round8(residues), 4 * inner), F32),
            pltpu.VMEM((9, tile_rows, cols), F32),
            pltpu.VMEM((9, rows, cols + LANES), F32),
            pltpu.VMEM((owners, *message), F32),
            pltpu.VMEM((owners, *packed), BF16), pltpu.VMEM((parts, *packed), BF16),
            pltpu.VMEM((owners, *ens_packed), BF16), pltpu.VMEM((parts, *ens_packed), BF16),
            pltpu.VMEM((parts, *message), BF16), pltpu.VMEM((groups, owners, *message), BF16),
            pltpu.VMEM((owners, *message), BF16), pltpu.VMEM((parts, *message), BF16),
            pltpu.VMEM((parts, *packed), BF16), pltpu.VMEM((owners, *packed), BF16),
            pltpu.VMEM((groups, 9, tile_rows, cols), F32),
            pltpu.VMEM((tile_rows, LANES), F32), pltpu.VMEM((2, groups, tile_rows, LANES), F32),
            dma((len(operands),)),
            dma((owners,)), dma((parts,)), dma((owners,)), dma((parts,)),
            dma((parts, groups)), dma((groups, owners)),
            dma((owners,)), dma((parts,)), dma((parts,)), dma((owners,)),
            dma((3, groups)), dma((3, groups)),
            pltpu.SemaphoreType.REGULAR, pltpu.SemaphoreType.REGULAR, pltpu.SemaphoreType.REGULAR,
        ],
        compiler_params=pltpu.CompilerParams(collective_id=0, has_side_effects=True, vmem_limit_bytes=63 << 20),
    )(*operands)
    return pl.pallas_call(
        finish,
        out_shape=(jax.ShapeDtypeStruct(alpha.shape, F32), jax.ShapeDtypeStruct(control.shape, F32)),
        in_specs=[vmem] * 2,
        out_specs=(HBM, HBM),
        scratch_shapes=[dma((2,))],
        compiler_params=pltpu.CompilerParams(vmem_limit_bytes=1 << 20),
    )(corr, grad_control)


def solution(mesh):
    flat = P(("grp", "sp"))
    tile = P(None, "grp", "sp")
    return jax.shard_map(
        per_device,
        mesh=mesh,
        in_specs=(P("grp", None, "sp"), P("grp", None, None, "sp"), tile, tile, P(), flat, flat, flat, flat),
        out_specs=(P("grp", None, "sp"), tile),
        check_vma=False,
    )
```

```python
import functools
import math

import jax
import jax.numpy as jnp
import numpy as np
from jax import lax
from jax.experimental import pallas as pl
from jax.experimental.pallas import tpu as pltpu
from jax.sharding import PartitionSpec as P

COURANT = 0.4
LANES = 128
HALO = 8
BATCHES = 4
BF16, F32 = jnp.bfloat16, jnp.float32
HBM = pl.BlockSpec(memory_space=pltpu.HBM)


def dot(a, b, contract=((1,), (0,))):
    return lax.dot_general(a, b, (contract, ((), ())), preferred_element_type=F32)


def split2(x):
    hi = x.astype(BF16)
    return hi, (x - hi.astype(F32)).astype(BF16)


def both(table):
    table = np.asarray(table, np.float32)
    hi = table.astype(BF16)
    return hi, (table - hi.astype(np.float32)).astype(BF16)


def add(a, b, sign=1.0):
    re = a[0] + b[0] if sign > 0 else a[0] - b[0]
    if b[1] is None:
        return re, a[1]
    if a[1] is None:
        return re, b[1] if sign > 0 else -b[1]
    return re, a[1] + b[1] if sign > 0 else a[1] - b[1]


def conj(a):
    return a[0], None if a[1] is None else -a[1]


def turn(a, eighths, n):
    at = (eighths % n) / n
    if at == 0:
        return a
    re, im = a
    if at == 0.25:
        return (jnp.zeros_like(re) if im is None else -im), re
    if at == 0.75:
        return (jnp.zeros_like(re) if im is None else im), -re
    c, s = math.cos(2 * math.pi * at), math.sin(2 * math.pi * at)
    if im is None:
        return c * re, s * re
    return c * re - s * im, c * im + s * re


def real_dft(xs):
    n = len(xs)
    if n == 1:
        return [(xs[0], None)]
    if n == 2:
        return [(xs[0] + xs[1], None), (xs[0] - xs[1], None)]
    half = n // 2
    even, odd = real_dft(xs[0::2]), real_dft(xs[1::2])
    out = [None] * (half + 1)
    for k in range(half // 2 + 1):
        t = turn(odd[k], -k, n)
        out[k] = add(even[k], t)
        if half - k != k:
            out[half - k] = conj(add(even[k], t, -1.0))
    return out


def real_sum(zs, n):
    if n == 1:
        return [zs[0][0]]
    if n == 2:
        return [zs[0][0] + zs[1][0], zs[0][0] - zs[1][0]]
    half = n // 2
    even, odd = [], []
    for k in range(half // 2 + 1):
        if half - k == k:
            even.append(zs[k])
            odd.append(turn(zs[k], k, n))
        else:
            other = conj(zs[half - k])
            even.append(add(zs[k], other))
            odd.append(turn(add(zs[k], other, -1.0), k, n))
    even, odd = real_sum(even, half), real_sum(odd, half)
    return [(even, odd)[p % 2][p // 2] for p in range(n)]


def dx(q):
    width = q.shape[1]
    return 0.5 * (pltpu.roll(q, width - 1, 1) - pltpu.roll(q, 1, 1))


def dy(q):
    rows = q.shape[0]
    at = lax.broadcasted_iota(jnp.int32, q.shape, 0)
    above = jnp.where(at < rows - 1, pltpu.roll(q, rows - 1, 0), 0.0)
    below = jnp.where(at > 0, pltpu.roll(q, 1, 0), 0.0)
    return 0.5 * (above - below)


def model_step(state, rotation):
    h, u, w = state
    h = h - COURANT * (dx(u) + dy(w))
    return h, u - COURANT * dx(h) + rotation * w, w - COURANT * dy(h) - rotation * u


def adjoint_step(state, rotation):
    h, u, w = state
    a = h + COURANT * (dx(u) + dy(w))
    return a, u - rotation * w + COURANT * dx(a), w + rotation * u + COURANT * dy(a)


def round8(n):
    return -(-n // 8) * 8


def layout(members, rows, parts):
    owners = parts // 2
    per = rows // owners
    items = per * members
    slots = round8(items)
    spare = slots - items
    return owners, per, items, slots, spare, 2 * slots + round8(items - 2 * spare)


def half_row(slot, half, halves, used):
    whole_rows = used // 8 * 8
    if slot < whole_rows:
        return half * whole_rows + slot
    return halves * whole_rows + half * (used - whole_rows) + slot - whole_rows


def slot_of(v, item, items, slots, spare):
    if v < 2:
        return v * slots + item
    if item < spare:
        return items + item
    if item < 2 * spare:
        return slots + items + item - spare
    return 2 * slots + item - 2 * spare


def kernel(
    groups, parts, spread,
    alpha_any, ens_any, std_any, control_any, spectrum_any, cell_any, step_any, innovation_any, weight_any,
    fwd_hi_any, fwd_lo_any, inv_hi_any, inv_lo_any, tw_c_any, tw_s_any, pick_any,
    corr_ref, grad_control_ref,
    alpha, ens, std, control, spectrum, cell, step, innovation, weight,
    fwd_hi, fwd_lo, inv_hi, inv_lo, tw_c, tw_s, pick,
    stage, out_stage, ens_stage, loc_buf, adjoint, waves, fields, wide, message,
    snd_a, rcv_a, snd_e, rcv_e, snd_i, rcv_i, snd_h, rcv_h, snd_o, rcv_o, rcv_f, edge, rcv_edge,
    load_sem, a_send, a_recv, e_send, e_recv, i_send, i_recv, h_send, h_recv, o_send, o_recv, f_send, f_recv, here, whole, go,
):
    group, part = lax.axis_index("grp"), lax.axis_index("sp")
    left, right = lax.rem(part + parts - 1, parts), lax.rem(part + 1, parts)
    members, rows, cols = alpha.shape
    tile_rows = control.shape[1]
    tile = pl.ds(pl.multiple_of(group * tile_rows, tile_rows), tile_rows)
    owners, per, items, slots, spare, total_slots = layout(members, rows, parts)
    used = 3 * items
    low = parts // 4
    mine = part - low
    owner = (part >= low) & (part < low + owners)
    halves = cols // LANES
    residues = parts // 2 + 1

    barrier = pltpu.get_barrier_semaphore()

    @pl.when(owner)
    def _():
        for i in range(1, parts):
            pl.semaphore_signal(barrier, inc=1, device_id={"sp": lax.rem(part + i, parts)})

    for j in range(1, groups):
        pl.semaphore_signal(barrier, inc=1, device_id={"grp": lax.rem(group + j, groups)})

    pairs = [
        (alpha_any, alpha), (ens_any, ens), (cell_any, cell), (step_any, step), (innovation_any, innovation),
        (weight_any, weight), (std_any, std), (control_any, control), (spectrum_any, spectrum),
        (fwd_hi_any, fwd_hi), (fwd_lo_any, fwd_lo), (inv_hi_any, inv_hi), (inv_lo_any, inv_lo),
        (tw_c_any, tw_c), (tw_s_any, tw_s), (pick_any, pick),
    ]
    loads = [pltpu.make_async_copy(a, b, load_sem.at[i]) for i, (a, b) in enumerate(pairs)]
    for load in loads:
        load.start()

    loads[0].wait()
    filled = halves * items
    if stage.shape[1] > filled:
        stage[:, filled:, :] = jnp.zeros((owners, stage.shape[1] - filled, LANES), F32)
    for m in range(members):
        for j in range(per):
            for h in range(halves):
                stage[:, h * items + j * members + m, :] = (
                    alpha[m, j * owners : (j + 1) * owners, h * LANES : (h + 1) * LANES]
                )
    snd_a[...] = stage[...].astype(BF16)

    @pl.when(owner)
    def _():
        pl.semaphore_wait(barrier, owners + groups - 2)

    @pl.when(jnp.logical_not(owner))
    def _():
        pl.semaphore_wait(barrier, owners + groups - 1)
        for i in range(owners):
            pl.semaphore_signal(here, inc=1, device_id={"sp": low + lax.rem(part + i, owners)})

    class ToOwners:
        def __init__(self, source, target, send, recv):
            self.source, self.target, self.send, self.recv = source, target, send, recv

        def copy(self, i):
            at = lax.rem(part + i, owners)
            return low + at, pltpu.make_async_remote_copy(
                src_ref=self.source.at[at], dst_ref=self.target.at[part],
                send_sem=self.send.at[i], recv_sem=self.recv.at[part], device_id={"sp": low + at},
            )

        def start(self):
            for i in range(owners):
                to, copy = self.copy(i)
                pl.when(to != part)(copy.start)

        def take_own(self):
            self.target[part] = self.source[mine]

        def receive(self, i):
            at = lax.rem(part + parts - i, parts)
            pltpu.make_async_remote_copy(
                src_ref=self.source.at[0], dst_ref=self.target.at[at],
                send_sem=self.send.at[0], recv_sem=self.recv.at[at], device_id={"sp": left},
            ).wait_recv()

        def receive_from(self, p):
            arrival = pltpu.make_async_remote_copy(
                src_ref=self.source.at[0], dst_ref=self.target.at[p],
                send_sem=self.send.at[0], recv_sem=self.recv.at[p], device_id={"sp": left},
            )
            if low <= p < low + owners:
                pl.when(part != p)(arrival.wait_recv)
            else:
                arrival.wait_recv()

        def finish(self):
            for i in range(owners):
                to, copy = self.copy(i)
                pl.when(to != part)(copy.wait_send)

    alphas = ToOwners(snd_a, rcv_a, a_send, a_recv)
    enses = ToOwners(snd_e, rcv_e, e_send, e_recv)
    halfs = ToOwners(snd_h, rcv_h, h_send, h_recv)
    alphas.start()
    loads[1].wait()
    if ens_stage.shape[1] > halves * used:
        ens_stage[:, halves * used :, :] = jnp.zeros((owners, ens_stage.shape[1] - halves * used, LANES), F32)
    for v in range(3):
        for m in range(members):
            field = ens[m, v].astype(F32)
            for j in range(per):
                for h in range(halves):
                    at = half_row(slot_of(v, j * members + m, items, slots, spare), h, halves, used)
                    ens_stage[:, at, :] = field[j * owners : (j + 1) * owners, h * LANES : (h + 1) * LANES]
    snd_e[...] = ens_stage[...].astype(BF16)
    enses.start()

    for load in loads[2:8]:
        load.wait()
    pitch = -(-tile_rows // 8) * 8
    nx = cols * parts
    first = group * tile_rows
    row = jnp.zeros_like(cell)
    cells = cell[...]
    for r in range(1, tile_rows):
        row = row + jnp.where(cells >= (first + r) * nx, 1, 0)
    col = cells - (first + row) * nx - part * cols
    slot = step[...] * pitch + row
    observations = cells.shape[1]
    in_col = (lax.broadcasted_iota(jnp.int32, (cols, observations), 0) == col).astype(F32).astype(BF16)
    in_slot = lax.broadcasted_iota(jnp.int32, (3 * pitch, observations), 0) == slot
    obs_weight = weight[...]
    values = jnp.concatenate([
        jnp.where(in_slot, obs_weight, 0.0), jnp.where(in_slot, obs_weight * innovation[...], 0.0)
    ], axis=0)
    hi, lo = split2(values)
    summed = dot(hi, in_col, ((1,), (1,))) + dot(lo, in_col, ((1,), (1,)))
    for v in range(3):
        fields[v] = std[v] * control[v]
    for f in range(6):
        fields[3 + f] = summed[f * pitch : f * pitch + tile_rows]
    haloed = (0, 1, 2, 4, 5, 7, 8)
    lane = lax.broadcasted_iota(jnp.int32, (tile_rows, LANES), 1)
    packed = jnp.zeros((tile_rows, LANES), F32)
    for e, f in enumerate(haloed):
        ends = jnp.where(lane < LANES // 2, fields[f, :, :LANES], fields[f, :, cols - LANES :])
        window = (lane >= 2 * HALO * e) & (lane < 2 * HALO * (e + 1))
        packed = jnp.where(window, pltpu.roll(ends, (2 * HALO * e + HALO) % LANES, 1), packed)
    edge[...] = packed

    rcv_f[group] = fields[...]
    full_copies = [
        pltpu.make_async_remote_copy(
            src_ref=fields, dst_ref=rcv_f.at[group],
            send_sem=f_send.at[0, j], recv_sem=f_recv.at[0, j], device_id={"grp": lax.rem(group + j, groups)},
        )
        for j in range(1, groups)
    ]
    for copy in full_copies:
        copy.start()

    @pl.when(owner)
    def _():
        pl.semaphore_wait(here, parts - owners)
        for j in range(1, groups):
            pl.semaphore_signal(whole, inc=1, device_id={"grp": lax.rem(group + j, groups)})

    for load in loads[8:]:
        load.wait()

    def filtered(xs, exact):
        pieces = xs
        spectra = [real_dft(piece) for piece in pieces]
        res, ims = [], []
        for k1 in range(residues):
            parts_re, parts_im = [], []
            for h in range(halves):
                c = tw_c[k1 : k1 + 1, h * LANES : (h + 1) * LANES]
                s = tw_s[k1 : k1 + 1, h * LANES : (h + 1) * LANES]
                re, im = spectra[h][k1]
                if k1 == 0:
                    parts_re.append(re)
                    parts_im.append(jnp.zeros_like(re))
                elif im is None:
                    parts_re.append(re * c)
                    parts_im.append(-re * s)
                else:
                    parts_re.append(re * c + im * s)
                    parts_im.append(im * c - re * s)
            res.append(jnp.concatenate(parts_re + parts_im, axis=1))
        y_hi, y_lo = split2(jnp.concatenate(res, axis=0))
        z = dot(y_hi, fwd_hi[...])
        if exact:
            z = z + dot(y_lo, fwd_hi[...]) + dot(y_hi, fwd_lo[...])
        z = jnp.concatenate(
            [z[k1 * slots : (k1 + 1) * slots] * waves[k1 : k1 + 1, :] for k1 in range(residues)], axis=0
        )
        z_hi, z_lo = split2(z)
        v = dot(z_hi, inv_hi[...])
        if exact:
            v = v + dot(z_lo, inv_hi[...]) + dot(z_hi, inv_lo[...])
        outs = []
        for h in range(halves):
            zs = []
            for k1 in range(residues):
                c = tw_c[k1 : k1 + 1, h * LANES : (h + 1) * LANES]
                s = tw_s[k1 : k1 + 1, h * LANES : (h + 1) * LANES]
                at = slice(k1 * slots, (k1 + 1) * slots)
                re = v[at, h * LANES : (h + 1) * LANES]
                im = v[at, cols + h * LANES : cols + (h + 1) * LANES]
                zs.append((re, im) if k1 == 0 else (re * c - im * s, im * c + re * s))
            outs.append(real_sum(zs, parts))
        return outs

    at_slot = lax.broadcasted_iota(jnp.int32, (slots, cols), 0)

    def ens_rows(p, first_slot, last_slot):
        full = used // 8 * 8
        pieces = []
        for h in range(halves):
            rows_of = [rcv_e[p, h * full + first_slot : h * full + min(last_slot, full)].astype(F32)]
            if last_slot > full:
                tail = rcv_e[p, halves * full : halves * full + 8].astype(F32)
                rows_of.append(tail if h == 0 else pltpu.roll(tail, 8 - h * (used - full), 0))
            pieces.append(jnp.concatenate(rows_of, axis=0))
        return jnp.concatenate(pieces, axis=1)

    def inc_copy(i, j):
        return pltpu.make_async_remote_copy(
            src_ref=snd_i.at[i], dst_ref=rcv_i.at[group, mine],
            send_sem=i_send.at[i, j], recv_sem=i_recv.at[group, mine],
            device_id={"grp": lax.rem(group + j, groups), "sp": lax.rem(part + parts - i, parts)},
        )

    def out_copy(i):
        to = i
        return pltpu.make_async_remote_copy(
            src_ref=snd_o.at[to], dst_ref=rcv_o.at[mine],
            send_sem=o_send.at[i], recv_sem=o_recv.at[mine], device_id={"sp": to},
        )

    @pl.when(owner)
    def _():
        count = spectrum.shape[1]
        inner = count // parts
        wave = lax.broadcasted_iota(jnp.int32, (waves.shape[0], count), 1)
        residue = lax.broadcasted_iota(jnp.int32, wave.shape, 0)
        weights = jnp.broadcast_to(spectrum[...], wave.shape)
        forward = jnp.where((lax.rem(wave, parts) == residue) & (residue < residues), weights, 0.0)
        mirrored = (lax.rem(wave + residue, parts) == 0) & (residue > 0) & (residue < residues - 1)
        backward = jnp.where(mirrored, weights, 0.0)
        k = lax.broadcasted_iota(jnp.int32, (count, 4 * inner), 0)
        j = lax.rem(lax.broadcasted_iota(jnp.int32, (count, 4 * inner), 1), 2 * inner)
        ahead, behind = k - parts * (j - inner), k - parts * (inner - 1 - j)
        ahead = jnp.where((ahead >= 0) & (ahead < parts), 1.0, 0.0).astype(BF16)
        behind = jnp.where((behind >= 0) & (behind < parts), 1.0, 0.0).astype(BF16)
        f_hi, f_lo = split2(forward)
        b_hi, b_lo = split2(backward)
        waves[...] = dot(f_hi, ahead) + dot(f_lo, ahead) + dot(b_hi, behind) + dot(b_lo, behind)

        alphas.take_own()
        enses.take_own()
        for i in range(1, parts):
            alphas.receive(i)
        came = [[None] * parts for _ in range(halves)]
        for p in range(parts):
            x = rcv_a[p].astype(F32)
            for h in range(halves):
                came[h][p] = (x if h == 0 else pltpu.roll(x, x.shape[0] - h * items, 0))[:slots]
        localized = filtered(came, True)
        for p in range(parts):
            loc = jnp.concatenate([localized[h][p] for h in range(halves)], axis=1)
            loc_buf[p] = loc.astype(BF16).astype(F32)
    @pl.when(owner)
    def _():
        if groups > 1:
            pl.semaphore_wait(whole, groups - 1)
        for i in range(parts // owners):
            to = mine * (parts // owners) + i

            @pl.when(to != part)
            def _():
                pl.semaphore_signal(go, inc=1, device_id={"sp": to})

    @pl.when(part // (parts // owners) != mine)
    def _():
        pl.semaphore_wait(go, 1)

    end_copies = []
    for j in range(groups):
        for kind, at, target in ((1, right, rcv_edge.at[0, group]), (2, left, rcv_edge.at[1, group])):
            end_copies.append(pltpu.make_async_remote_copy(
                src_ref=edge, dst_ref=target, send_sem=f_send.at[kind, j], recv_sem=f_recv.at[kind, j],
                device_id={"grp": lax.rem(group + j, groups), "sp": at},
            ))
            end_copies[-1].start()
    field_copies = full_copies + end_copies

    @pl.when(owner)
    def _():
        lane = lax.broadcasted_iota(jnp.int32, (8, LANES), 1)
        at_row = lax.broadcasted_iota(jnp.int32, (8, LANES), 0)
        tiles = [None] * parts

        def increments(p):
            loc = loc_buf[p]
            a = ens_rows(p, 0, slots) * jnp.where(at_slot < items, loc, pltpu.roll(loc, items, 0))
            b = ens_rows(p, slots, 2 * slots) * jnp.where(at_slot < items, loc, pltpu.roll(loc, items - spare, 0))
            rest = total_slots - 2 * slots
            c = ens_rows(p, 2 * slots, total_slots) * loc[2 * spare : 2 * spare + rest]
            return spread * dot(pick[:, :total_slots], jnp.concatenate([a, b, c], axis=0).astype(BF16))

        def offset(i):
            return (i + low) % parts

        def put_increments(i):
            after, before = tiles[i - 1][:, :LANES], tiles[(i + 1) % parts][:, cols - LANES :]
            ends = jnp.where(lane < LANES // 2, after, before)
            pieces = [tiles[i][:, h * LANES : (h + 1) * LANES] for h in range(halves)]
            for v in range(3):
                window = (lane >= 2 * HALO * v) & (lane < 2 * HALO * (v + 1)) & (at_row >= 3 * per)
                moved = pltpu.roll(ends, 2 * HALO * v + HALO, 1)
                if 3 * per - per * v:
                    moved = pltpu.roll(moved, 3 * per - per * v, 0)
                pieces[0] = jnp.where(window, moved, pieces[0])
            snd_i[offset(i)] = jnp.concatenate(pieces, axis=0).astype(BF16)

        batch = owners // BATCHES
        for first_of in range(0, owners, batch):
            blocks = [i for k in range(first_of, first_of + batch) for i in (k, k + owners)]
            for i in blocks:
                if offset(i) > 0:
                    enses.receive(offset(i))
            for i in blocks:
                tiles[i] = increments(lax.rem(part + parts - offset(i), parts))
            ready = [i for k in range(first_of - 1, first_of + batch - 1) if k > 0 for i in (k, k + owners)]
            if first_of + batch == owners:
                ready += [owners - 1, parts - 1, 0, owners]
            for i in ready:
                put_increments(i)
            for i in ready:
                for j in range(groups):
                    if offset(i) + j > 0:
                        inc_copy(offset(i), j).start()
        rcv_i[group, mine] = snd_i[0]

    for copy in field_copies:
        copy.wait_recv()
    lane = lax.broadcasted_iota(jnp.int32, (tile_rows, LANES), 1)
    for g in range(groups):
        at = slice(g * tile_rows, (g + 1) * tile_rows)
        for f in range(9):
            wide[f, at, :cols] = rcv_f[g, f]
            if f in haloed:
                back = LANES - (2 * HALO * haloed.index(f) + HALO)
                before, after = (pltpu.roll(rcv_edge[side, g], back, 1) for side in (0, 1))
                wide[f, at, cols:] = jnp.where(lane < LANES // 2, after, before)
            else:
                wide[f, at, cols:] = jnp.zeros((tile_rows, LANES), F32)

    row_at = lax.broadcasted_iota(jnp.int32, (rows, cols + LANES), 0).astype(F32)
    rotation = 0.1 + 0.2 * (row_at + 0.5) / rows
    for j in range(groups):
        for k in range(owners):
            g, at = lax.rem(group + j, groups), lax.rem(part + k, owners)
            arrival = pltpu.make_async_remote_copy(
                src_ref=snd_i.at[0], dst_ref=rcv_i.at[g, at],
                send_sem=i_send.at[0, 0], recv_sem=i_recv.at[g, at], device_id={"sp": left},
            )
            if j == 0:
                pl.when(at != mine)(arrival.wait_recv)
            else:
                arrival.wait_recv()
    total = rcv_i[0].astype(F32)
    for g in range(1, groups):
        total = total + rcv_i[g].astype(F32)
    message[...] = total

    def gathered(index):
        return jnp.concatenate([message[:, index + j, :] for j in range(per)], axis=0)

    ends = gathered(3 * per)
    state0 = []
    for v in range(3):
        pieces = [gathered(8 * h + per * v) for h in range(halves)]
        pieces.append(pltpu.roll(ends, LANES - (2 * HALO * v + HALO), 1))
        state0.append(jnp.concatenate(pieces, axis=1) + wide[v])
    state1 = model_step(state0, rotation)
    state2 = model_step(state1, rotation)
    forcing = [wide[3 + t] * s[0] - wide[6 + t] for t, s in enumerate((state0, state1, state2))]
    h, u, w = forcing[2], COURANT * dx(forcing[2]), COURANT * dy(forcing[2])
    h, u, w = adjoint_step((h + forcing[1], u, w), rotation)
    for v, field in enumerate((h + forcing[0], u, w)):
        field = field[:, :cols]
        adjoint[v] = field
        half = field.astype(BF16).astype(F32)
        for h in range(halves):
            for j in range(per):
                message[:, 8 * h + per * v + j, :] = half[j * owners : (j + 1) * owners, h * LANES : (h + 1) * LANES]
    snd_h[...] = message[...].astype(BF16)
    halfs.start()
    for v in range(3):
        grad_control_ref[v] = control[v] + std[v] * adjoint[v, tile, :]

    @pl.when(owner)
    def _():
        halfs.take_own()
        weighted = [None] * parts
        middle = range(low, low + owners)
        for p in middle:
            halfs.receive_from(p)
        for p in [*middle, *[p for p in range(parts) if p not in middle]]:
            if p == 0:
                for other in range(parts):
                    if other not in middle:
                        halfs.receive_from(other)
            came_h = rcv_h[p].astype(F32)

            def row_of(v, j):
                pieces = [came_h[8 * h + per * v + j : 8 * h + per * v + j + 1] for h in range(halves)]
                return jnp.broadcast_to(jnp.concatenate(pieces, axis=1), (slots, cols))

            def field_of(v, count):
                out = row_of(v, per - 1)
                for j in reversed(range(per - 1)):
                    out = jnp.where(at_slot < (j + 1) * members, row_of(v, j), out)
                return out

            third = field_of(2, items)
            a = ens_rows(p, 0, slots) * jnp.where(at_slot < items, field_of(0, items), pltpu.roll(third, items, 0))
            b = ens_rows(p, slots, 2 * slots) * jnp.where(
                at_slot < items, field_of(1, items), pltpu.roll(third, items - spare, 0)
            )
            rest = total_slots - 2 * slots
            c = ens_rows(p, 2 * slots, total_slots) * third[2 * spare : 2 * spare + rest]
            own = jnp.concatenate([jnp.zeros((2 * spare, cols), F32), c], axis=0)[:slots]
            own = jnp.where(at_slot < 2 * spare, pltpu.roll(b, slots - (items - spare), 0), own)
            own = jnp.where(at_slot < spare, pltpu.roll(a, slots - items, 0), own)
            weighted[p] = a + b + own
        outs = filtered([[x[:, h * LANES : (h + 1) * LANES] for x in weighted] for h in range(halves)], False)
        for p in range(parts):
            for h in range(halves):
                out_stage[p, h * items : (h + 1) * items, :] = outs[h][p][:items]
            snd_o[p] = out_stage[p].astype(BF16)
        for i in range(parts):
            pl.when(part != i)(out_copy(i).start)
        rcv_o[mine] = snd_o[part]

    for k in range(owners):
        at = lax.rem(part + k, owners)
        arrival = pltpu.make_async_remote_copy(
            src_ref=snd_o.at[0], dst_ref=rcv_o.at[at],
            send_sem=o_send.at[0], recv_sem=o_recv.at[at], device_id={"sp": left},
        )
        pl.when(at != mine)(arrival.wait_recv)
        stage[at] = rcv_o[at].astype(F32)
    for m in range(members):
        for j in range(per):
            for h in range(halves):
                at, lanes = slice(j * owners, (j + 1) * owners), slice(h * LANES, (h + 1) * LANES)
                corr_ref[m, at, lanes] = alpha[m, at, lanes] + spread * stage[:, h * items + j * members + m, :]
    alphas.finish()
    enses.finish()
    halfs.finish()
    for copy in field_copies:
        copy.wait_send()

    @pl.when(owner)
    def _():
        for i in range(parts):
            for j in range(groups):
                if i + j > 0:
                    inc_copy(i, j).wait_send()
        for i in range(parts):
            pl.when(part != i)(out_copy(i).wait_send)


def finish(corr_ref, grad_control_ref, corr_out, grad_control_out, sem):
    copies = [
        pltpu.make_async_copy(corr_ref, corr_out, sem.at[0]),
        pltpu.make_async_copy(grad_control_ref, grad_control_out, sem.at[1]),
    ]
    for copy in copies:
        copy.start()
    for copy in copies:
        copy.wait()


def tables(parts, cols, waves, members, rows):
    length = parts * cols
    inner = waves // parts
    residues = parts // 2 + 1
    twist = 2 * np.pi * np.outer(np.arange(residues), np.arange(cols)) / length
    quotient = np.arange(-inner, inner)
    phase = 2 * np.pi * (np.outer(np.arange(cols), quotient) % cols) / cols
    c, s = np.cos(phase), np.sin(phase)
    forward = np.block([[c, -s], [s, c]])
    owners, per, items, slots, spare, total_slots = layout(members, rows, parts)
    pick = np.zeros((8, 2, total_slots), np.float32)
    for v in range(3):
        for j in range(per):
            for m in range(members):
                pick[v * per + j, :, slot_of(v, j * members + m, items, slots, spare)] = 1.0
    return (
        *both(forward), *both(forward.T.copy()), np.cos(twist).astype(np.float32), np.sin(twist).astype(np.float32),
        pick.reshape(8, 2 * total_slots).astype(BF16),
    )


def per_device(alpha, ensemble, static_std, control, loc_spectrum, obs_cell, obs_step, innovation, obs_weight):
    members, rows, cols = alpha.shape
    groups, parts = lax.axis_size("grp"), lax.axis_size("sp")
    spread = 1.0 / math.sqrt(members * groups - 1)
    owners, per, items, slots, spare, total_slots = layout(members, rows, parts)
    assert owners * per == rows and 4 * per <= 8 and spare % 4 == 0
    tile_rows = control.shape[1]
    halves = cols // LANES
    residues = parts // 2 + 1
    inner = loc_spectrum.shape[0] // parts
    operands = (
        alpha, ensemble, static_std, control, loc_spectrum[None],
        obs_cell[None], obs_step[None], innovation[None], obs_weight[None],
        *tables(parts, cols, loc_spectrum.shape[0], members, rows),
    )
    packed = (round8(halves * items), LANES)
    ens_packed = (round8(3 * halves * items), LANES)
    message = (8 * halves, LANES)
    vmem = pl.BlockSpec(memory_space=pltpu.VMEM)
    dma = pltpu.SemaphoreType.DMA
    corr, grad_control = pl.pallas_call(
        functools.partial(kernel, groups, parts, spread),
        out_shape=(
            pltpu.VMEM(alpha.shape, F32),
            pltpu.VMEM(control.shape, F32),
        ),
        in_specs=[HBM] * len(operands),
        out_specs=(vmem, vmem),
        scratch_shapes=[
            *[pltpu.VMEM(t.shape, t.dtype) for t in operands],
            pltpu.VMEM((owners, *packed), F32),
            pltpu.VMEM((parts, *packed), F32),
            pltpu.VMEM((owners, *ens_packed), F32),
            pltpu.VMEM((parts, slots, cols), F32),
            pltpu.VMEM((3, rows, cols), F32),
            pltpu.VMEM((round8(residues), 4 * inner), F32),
            pltpu.VMEM((9, tile_rows, cols), F32),
            pltpu.VMEM((9, rows, cols + LANES), F32),
            pltpu.VMEM((owners, *message), F32),
            pltpu.VMEM((owners, *packed), BF16), pltpu.VMEM((parts, *packed), BF16),
            pltpu.VMEM((owners, *ens_packed), BF16), pltpu.VMEM((parts, *ens_packed), BF16),
            pltpu.VMEM((parts, *message), BF16), pltpu.VMEM((groups, owners, *message), BF16),
            pltpu.VMEM((owners, *message), BF16), pltpu.VMEM((parts, *message), BF16),
            pltpu.VMEM((parts, *packed), BF16), pltpu.VMEM((owners, *packed), BF16),
            pltpu.VMEM((groups, 9, tile_rows, cols), F32),
            pltpu.VMEM((tile_rows, LANES), F32), pltpu.VMEM((2, groups, tile_rows, LANES), F32),
            dma((len(operands),)),
            dma((owners,)), dma((parts,)), dma((owners,)), dma((parts,)),
            dma((parts, groups)), dma((groups, owners)),
            dma((owners,)), dma((parts,)), dma((parts,)), dma((owners,)),
            dma((3, groups)), dma((3, groups)),
            pltpu.SemaphoreType.REGULAR, pltpu.SemaphoreType.REGULAR, pltpu.SemaphoreType.REGULAR,
        ],
        compiler_params=pltpu.CompilerParams(collective_id=0, has_side_effects=True, vmem_limit_bytes=63 << 20),
    )(*operands)
    return pl.pallas_call(
        finish,
        out_shape=(jax.ShapeDtypeStruct(alpha.shape, F32), jax.ShapeDtypeStruct(control.shape, F32)),
        in_specs=[vmem] * 2,
        out_specs=(HBM, HBM),
        scratch_shapes=[dma((2,))],
        compiler_params=pltpu.CompilerParams(vmem_limit_bytes=1 << 20),
    )(corr, grad_control)


def solution(mesh):
    flat = P(("grp", "sp"))
    tile = P(None, "grp", "sp")
    return jax.shard_map(
        per_device,
        mesh=mesh,
        in_specs=(P("grp", None, "sp"), P("grp", None, None, "sp"), tile, tile, P(), flat, flat, flat, flat),
        out_specs=(P("grp", None, "sp"), tile),
        check_vma=False,
    )
```
